32 devices in a mesh: dp: 8 (over y, x, core), mp: 4 (over z).
Axes of the slice: x: 2, y: 2, z: 4, core: 2. Of those that a mesh axis runs over, the one named last changes fastest.
Arguments:
- tokens: bfloat16 [4096, 1024], P('dp', 'mp'), may hold values from -150 to 150
- pre_gain: bfloat16 [1024], P('mp'), may hold values from 0.25 to 1.75
- input_weight: bfloat16 [3, 1024, 1024], P(None, 'dp', 'mp'), may hold values from -0.125 to 0.125
- output_weight: bfloat16 [1024, 1024], P('mp', 'dp'), may hold values from -1 to 1
- position_bias: bfloat16 [16, 512, 512], P('mp'), may hold values from -3 to 353
- post_gain: bfloat16 [1024], P('mp'), may hold values from 0.25 to 1.75
Outputs:
- stream: bfloat16 [4096, 1024], P('dp', 'mp')
- normed: bfloat16 [4096, 1024], P('dp', 'mp')
The draws below stay inside these ranges and needn't reach their ends.
All inputs are finite; a program needn't handle non-finite values.
Results may differ from the reference program's by a relative error of at most 0.013.
Values may be sent and summed in bfloat16 or wider, within the bound.
A program may use at most 64 MiB of HBM per device.

```python
import math
import jax
import jax.numpy as jnp
from jax import lax

SEQ = 512
HEAD_DIM = 64
HEADS = 16
D = 1024
INNER = 1024
TOKENS = 4096


def draw_tokens(key, part):
    subkeys = jax.random.split(jax.random.fold_in(key, 11), 4)
    column_place = jnp.arange(D, dtype=jnp.float32) / D
    baseline = jnp.clip(jax.random.normal(subkeys[0], (TOKENS, D), jnp.float32), -4.0, 4.0)
    row_scale = jnp.exp(jax.random.uniform(subkeys[2], (TOKENS, 1), jnp.float32, math.log(0.4), math.log(4.0)))
    column_scale = jnp.exp(column_place * math.log(3.0))[None, :] * jnp.exp(jax.random.uniform(subkeys[3], (1, D), jnp.float32, math.log(0.7), math.log(1.4)))
    return (baseline * row_scale * column_scale).astype(jnp.bfloat16)


def draw_position_bias(key, part):
    subkeys = jax.random.split(jax.random.fold_in(key, 23), 1)
    bias_shape = (HEADS, SEQ, SEQ)
    return jnp.clip(jax.random.normal(subkeys[0], bias_shape, jnp.float32), -3.0, 3.0).astype(jnp.bfloat16)


def raised(drawn, stream_key, source, target, blocks, factor):
    owner, partner = [(jnp.arange(drawn.shape[axis_at]) // (drawn.shape[axis_at] // blocks)).reshape([-1 if axis == axis_at else 1 for axis in range(drawn.ndim)]) for axis_at in (source, target)]
    chosen = jax.random.permutation(stream_key, blocks)[partner]
    strong = (owner == chosen) | (owner == (partner + blocks // 2) % blocks)
    return jnp.where(strong, factor * drawn, drawn)


def block_levels(rng, dims, cuts, smallest, top_value):
    factor_of, own = 1.0, jax.random.fold_in(rng, 6)
    for dim, shards_of in cuts:
        steps = jnp.exp(jax.random.uniform(jax.random.fold_in(own, dim), (shards_of,), jnp.float32, smallest / len(cuts), top_value / len(cuts)))
        factor_of = factor_of * jnp.repeat(steps, dims[dim] // shards_of).reshape([-1 if axis == dim else 1 for axis in range(len(dims))])
    return factor_of


def normal_values(key, shape, width, reach, cuts=(), kind=jnp.bfloat16):
    entries = jax.random.normal(key, shape, jnp.float32) * width
    if len(cuts) > 0:
        entries = block_levels(key, shape, cuts, -0.22, 0.18) * entries
    return jnp.clip(entries, min=-reach, max=reach).astype(kind)


def heavy_noise(stream_key, shape, width, bound, cuts, heavy, kind=jnp.bfloat16):
    array = width * jax.random.normal(stream_key, shape, jnp.float32)
    if cuts:
        array = array * block_levels(stream_key, shape, cuts, -0.22, 0.18)
    return jnp.clip(raised(array, jax.random.fold_in(stream_key, 3), *heavy), -bound, bound).astype(kind)


def setup_inputs(seed: int = 0) -> dict:
    streams_of = jax.random.split(jax.random.key(seed), 7)
    return {
        "tokens": draw_tokens(jax.random.fold_in(streams_of[6], 71), 0),
        "pre_gain": jnp.clip(1.0 + 0.15 * jax.random.normal(streams_of[1], (D,), jnp.float32), 0.25, 1.75).astype(jnp.bfloat16),
        "input_weight": normal_values(streams_of[2], (3, D, INNER), (2 * D) ** -0.5, 0.125, ((1, 8), (2, 4))),
        "output_weight": heavy_noise(streams_of[3], (INNER, D), (INNER // 16) ** -0.5, 1.0, ((0, 4), (1, 8)), (0, 1, 8, 2.0)),
        "position_bias": draw_position_bias(jax.random.fold_in(streams_of[6], 71), 0),
        "post_gain": jnp.clip(1.0 + 0.15 * jax.random.normal(streams_of[5], (D,), jnp.float32), 0.25, 1.75).astype(jnp.bfloat16),
    }


epsilon = 1e-06

def reference(tokens, pre_gain, input_weight, output_weight, position_bias, post_gain):
    widened = tokens.astype(jnp.float32)
    inverse_rms = lax.rsqrt(lax.optimization_barrier(jnp.mean(widened * widened, axis=1, keepdims=True)) + epsilon)
    normed_in = (widened * inverse_rms * pre_gain.astype(jnp.float32)).astype(jnp.bfloat16)
    projected = [jnp.dot(normed_in, input_weight[member], preferred_element_type=jnp.float32).astype(jnp.bfloat16) for member in range(3)]
    row_count = tokens.shape[0]
    bias_wide = position_bias.astype(jnp.float32)

    def one_sequence(sequence):
        offset = (sequence * SEQ).astype(jnp.int32)
        sliced = [lax.dynamic_slice_in_dim(matrix, offset, SEQ, 0).reshape(SEQ, HEADS, HEAD_DIM).astype(jnp.float32) for matrix in projected]
        scores = jnp.einsum('qhd,khd->hqk', sliced[0], sliced[1]) + bias_wide
        row_max = lax.optimization_barrier(jnp.max(scores, axis=2, keepdims=True))
        weights = jnp.exp(scores - row_max)
        probabilities = (weights / lax.optimization_barrier(jnp.sum(weights, axis=2, keepdims=True))).astype(jnp.bfloat16)
        context = jnp.einsum('hqk,khd->qhd', probabilities.astype(jnp.float32), sliced[2])
        return context.reshape(SEQ, HEADS * HEAD_DIM).astype(jnp.bfloat16)
    stacked = lax.map(one_sequence, jnp.arange(row_count // SEQ, dtype=jnp.int32))
    context = stacked.reshape(row_count, HEADS * HEAD_DIM)
    attention_out = jnp.dot(context, output_weight, preferred_element_type=jnp.float32)
    stream = (widened + attention_out).astype(jnp.bfloat16)
    restored = lax.optimization_barrier(stream).astype(jnp.float32)
    post_rms = lax.rsqrt(lax.optimization_barrier(jnp.mean(restored * restored, axis=1, keepdims=True)) + epsilon)
    normed = (restored * post_rms * post_gain.astype(jnp.float32)).astype(jnp.bfloat16)
    return (stream, normed)
```

```python
import functools

import jax
import jax.numpy as jnp
from jax import lax
from jax.experimental import pallas as pl
from jax.experimental.pallas import tpu as pltpu
from jax.sharding import PartitionSpec as P

epsilon = 1e-06
F32, BF16 = jnp.float32, jnp.bfloat16


def kernel(
    n,
    groups,
    chunks,
    lag,
    wide,
    tok,
    pre,
    win,
    wout,
    bias,
    stream_o,
    square_o,
    x_all,
    gain_all,
    w_all,
    wo_all,
    bias_v,
    acc,
    square,
    qkv,
    part,
    out_buf,
    from_below,
    from_above,
    ss_mine,
    ss_all,
    ag_send,
    ag_recv,
    g_send,
    g_recv,
    w_send,
    w_recv,
    o_send,
    o_recv,
    rs_send,
    rs_recv,
    ss_send,
    ss_recv,
    local_sem,
    link_free,
):
    rows, feats = tok.shape
    step = rows // chunks
    heads, seq = bias.shape[0], bias.shape[1]
    inner = win.shape[2]
    head_dim = inner // heads
    model = n * feats
    wrows = win.shape[1]
    wcols = model // groups
    half = groups // 2
    me = lax.axis_index("mp")
    d = lax.axis_index("dp")
    odd = lax.rem(d, 2)
    pair = d // 2
    partner = d + 1 - 2 * odd

    def rows_at(c):
        return pl.ds(pl.multiple_of(c * step, step), step)

    def feats_at(s):
        return pl.ds(pl.multiple_of(s * feats, feats), feats)

    def tok_copy(s, c, up, own):
        src = tok.at[rows_at(c)] if own else x_all.at[s, rows_at(c)]
        return pltpu.make_async_remote_copy(
            src_ref=src,
            dst_ref=x_all.at[s, rows_at(c)],
            send_sem=ag_send.at[up, s, c],
            recv_sem=ag_recv.at[s, c],
            device_id={"mp": me + 2 * up - 1},
            device_id_type=pl.DeviceIdType.MESH,
        )

    def gain_copy(origin, target):
        return pltpu.make_async_remote_copy(
            src_ref=pre,
            dst_ref=gain_all.at[feats_at(origin)],
            send_sem=g_send.at[target],
            recv_sem=g_recv.at[origin],
            device_id={"mp": target},
            device_id_type=pl.DeviceIdType.MESH,
        )

    def w_slot(o):
        return w_all.at[:, pl.ds(pl.multiple_of(o * wrows, wrows), wrows), :]

    def o_slot(o):
        block = pl.ds(pl.multiple_of(o * wcols, wcols), wcols)
        return wo_all.at[:, block] if wide else wo_all.at[block, :]

    def weight_copy(which, o, target, forward):
        slot, ref, send, recv = (
            (w_slot, win, w_send, w_recv) if which == 0 else (o_slot, wout, o_send, o_recv)
        )
        return pltpu.make_async_remote_copy(
            src_ref=slot(o) if forward else ref,
            dst_ref=slot(o),
            send_sem=send.at[1, o] if forward else send.at[0, target],
            recv_sem=recv.at[o],
            device_id={"dp": target},
            device_id_type=pl.DeviceIdType.MESH,
        )

    def rs_copy(s, c, up):
        return pltpu.make_async_remote_copy(
            src_ref=out_buf.at[s, rows_at(c)],
            dst_ref=(from_below if up else from_above).at[s, rows_at(c)],
            send_sem=rs_send.at[s, c],
            recv_sem=rs_recv.at[up, s, c],
            device_id={"mp": me + 2 * up - 1},
            device_id_type=pl.DeviceIdType.MESH,
        )

    def ss_copy(origin, c, target):
        return pltpu.make_async_remote_copy(
            src_ref=ss_mine.at[c],
            dst_ref=ss_all.at[origin, c],
            send_sem=ss_send.at[target, c],
            recv_sem=ss_recv.at[origin, c],
            device_id={"mp": target},
            device_id_type=pl.DeviceIdType.MESH,
        )

    def loop(count, body, start=0):
        def wrapped(i, carry):
            body(i)
            return carry

        lax.fori_loop(start, count, wrapped, 0)

    def local_copies():
        return (
            pltpu.make_async_copy(win, w_slot(d), local_sem.at[0]),
            pltpu.make_async_copy(wout, o_slot(d), local_sem.at[1]),
            pltpu.make_async_copy(tok, x_all.at[me], local_sem.at[2]),
            pltpu.make_async_copy(pre, gain_all.at[feats_at(me)], local_sem.at[3]),
            pltpu.make_async_copy(bias, bias_v, local_sem.at[4]),
        )

    for copy in local_copies():
        copy.start()

    barrier = pltpu.get_barrier_semaphore()

    def greet_mp(k):
        pl.semaphore_signal(
            barrier,
            inc=1,
            device_id={"mp": lax.rem(me + k, n)},
            device_id_type=pl.DeviceIdType.MESH,
        )

    def greet_dp(k):
        pl.semaphore_signal(
            barrier,
            inc=1,
            device_id={"dp": lax.rem(d + k, groups)},
            device_id_type=pl.DeviceIdType.MESH,
        )

    loop(n, greet_mp, 1)
    loop(groups, greet_dp, 1)
    pl.semaphore_wait(barrier, n - 1 + groups - 1)

    def peer_mp(k):
        return lax.rem(me + k, n)

    def same_core(k):
        return 2 * lax.rem(pair + k, half) + odd

    def from_core(k):
        return 2 * lax.rem(pair + half - k, half) + odd

    loop(n, lambda k: gain_copy(me, peer_mp(k)).start(), 1)
    def send_own(up):
        @pl.when((me < n - 1) if up else (me > 0))
        def _():
            @pl.when(odd == 1)
            def _():
                pl.semaphore_wait(link_free.at[up], 1)

            loop(chunks, lambda c: tok_copy(me, c, up, True).start())

    def release(up):
        s = 0 if up else n - 1

        @pl.when(((me < n - 1) if up else (me > 0)) & (odd == 0))
        def _():
            loop(chunks, lambda c: tok_copy(s, c, up, False).wait_send())
            pl.semaphore_signal(
                link_free.at[up],
                inc=1,
                device_id={"dp": partner},
                device_id_type=pl.DeviceIdType.MESH,
            )

    def send_both():
        @pl.when(2 * me < n)
        def _():
            send_own(1)
            send_own(0)

        @pl.when(2 * me >= n)
        def _():
            send_own(0)
            send_own(1)

    pl.when(odd == 0)(send_both)
    weight_copy(0, d, partner, False).start()
    loop(half, lambda k: weight_copy(0, d, same_core(k), False).start(), 1)
    weight_copy(1, d, partner, False).start()
    loop(half, lambda k: weight_copy(1, d, same_core(k), False).start(), 1)

    pl.when((odd == 0) & (me == 0))(lambda: release(1))
    pl.when((odd == 0) & (me == n - 1))(lambda: release(0))

    acc[...] = jnp.zeros_like(acc)
    square[...] = jnp.zeros_like(square)

    def take_shards(j):
        below, above = me - j, me + j

        def one(c):
            @pl.when(below >= 0)
            def _():
                tok_copy(below, c, 1, False).wait_recv()

                @pl.when(me < n - 1)
                def _():
                    tok_copy(below, c, 1, False).start()

            @pl.when(above < n)
            def _():
                tok_copy(above, c, 0, False).wait_recv()

                @pl.when(me > 0)
                def _():
                    tok_copy(above, c, 0, False).start()

        loop(chunks, one)
        pl.when((j == me))(lambda: release(1))
        pl.when((j == n - 1 - me))(lambda: release(0))

    def project(j):
        def side(up):
            s = me + (2 * up - 1) * j

            @pl.when((s >= 0) & (s < n) & ((j > 0) | (up == 0)))
            def _():
                block = feats_at(s)
                gain = gain_all[feats_at(s)].astype(F32).reshape(1, feats)

                x = x_all[s].astype(F32)
                square[...] += x * x
                xg = (x * gain).astype(BF16)
                for m in range(3):
                    acc[m] += jnp.dot(xg, w_all[m, block, :], preferred_element_type=F32)

        loop(2, side)

    def forward_weights(which):
        def forward(k):
            o = from_core(k)
            weight_copy(which, o, partner, False).wait_recv()
            weight_copy(which, o, partner, True).start()

        loop(half, forward, 1)

    def other_weights(which):
        loop(half, lambda k: weight_copy(which, 2 * k + 1 - odd, partner, False).wait_recv())

    @pl.when(odd == 1)
    def _():
        forward_weights(0)
        send_both()
        take_shards(1)
        forward_weights(1)

    @pl.when(odd == 0)
    def _():
        loop(n, take_shards, 1)
        forward_weights(0)

    for copy in local_copies():
        copy.wait()
    loop(n, lambda k: gain_copy(peer_mp(k), peer_mp(k)).wait_recv(), 1)
    other_weights(0)
    loop(2, project)

    def later(j):
        pl.when(odd == 1)(lambda: take_shards(j))
        project(j)

    loop(n, later, 2)
    pl.when(odd == 0)(lambda: forward_weights(1))
    other_weights(1)

    def finish(c):
        total = jnp.sum(square[rows_at(c), :], axis=1, keepdims=True)
        inverse = lax.rsqrt(total / model + epsilon)
        for m in range(3):
            qkv[m, rows_at(c), :] = (acc[m, rows_at(c), :] * inverse).astype(BF16)

    loop(chunks, finish)

    lane_head = lax.broadcasted_iota(jnp.int32, (1, inner), 1) // head_dim
    contract = (((1,), (1,)), ((), ()))

    def send_out(s, c, up, value):
        out_buf[s, rows_at(c), :] = value.astype(BF16)
        rs_copy(s, c, up).start()

    def attend(c):
        first = (c * step) // seq * seq
        keys_at = pl.ds(pl.multiple_of(first, seq), seq)
        bias_at = pl.ds(pl.multiple_of(c * step - first, step), step)
        q = qkv[0, rows_at(c), :]
        k = qkv[1, keys_at, :]
        v = qkv[2, keys_at, :]
        context = jnp.zeros((step, inner), F32)
        for h in range(heads):
            qh = jnp.where(lane_head == h, q, jnp.zeros_like(q))
            scores = lax.dot_general(qh, k, contract, preferred_element_type=F32)
            scores = scores + bias_v[h, bias_at, :].astype(F32)
            weights = jnp.exp(scores - jnp.max(scores, axis=1, keepdims=True))
            scale = 1.0 / jnp.sum(weights, axis=1, keepdims=True)
            mixed = jnp.dot(weights.astype(BF16), v, preferred_element_type=F32)
            context = jnp.where(lane_head == h, mixed * scale, context)
        context = context.astype(BF16)

        def share(s):
            block = feats_at(s)
            if wide:
                value = jnp.dot(context, wo_all[:, block], preferred_element_type=F32)
            else:
                value = lax.dot_general(
                    context, wo_all[block, :], contract, preferred_element_type=F32
                )
            part[s, rows_at(c), :] = value

        for s in range(n):
            share(s)

        @pl.when(me == 0)
        def _():
            loop(n - 1, lambda k: send_out(n - 1 - k, c, 1, part[n - 1 - k, rows_at(c), :]))

        @pl.when(me == n - 1)
        def _():
            loop(n - 1, lambda k: send_out(k, c, 0, part[k, rows_at(c), :]))

    loop(rows // step, attend)

    def finalize(c):
        own = x_all[me, rows_at(c), :].astype(F32) + part[me, rows_at(c), :]
        stream = own.astype(BF16)
        stream_o[rows_at(c), :] = stream
        wide_stream = stream.astype(F32)
        total = jnp.sum(wide_stream * wide_stream, axis=1, keepdims=True)
        turned = jnp.transpose(jnp.broadcast_to(total, (step, 128)))
        ss_mine[c] = turned[0:8, :]
        ss_all[me, c] = turned[0:8, :]
        loop(n, lambda k: ss_copy(me, c, peer_mp(k)).start(), 1)

    messages = chunks * (n - 1)

    def chain(t, up, lead):
        m = t - lead
        landed = from_below if up else from_above

        @pl.when((m >= 0) & (m < messages))
        def _():
            c, k = m // (n - 1), lax.rem(m, n - 1)
            s = n - 1 - k if up else k
            further = s > me if up else s < me

            @pl.when(further | (s == me))
            def _():
                rs_copy(s, c, up).wait_recv()
                value = part[s, rows_at(c), :] + landed[s, rows_at(c), :].astype(F32)

                @pl.when(s == me)
                def _():
                    part[s, rows_at(c), :] = value

                @pl.when(further)
                def _():
                    send_out(s, c, up, value)

    up_lead, down_lead = (me - 1) * lag, (n - 2 - me) * lag
    up_last, down_last = n - 1 - me + up_lead, me + down_lead
    last = jnp.where(
        me == 0, down_last, jnp.where(me == n - 1, up_last, jnp.maximum(up_last, down_last))
    )

    def tick(t):
        @pl.when(me > 0)
        def _():
            chain(t, 1, up_lead)

        @pl.when(me < n - 1)
        def _():
            chain(t, 0, down_lead)

        @pl.when((t >= last) & (lax.rem(t - last + n - 1, n - 1) == 0))
        def _():
            c = (t - last + n - 1) // (n - 1) - 1

            @pl.when(c < chunks)
            def _():
                finalize(c)

    loop(messages + (n - 2) * lag, tick)

    def normalize(c):
        loop(n, lambda k: ss_copy(peer_mp(k), c, peer_mp(k)).wait_recv(), 1)
        total = jnp.zeros((8, step), F32)
        for s in range(n):
            total = total + ss_all[s, c]
        square_o[c] = total

    loop(chunks, normalize)

    loop(n, lambda k: gain_copy(me, peer_mp(k)).wait_send(), 1)

    def drain_tokens(s):
        def one(c):
            @pl.when((s <= me) & (me < n - 1) & ((s > 0) | (odd == 1)))
            def _():
                tok_copy(s, c, 1, False).wait_send()

            @pl.when((s >= me) & (me > 0) & ((s < n - 1) | (odd == 1)))
            def _():
                tok_copy(s, c, 0, False).wait_send()

            @pl.when(s != me)
            def _():
                rs_copy(s, c, 1).wait_send()
                ss_copy(me, c, s).wait_send()

        loop(chunks, one)

    loop(n, drain_tokens)
    for which in range(2):
        weight_copy(which, d, partner, False).wait_send()

        def drain(k):
            weight_copy(which, d, same_core(k), False).wait_send()
            weight_copy(which, from_core(k), partner, True).wait_send()

        loop(half, drain, 1)


def post_norm(model, stream_i, square_i, gain_i, stream_o, normed_o, normed_v, sems):
    chunks, _, step = square_i.shape
    copies = [pltpu.make_async_copy(stream_i, stream_o, sems.at[0])]
    copies[0].start()
    gain = gain_i[...].astype(F32).reshape(1, stream_i.shape[1])
    for c in range(chunks):
        at = pl.ds(c * step, step)
        post = jnp.transpose(lax.rsqrt(square_i[c] / model + epsilon))[:, 0:1]
        normed_v[at, :] = (stream_i[at, :].astype(F32) * post * gain).astype(BF16)
        copies.append(pltpu.make_async_copy(normed_v.at[at], normed_o.at[at], sems.at[1 + c]))
        copies[-1].start()
    for copy in copies:
        copy.wait()


def on_device(n, groups, tokens, pre_gain, input_weight, output_weight, position_bias, post_gain):
    rows, feats = tokens.shape
    chunks, lag = rows // 256, 2
    step = rows // chunks
    inner = input_weight.shape[2]
    model = n * feats
    wide = output_weight.shape[1] % 128 == 0
    if not wide:
        output_weight = output_weight.T
    dma, any_space = pltpu.SemaphoreType.DMA, pl.BlockSpec(memory_space=pl.ANY)
    shape = jax.ShapeDtypeStruct((rows, feats), BF16)
    stream, squares = pl.pallas_call(
        functools.partial(kernel, n, groups, chunks, lag, wide),
        out_shape=(pltpu.VMEM((rows, feats), BF16), pltpu.VMEM((chunks, 8, step), F32)),
        in_specs=[any_space] * 5,
        out_specs=[pl.BlockSpec(memory_space=pltpu.VMEM)] * 2,
        scratch_shapes=[
            pltpu.VMEM((n, rows, feats), BF16),
            pltpu.VMEM((n * feats,), BF16),
            pltpu.VMEM((3, model, inner), BF16),
            pltpu.VMEM((inner, model) if wide else (model, inner), BF16),
            pltpu.VMEM(position_bias.shape, BF16),
            pltpu.VMEM((3, rows, inner), F32),
            pltpu.VMEM((rows, feats), F32),
            pltpu.VMEM((3, rows, inner), BF16),
            pltpu.VMEM((n, rows, feats), F32),
            pltpu.VMEM((n, rows, feats), BF16),
            pltpu.VMEM((n, rows, feats), BF16),
            pltpu.VMEM((n, rows, feats), BF16),
            pltpu.VMEM((chunks, 8, step), F32),
            pltpu.VMEM((n, chunks, 8, step), F32),
            dma((2, n, chunks)),
            dma((n, chunks)),
            dma((n,)),
            dma((n,)),
            dma((2, groups)),
            dma((groups,)),
            dma((2, groups)),
            dma((groups,)),
            dma((n, chunks)),
            dma((2, n, chunks)),
            dma((n, chunks)),
            dma((n, chunks)),
            dma((5,)),
            pltpu.SemaphoreType.REGULAR((2,)),
        ],
        compiler_params=pltpu.CompilerParams(
            collective_id=0, has_side_effects=True, vmem_limit_bytes=56 * 1024 * 1024
        ),
    )(tokens, pre_gain, input_weight, output_weight, position_bias)
    vmem = pl.BlockSpec(memory_space=pltpu.VMEM)
    return pl.pallas_call(
        functools.partial(post_norm, model),
        out_shape=(shape, shape),
        in_specs=[vmem] * 3,
        out_specs=[any_space] * 2,
        scratch_shapes=[pltpu.VMEM((rows, feats), BF16), dma((1 + chunks,))],
        compiler_params=pltpu.CompilerParams(vmem_limit_bytes=8 * 1024 * 1024),
    )(stream, squares, post_gain)


def solution(mesh):
    return jax.shard_map(
        functools.partial(on_device, mesh.shape["mp"], mesh.shape["dp"]),
        mesh=mesh,
        in_specs=(
            P("dp", "mp"),
            P("mp"),
            P(None, "dp", "mp"),
            P("mp", "dp"),
            P("mp", None, None),
            P("mp"),
        ),
        out_specs=(P("dp", "mp"), P("dp", "mp")),
        check_vma=False,
    )
```

```python
import functools

import jax
import jax.numpy as jnp
from jax import lax
from jax.experimental import pallas as pl
from jax.experimental.pallas import tpu as pltpu
from jax.sharding import PartitionSpec as P

epsilon = 1e-06
F32, BF16 = jnp.float32, jnp.bfloat16
MESH = pl.DeviceIdType.MESH


def kernel(
    n,
    groups,
    chunks,
    wide,
    tok,
    pre,
    win,
    wout,
    bias,
    post,
    stream_o,
    normed_o,
    x_all,
    gain_all,
    post_v,
    w_all,
    wo_all,
    wo_end,
    bias_v,
    acc,
    square,
    qkv,
    part,
    out_buf,
    landed,
    ctx_buf,
    ctx_in,
    ss_mine,
    ss_all,
    ag_send,
    ag_recv,
    g_send,
    g_recv,
    w_send,
    w_recv,
    ctx_send,
    ctx_recv,
    rs_send,
    rs_recv,
    ss_send,
    ss_recv,
    local_sem,
    link_free,
):
    rows, feats = tok.shape
    step = rows // chunks
    heads, seq = bias.shape[0], bias.shape[1]
    inner = win.shape[2]
    head_dim = inner // heads
    model = n * feats
    wrows = win.shape[1]
    wcols = model // groups
    half = groups // 2
    me = lax.axis_index("mp")
    d = lax.axis_index("dp")
    odd = lax.rem(d, 2)
    pair = d // 2
    partner = d + 1 - 2 * odd
    is_end = (me == 0) | (me == n - 1)
    is_edge = (me == 1) | (me == n - 2)
    all_rows = pl.ds(0, rows)

    def rows_at(c):
        return pl.ds(pl.multiple_of(c * step, step), step)

    def feats_at(s):
        return pl.ds(pl.multiple_of(s * feats, feats), feats)

    def loop(count, body, start=0):
        def wrapped(i, carry):
            body(i)
            return carry

        lax.fori_loop(start, count, wrapped, 0)

    def remote(src, dst, send, recv, target):
        return pltpu.make_async_remote_copy(
            src_ref=src,
            dst_ref=dst,
            send_sem=send,
            recv_sem=recv,
            device_id=target,
            device_id_type=MESH,
        )

    def tok_copy(s, c, up):
        ref = x_all.at[s, rows_at(c)]
        return remote(ref, ref, ag_send.at[up, s, c], ag_recv.at[s, c], {"mp": me + 2 * up - 1})

    def gain_copy(origin, target):
        ref = gain_all.at[feats_at(origin)]
        return remote(ref, ref, g_send.at[target], g_recv.at[origin], {"mp": target})

    def w_slot(o):
        return w_all.at[:, pl.ds(pl.multiple_of(o * wrows, wrows), wrows), :]

    def o_slot(ref, o):
        block = pl.ds(pl.multiple_of(o * wcols, wcols), wcols)
        return ref.at[:, block] if wide else ref.at[block, :]

    def slot(which, o):
        return w_slot(o) if which == 0 else o_slot(wo_all if which == 1 else wo_end, o)

    def weight_copy(which, o, target, forward):
        ref = slot(which, o)
        send = w_send.at[which, 1, o] if forward else w_send.at[which, 0, target]
        return remote(ref, ref, send, w_recv.at[which, o], {"dp": target})

    def cross_copy():
        inwards = jnp.where(me == 0, 1, n - 2)
        return remote(
            o_slot(wo_all, d), o_slot(wo_end, d), w_send.at[2, 0, d], w_recv.at[2, d], {"mp": inwards}
        )

    def ctx_copy(c):
        inwards = jnp.where(me == 0, 1, n - 2)
        return remote(
            ctx_buf.at[rows_at(c)], ctx_in.at[rows_at(c)], ctx_send.at[c], ctx_recv.at[c], {"mp": inwards}
        )

    def rs_copy(s, c, up):
        return remote(
            out_buf.at[s, rows_at(c)],
            landed.at[up, s, rows_at(c)],
            rs_send.at[s, c],
            rs_recv.at[up, s, c],
            {"mp": me + 2 * up - 1},
        )

    def ss_copy(origin, c, target):
        return remote(
            ss_mine.at[c], ss_all.at[origin, c], ss_send.at[target, c], ss_recv.at[origin, c], {"mp": target}
        )

    local = (
        pltpu.make_async_copy(tok, x_all.at[me], local_sem.at[0]),
        pltpu.make_async_copy(pre, gain_all.at[feats_at(me)], local_sem.at[1]),
        pltpu.make_async_copy(win, w_slot(d), local_sem.at[2]),
        pltpu.make_async_copy(wout, o_slot(wo_all, d), local_sem.at[3]),
        pltpu.make_async_copy(post, post_v, local_sem.at[4]),
        pltpu.make_async_copy(bias, bias_v, local_sem.at[5]),
    )
    for copy in local:
        copy.start()

    def peer_mp(k):
        return lax.rem(me + k, n)

    def same_core(k):
        return 2 * lax.rem(pair + k, half) + odd

    def from_core(k):
        return 2 * lax.rem(pair + half - k, half) + odd

    barrier = pltpu.get_barrier_semaphore()

    def greet(target):
        pl.semaphore_signal(barrier, inc=1, device_id=target, device_id_type=MESH)

    loop(n, lambda k: greet({"mp": peer_mp(k)}), 1)
    loop(half, lambda k: greet({"dp": same_core(k)}), 1)
    greet({"dp": partner})
    acc[...] = jnp.zeros_like(acc)
    square[...] = jnp.zeros_like(square)
    for copy in local[:5]:
        copy.wait()
    pl.semaphore_wait(barrier, n - 1 + half - 1 + 1)

    def can_send(up):
        return (me < n - 1) if up else (me > 0)

    def send_own(up):
        @pl.when(can_send(up))
        def _():
            @pl.when(odd == 1)
            def _():
                pl.semaphore_wait(link_free.at[up], 1)

            loop(chunks, lambda c: tok_copy(me, c, up).start())

    def release(up):
        @pl.when(can_send(up))
        def _():
            pl.semaphore_signal(
                link_free.at[up], inc=1, device_id={"dp": partner}, device_id_type=MESH
            )

    early = max(chunks - 2, 0)

    def send_weights(which):
        weight_copy(which, d, partner, False).start()
        loop(half, lambda k: weight_copy(which, d, same_core(k), False).start(), 1)

    def forward_weights(which):
        def forward(k):
            o = from_core(k)
            weight_copy(which, o, partner, False).wait_recv()
            weight_copy(which, o, partner, True).start()

        loop(half, forward, 1)

    def other_weights(which):
        loop(half, lambda k: weight_copy(which, 2 * k + 1 - odd, partner, False).wait_recv())

    def pass_end_weights():
        @pl.when(is_edge)
        def _():
            weight_copy(2, d, partner, False).wait_recv()
            send_weights(2)

    def take(up, j, use=None):
        s = me - j if up else me + j

        @pl.when((s >= 0) & (s < n))
        def _():
            def one(c):
                tok_copy(s, c, up).wait_recv()

                @pl.when(can_send(up))
                def _():
                    tok_copy(s, c, up).start()

                if use is not None:
                    use(s, c)

            loop(chunks, one)

    def accumulate(s, at):
        gain = gain_all[feats_at(s)].astype(F32).reshape(1, feats)
        x = x_all[s, at, :].astype(F32)
        square[at, :] += x * x
        xg = (x * gain).astype(BF16)
        for m in range(3):
            acc[m, at, :] += jnp.dot(xg, w_all[m, feats_at(s), :], preferred_element_type=F32)

    def gather_even():
        send_own(1)
        send_own(0)
        send_weights(0)
        pl.when(is_end)(lambda: cross_copy().start())
        pl.when(jnp.logical_not(is_end))(lambda: send_weights(1))

        @pl.when(me == 0)
        def _():
            loop(early, lambda c: tok_copy(me, c, 1).wait_send())
            release(1)

        @pl.when(me == n - 1)
        def _():
            loop(early, lambda c: tok_copy(me, c, 0).wait_send())
            release(0)

        def hop(j):
            def one(c):
                for up in (1, 0):
                    s = me - j if up else me + j

                    @pl.when((s >= 0) & (s < n))
                    def _():
                        tok_copy(s, c, up).wait_recv()
                        pl.when(can_send(up))(lambda: tok_copy(s, c, up).start())

            loop(chunks, one)
            pl.when(j == me)(lambda: release(1))
            pl.when(j == n - 1 - me)(lambda: release(0))

        loop(n, hop, 1)
        pass_end_weights()
        forward_weights(0)
        loop(n, lambda k: gain_copy(peer_mp(k), peer_mp(k)).wait_recv(), 1)
        other_weights(0)
        loop(n, lambda s: accumulate(s, all_rows))

    def gather_odd():
        send_weights(0)
        pl.when(is_end)(lambda: cross_copy().start())
        pl.when(jnp.logical_not(is_end))(lambda: send_weights(1))

        def toward(near):
            far = 1 - near
            send_own(near)
            loop(n, lambda j: take(near, j), 1)
            pass_end_weights()
            send_own(far)
            forward_weights(0)
            loop(n, lambda k: gain_copy(peer_mp(k), peer_mp(k)).wait_recv(), 1)
            take(far, 1)
            other_weights(0)

            def known(s):
                pl.when((s <= me + 1) if near else (s >= me - 1))(lambda: accumulate(s, all_rows))

            loop(n, known)

            def later(j):
                take(far, j)
                s = me + j if near else me - j
                pl.when((s >= 0) & (s < n))(lambda: accumulate(s, all_rows))

            loop(n, later, 2)

        pl.when(2 * me < n)(lambda: toward(1))
        pl.when(2 * me >= n)(lambda: toward(0))

    loop(n, lambda k: gain_copy(me, peer_mp(k)).start(), 1)
    pl.when(odd == 0)(gather_even)
    pl.when(odd == 1)(gather_odd)

    def finish(c):
        total = jnp.sum(square[rows_at(c), :], axis=1, keepdims=True)
        inverse = lax.rsqrt(total / model + epsilon)
        for m in range(3):
            qkv[m, rows_at(c), :] = (acc[m, rows_at(c), :] * inverse).astype(BF16)

    loop(chunks, finish)
    local[5].wait()

    lane_head = lax.broadcasted_iota(jnp.int32, (1, inner), 1) // head_dim
    contract = (((1,), (1,)), ((), ()))

    def attend(c):
        first = (c * step) // seq * seq
        keys_at = pl.ds(pl.multiple_of(first, seq), seq)
        bias_at = pl.ds(pl.multiple_of(c * step - first, step), step)
        q = qkv[0, rows_at(c), :]
        k = qkv[1, keys_at, :]
        v = qkv[2, keys_at, :]
        context = jnp.zeros((step, inner), F32)
        for h in range(heads):
            qh = jnp.where(lane_head == h, q, jnp.zeros_like(q))
            scores = lax.dot_general(qh, k, contract, preferred_element_type=F32)
            scores = scores + bias_v[h, bias_at, :].astype(F32)
            weights = jnp.exp(scores - jnp.max(scores, axis=1, keepdims=True))
            scale = 1.0 / jnp.sum(weights, axis=1, keepdims=True)
            mixed = jnp.dot(weights.astype(BF16), v, preferred_element_type=F32)
            context = jnp.where(lane_head == h, mixed * scale, context)
        ctx_buf[rows_at(c), :] = context.astype(BF16)
        pl.when(is_end)(lambda: ctx_copy(c).start())

    loop(chunks, attend)

    def project_out(context, ref, s):
        block = feats_at(s)
        if wide:
            return jnp.dot(context, ref[:, block], preferred_element_type=F32)
        return lax.dot_general(context, ref[block, :], contract, preferred_element_type=F32)

    def send_out(s, c, up, value):
        out_buf[s, rows_at(c), :] = value.astype(BF16)
        rs_copy(s, c, up).start()

    def own_share(s):
        part[s] = project_out(ctx_buf[...], wo_all, s)

    def originate(c):
        ctx_copy(c).wait_recv()
        context = ctx_in[rows_at(c), :]

        def far(k):
            s = jnp.where(me == 1, n - 1 - k, k)
            value = part[s, rows_at(c), :] + project_out(context, wo_end, s)
            send_out(s, c, jnp.where(me == 1, 1, 0), value)

        def near(k):
            s = jnp.where(me == 1, k, n - 2 + k)
            part[s, rows_at(c), :] += project_out(context, wo_end, s)

        loop(n - 2, far)
        loop(2, near)

    def finished(s, c):
        value = x_all[s, rows_at(c), :].astype(F32) + part[s, rows_at(c), :]
        stream = value.astype(BF16)
        wide_stream = stream.astype(F32)
        return stream, wide_stream * wide_stream

    def finalize(c):
        stream, squares = finished(me, c)
        stream_o[rows_at(c), :] = stream
        part[me, rows_at(c), :] = squares

        @pl.when(is_edge)
        def _():
            end, up = jnp.where(me == 1, 0, n - 1), jnp.where(me == 1, 0, 1)
            stream_end, squares_end = finished(end, c)
            out_buf[end, rows_at(c), :] = stream_end
            rs_copy(end, c, up).start()
            part[me, rows_at(c), :] += squares_end

        total = jnp.sum(part[me, rows_at(c), :], axis=1, keepdims=True)
        turned = jnp.transpose(jnp.broadcast_to(total, (step, 128)))
        ss_mine[c] = turned[0:8, :]
        ss_all[me, c] = turned[0:8, :]
        loop(n, lambda k: ss_copy(me, c, peer_mp(k)).start(), 1)

    def combine(c):
        def message(k):
            for up in (1, 0):
                s = n - 1 - k if up else k
                follows = (me >= 2) if up else (me <= n - 3)
                further = (s > me) if up else (s < me)
                last = (me == n - 2) if up else (me == 1)

                @pl.when(follows & (further | (s == me)))
                def _():
                    rs_copy(s, c, up).wait_recv()
                    value = part[s, rows_at(c), :] + landed[up, s, rows_at(c), :].astype(F32)

                    @pl.when((s == me) | last)
                    def _():
                        part[s, rows_at(c), :] = value

                    @pl.when((s != me) & jnp.logical_not(last))
                    def _():
                        send_out(s, c, up, value)

        loop(n - 2, message)
        finalize(c)

    @pl.when(jnp.logical_not(is_end))
    def _():
        forward_weights(1)
        pl.when(is_edge)(lambda: forward_weights(2))
        other_weights(1)
        pl.when(is_edge)(lambda: other_weights(2))
        loop(n, own_share)
        pl.when(is_edge)(lambda: loop(chunks, originate))
        loop(chunks, combine)

    gain = post_v[...].astype(F32).reshape(1, feats)

    def normalize(c):
        def arrived(s):
            pl.when(s != me)(lambda: ss_copy(s, c, s).wait_recv())

        loop(n - 1, arrived, 1)

        @pl.when(is_end)
        def _():
            up = jnp.where(me == 0, 0, 1)
            rs_copy(me, c, up).wait_recv()
            stream_o[rows_at(c), :] = landed[up, me, rows_at(c), :]

        total = jnp.zeros((8, step), F32)
        for s in range(1, n - 1):
            total = total + ss_all[s, c]
        scale = jnp.transpose(lax.rsqrt(total / model + epsilon))[:, 0:1]
        stream = stream_o[rows_at(c), :].astype(F32)
        normed_o[rows_at(c), :] = (stream * scale * gain).astype(BF16)

    loop(chunks, normalize)

    loop(n, lambda k: gain_copy(me, peer_mp(k)).wait_send(), 1)

    def drain_tokens(s):
        def one(c):
            waited = (odd == 0) & (s == me) & (c < early)

            @pl.when((s <= me) & (me < n - 1) & jnp.logical_not(waited & (me == 0)))
            def _():
                tok_copy(s, c, 1).wait_send()

            @pl.when((s >= me) & (me > 0) & jnp.logical_not(waited & (me == n - 1)))
            def _():
                tok_copy(s, c, 0).wait_send()

            @pl.when(jnp.logical_not(is_end) & (s != me))
            def _():
                rs_copy(s, c, 1).wait_send()
                ss_copy(me, c, s).wait_send()

        loop(chunks, one)

    loop(n, drain_tokens)

    def drain_weights(which):
        weight_copy(which, d, partner, False).wait_send()

        def drain(k):
            weight_copy(which, d, same_core(k), False).wait_send()
            weight_copy(which, from_core(k), partner, True).wait_send()

        loop(half, drain, 1)

    drain_weights(0)
    pl.when(is_edge)(lambda: drain_weights(2))

    @pl.when(is_end)
    def _():
        cross_copy().wait_send()
        loop(chunks, lambda c: ctx_copy(c).wait_send())

    pl.when(jnp.logical_not(is_end))(lambda: drain_weights(1))


def publish(stream_i, normed_i, stream_o, normed_o, sems):
    copies = (
        pltpu.make_async_copy(stream_i, stream_o, sems.at[0]),
        pltpu.make_async_copy(normed_i, normed_o, sems.at[1]),
    )
    for copy in copies:
        copy.start()
    for copy in copies:
        copy.wait()


def on_device(n, groups, tokens, pre_gain, input_weight, output_weight, position_bias, post_gain):
    rows, feats = tokens.shape
    step = 128
    chunks = rows // step
    inner = input_weight.shape[2]
    model = n * feats
    wide = output_weight.shape[1] % 128 == 0
    if not wide:
        output_weight = output_weight.T
    dma, any_space = pltpu.SemaphoreType.DMA, pl.BlockSpec(memory_space=pl.ANY)
    vmem = pl.BlockSpec(memory_space=pltpu.VMEM)
    wo_shape = (inner, model) if wide else (model, inner)
    stream, normed = pl.pallas_call(
        functools.partial(kernel, n, groups, chunks, wide),
        out_shape=(pltpu.VMEM((rows, feats), BF16), pltpu.VMEM((rows, feats), BF16)),
        in_specs=[any_space] * 6,
        out_specs=[vmem] * 2,
        scratch_shapes=[
            pltpu.VMEM((n, rows, feats), BF16),
            pltpu.VMEM((n * feats,), BF16),
            pltpu.VMEM((feats,), BF16),
            pltpu.VMEM((3, model, inner), BF16),
            pltpu.VMEM(wo_shape, BF16),
            pltpu.VMEM(wo_shape, BF16),
            pltpu.VMEM(position_bias.shape, BF16),
            pltpu.VMEM((3, rows, inner), F32),
            pltpu.VMEM((rows, feats), F32),
            pltpu.VMEM((3, rows, inner), BF16),
            pltpu.VMEM((n, rows, feats), F32),
            pltpu.VMEM((n, rows, feats), BF16),
            pltpu.VMEM((2, n, rows, feats), BF16),
            pltpu.VMEM((rows, inner), BF16),
            pltpu.VMEM((rows, inner), BF16),
            pltpu.VMEM((chunks, 8, step), F32),
            pltpu.VMEM((n, chunks, 8, step), F32),
            dma((2, n, chunks)),
            dma((n, chunks)),
            dma((n,)),
            dma((n,)),
            dma((3, 2, groups)),
            dma((3, groups)),
            dma((chunks,)),
            dma((chunks,)),
            dma((n, chunks)),
            dma((2, n, chunks)),
            dma((n, chunks)),
            dma((n, chunks)),
            dma((6,)),
            pltpu.SemaphoreType.REGULAR((2,)),
        ],
        compiler_params=pltpu.CompilerParams(
            collective_id=0, has_side_effects=True, vmem_limit_bytes=56 * 1024 * 1024
        ),
    )(tokens, pre_gain, input_weight, output_weight, position_bias, post_gain)
    shape = jax.ShapeDtypeStruct((rows, feats), BF16)
    return pl.pallas_call(
        publish,
        out_shape=(shape, shape),
        in_specs=[vmem] * 2,
        out_specs=[any_space] * 2,
        scratch_shapes=[dma((2,))],
        compiler_params=pltpu.CompilerParams(vmem_limit_bytes=4 * 1024 * 1024),
    )(stream, normed)


def solution(mesh):
    return jax.shard_map(
        functools.partial(on_device, mesh.shape["mp"], mesh.shape["dp"]),
        mesh=mesh,
        in_specs=(
            P("dp", "mp"),
            P("mp"),
            P(None, "dp", "mp"),
            P("mp", "dp"),
            P("mp", None, None),
            P("mp"),
        ),
        out_specs=(P("dp", "mp"), P("dp", "mp")),
        check_vma=False,
    )
```

```python
import functools

import jax
import jax.numpy as jnp
from jax import lax
from jax.experimental import pallas as pl
from jax.experimental.pallas import tpu as pltpu
from jax.sharding import PartitionSpec as P

epsilon = 1e-06
F32, BF16 = jnp.float32, jnp.bfloat16
MESH = pl.DeviceIdType.MESH


def kernel(
    n,
    groups,
    chunks,
    wide,
    tok,
    pre,
    win,
    wout,
    bias,
    post,
    stream_o,
    normed_o,
    x_all,
    gain_all,
    post_v,
    w_all,
    wo_all,
    wo_end,
    bias_v,
    acc,
    square,
    qkv,
    part,
    out_buf,
    landed,
    ctx_buf,
    ctx_in,
    ss_mine,
    ss_all,
    ag_send,
    ag_recv,
    g_send,
    g_recv,
    w_send,
    w_recv,
    ctx_send,
    ctx_recv,
    rs_send,
    rs_recv,
    ss_send,
    ss_recv,
    local_sem,
    link_free,
):
    rows, feats = tok.shape
    step = rows // chunks
    heads, seq = bias.shape[0], bias.shape[1]
    inner = win.shape[2]
    head_dim = inner // heads
    model = n * feats
    wrows = win.shape[1]
    wcols = model // groups
    half = groups // 2
    me = lax.axis_index("mp")
    d = lax.axis_index("dp")
    odd = lax.rem(d, 2)
    pair = d // 2
    partner = d + 1 - 2 * odd
    is_end = (me == 0) | (me == n - 1)
    is_edge = (me == 1) | (me == n - 2)
    all_rows = pl.ds(0, rows)

    def rows_at(c):
        return pl.ds(pl.multiple_of(c * step, step), step)

    def feats_at(s):
        return pl.ds(pl.multiple_of(s * feats, feats), feats)

    def loop(count, body, start=0):
        def wrapped(i, carry):
            body(i)
            return carry

        lax.fori_loop(start, count, wrapped, 0)

    def remote(src, dst, send, recv, target):
        return pltpu.make_async_remote_copy(
            src_ref=src,
            dst_ref=dst,
            send_sem=send,
            recv_sem=recv,
            device_id=target,
            device_id_type=MESH,
        )

    def tok_copy(s, c, up):
        ref = x_all.at[s, rows_at(c)]
        return remote(ref, ref, ag_send.at[up, s, c], ag_recv.at[s, c], {"mp": me + 2 * up - 1})

    def gain_copy(origin, target):
        ref = gain_all.at[feats_at(origin)]
        return remote(ref, ref, g_send.at[target], g_recv.at[origin], {"mp": target})

    def w_slot(o):
        return w_all.at[:, pl.ds(pl.multiple_of(o * wrows, wrows), wrows), :]

    def o_slot(ref, o):
        block = pl.ds(pl.multiple_of(o * wcols, wcols), wcols)
        return ref.at[:, block] if wide else ref.at[block, :]

    def slot(which, o):
        return w_slot(o) if which == 0 else o_slot(wo_all if which == 1 else wo_end, o)

    def weight_copy(which, o, target, forward):
        ref = slot(which, o)
        send = w_send.at[which, 1, o] if forward else w_send.at[which, 0, target]
        return remote(ref, ref, send, w_recv.at[which, o], {"dp": target})

    def cross_copy():
        inwards = jnp.where(me == 0, 1, n - 2)
        return remote(
            o_slot(wo_all, d), o_slot(wo_end, d), w_send.at[2, 0, d], w_recv.at[2, d], {"mp": inwards}
        )

    def ctx_copy(c):
        inwards = jnp.where(me == 0, 1, n - 2)
        return remote(
            ctx_buf.at[rows_at(c)], ctx_in.at[rows_at(c)], ctx_send.at[c], ctx_recv.at[c], {"mp": inwards}
        )

    def rs_copy(s, c, up):
        return remote(
            out_buf.at[s, rows_at(c)],
            landed.at[up, s, rows_at(c)],
            rs_send.at[s, c],
            rs_recv.at[up, s, c],
            {"mp": me + 2 * up - 1},
        )

    def ss_copy(origin, c, target):
        return remote(
            ss_mine.at[c], ss_all.at[origin, c], ss_send.at[target, c], ss_recv.at[origin, c], {"mp": target}
        )

    local = (
        pltpu.make_async_copy(tok, x_all.at[me], local_sem.at[0]),
        pltpu.make_async_copy(pre, gain_all.at[feats_at(me)], local_sem.at[1]),
        pltpu.make_async_copy(win, w_slot(d), local_sem.at[2]),
        pltpu.make_async_copy(wout, o_slot(wo_all, d), local_sem.at[3]),
        pltpu.make_async_copy(post, post_v, local_sem.at[4]),
        pltpu.make_async_copy(bias, bias_v, local_sem.at[5]),
    )
    for copy in local:
        copy.start()

    def peer_mp(k):
        return lax.rem(me + k, n)

    def same_core(k):
        return 2 * lax.rem(pair + k, half) + odd

    def from_core(k):
        return 2 * lax.rem(pair + half - k, half) + odd

    barrier = pltpu.get_barrier_semaphore()

    def greet(target):
        pl.semaphore_signal(barrier, inc=1, device_id=target, device_id_type=MESH)

    loop(n, lambda k: greet({"mp": peer_mp(k)}), 1)
    loop(half, lambda k: greet({"dp": same_core(k)}), 1)
    greet({"dp": partner})
    acc[...] = jnp.zeros_like(acc)
    square[...] = jnp.zeros_like(square)
    for copy in local[:5]:
        copy.wait()
    pl.semaphore_wait(barrier, n - 1 + half - 1 + 1)

    def can_send(up):
        return (me < n - 1) if up else (me > 0)

    def send_own(up):
        @pl.when(can_send(up))
        def _():
            @pl.when(odd == 1)
            def _():
                pl.semaphore_wait(link_free.at[up], 1)

            loop(chunks, lambda c: tok_copy(me, c, up).start())

    def release(up):
        @pl.when(can_send(up))
        def _():
            pl.semaphore_signal(
                link_free.at[up], inc=1, device_id={"dp": partner}, device_id_type=MESH
            )

    def send_weights(which):
        weight_copy(which, d, partner, False).start()
        loop(half, lambda k: weight_copy(which, d, same_core(k), False).start(), 1)

    def forward_weights(which):
        def forward(k):
            o = from_core(k)
            weight_copy(which, o, partner, False).wait_recv()
            weight_copy(which, o, partner, True).start()

        loop(half, forward, 1)

    def other_weights(which):
        loop(half, lambda k: weight_copy(which, 2 * k + 1 - odd, partner, False).wait_recv())

    def pass_end_weights():
        @pl.when(is_edge)
        def _():
            weight_copy(2, d, partner, False).wait_recv()
            send_weights(2)

    def forward_out_weights():
        pl.when(jnp.logical_not(is_end))(lambda: forward_weights(1))
        pl.when(is_edge)(lambda: forward_weights(2))

    def take(up, j, use=None):
        s = me - j if up else me + j

        @pl.when((s >= 0) & (s < n))
        def _():
            def one(c):
                tok_copy(s, c, up).wait_recv()

                @pl.when(can_send(up))
                def _():
                    tok_copy(s, c, up).start()

                if use is not None:
                    use(s, c)

            loop(chunks, one)

    def accumulate(s, at):
        gain = gain_all[feats_at(s)].astype(F32).reshape(1, feats)
        x = x_all[s, at, :].astype(F32)
        square[at, :] += x * x
        xg = (x * gain).astype(BF16)
        for m in range(3):
            acc[m, at, :] += jnp.dot(xg, w_all[m, feats_at(s), :], preferred_element_type=F32)

    def both_ways(action):
        @pl.when(2 * me < n)
        def _():
            action(0)
            action(1)

        @pl.when(2 * me >= n)
        def _():
            action(1)
            action(0)

    def finish(c):
        total = jnp.sum(square[rows_at(c), :], axis=1, keepdims=True)
        inverse = lax.rsqrt(total / model + epsilon)
        for m in range(3):
            qkv[m, rows_at(c), :] = (acc[m, rows_at(c), :] * inverse).astype(BF16)

    def send_all_weights():
        send_weights(0)
        pl.when(is_end)(lambda: cross_copy().start())
        pl.when(jnp.logical_not(is_end))(lambda: send_weights(1))

    def wait_gains():
        loop(n, lambda k: gain_copy(peer_mp(k), peer_mp(k)).wait_recv(), 1)

    def gather_even():
        both_ways(send_own)
        send_all_weights()

        @pl.when(is_end)
        def _():
            up = jnp.where(me == 0, 1, 0)
            loop(chunks, lambda c: tok_copy(me, c, up).wait_send())
            both_ways(release)

        def hop(j):
            def one(c):
                def side(up):
                    s = me - j if up else me + j

                    @pl.when((s >= 0) & (s < n))
                    def _():
                        tok_copy(s, c, up).wait_recv()
                        pl.when(can_send(up))(lambda: tok_copy(s, c, up).start())

                both_ways(side)

            loop(chunks, one)

        loop(n, hop, 1)
        pl.when(jnp.logical_not(is_end))(lambda: both_ways(release))
        pass_end_weights()
        forward_weights(0)
        wait_gains()
        other_weights(0)
        loop(n, lambda s: accumulate(s, all_rows))
        loop(chunks, finish)

    def gather_odd():
        send_all_weights()
        both_ways(send_own)

        def toward(near):
            far = 1 - near
            reach = n - 1 - me if near else me
            loop(n, lambda j: take(near, j), 1)
            pass_end_weights()
            forward_weights(0)
            wait_gains()
            take(far, 1)
            other_weights(0)

            def known(s):
                pl.when((s <= me + 1) if near else (s >= me - 1))(lambda: accumulate(s, all_rows))

            loop(n, known)

            def later(j):
                @pl.when(j < reach)
                def _():
                    take(far, j)
                    accumulate(me + j if near else me - j, all_rows)

            def use(s, c):
                accumulate(s, rows_at(c))
                finish(c)

            loop(n, later, 2)
            pl.when(reach > 1)(lambda: take(far, reach, use))
            pl.when(reach <= 1)(lambda: loop(chunks, finish))

        pl.when(2 * me < n)(lambda: toward(1))
        pl.when(2 * me >= n)(lambda: toward(0))
        forward_out_weights()

    loop(n, lambda k: gain_copy(me, peer_mp(k)).start(), 1)
    pl.when(odd == 0)(gather_even)
    pl.when(odd == 1)(gather_odd)

    local[5].wait()

    lane_head = lax.broadcasted_iota(jnp.int32, (1, inner), 1) // head_dim
    contract = (((1,), (1,)), ((), ()))

    def attend(c):
        first = (c * step) // seq * seq
        keys_at = pl.ds(pl.multiple_of(first, seq), seq)
        bias_at = pl.ds(pl.multiple_of(c * step - first, step), step)
        q = qkv[0, rows_at(c), :]
        k = qkv[1, keys_at, :]
        v = qkv[2, keys_at, :]
        stacked = jnp.concatenate([jnp.where(lane_head == h, q, jnp.zeros_like(q)) for h in range(heads)], axis=0)
        scores = lax.dot_general(stacked, k, contract, preferred_element_type=F32)
        scores = scores + bias_v[:, bias_at, :].reshape(heads * step, seq).astype(F32)
        weights = jnp.exp(scores - jnp.max(scores, axis=1, keepdims=True))
        scale = 1.0 / jnp.sum(weights, axis=1, keepdims=True)
        mixed = jnp.dot(weights.astype(BF16), v, preferred_element_type=F32) * scale
        context = mixed[0:step]
        for h in range(1, heads):
            context = jnp.where(lane_head == h, mixed[h * step : (h + 1) * step], context)
        ctx_buf[rows_at(c), :] = context.astype(BF16)
        pl.when(is_end)(lambda: ctx_copy(c).start())

    loop(chunks, attend)

    def project_out(context, ref, s):
        block = feats_at(s)
        if wide:
            return jnp.dot(context, ref[:, block], preferred_element_type=F32)
        return lax.dot_general(context, ref[block, :], contract, preferred_element_type=F32)

    def send_out(s, c, up, value):
        out_buf[s, rows_at(c), :] = value.astype(BF16)
        rs_copy(s, c, up).start()

    def own_share(s):
        part[s] = project_out(ctx_buf[...], wo_all, s)

    def originate(c):
        ctx_copy(c).wait_recv()
        context = ctx_in[rows_at(c), :]

        def far(k):
            s = jnp.where(me == 1, n - 1 - k, k)
            value = part[s, rows_at(c), :] + project_out(context, wo_end, s)
            send_out(s, c, jnp.where(me == 1, 1, 0), value)

        def near(k):
            s = jnp.where(me == 1, k, n - 2 + k)
            part[s, rows_at(c), :] += project_out(context, wo_end, s)

        loop(n - 2, far)
        loop(2, near)

    def finished(s, c):
        value = x_all[s, rows_at(c), :].astype(F32) + part[s, rows_at(c), :]
        stream = value.astype(BF16)
        wide_stream = stream.astype(F32)
        return stream, wide_stream * wide_stream

    def finalize(c):
        stream, squares = finished(me, c)
        stream_o[rows_at(c), :] = stream
        part[me, rows_at(c), :] = squares

        @pl.when(is_edge)
        def _():
            end, up = jnp.where(me == 1, 0, n - 1), jnp.where(me == 1, 0, 1)
            stream_end, squares_end = finished(end, c)
            out_buf[end, rows_at(c), :] = stream_end
            rs_copy(end, c, up).start()
            part[me, rows_at(c), :] += squares_end

        total = jnp.sum(part[me, rows_at(c), :], axis=1, keepdims=True)
        turned = jnp.transpose(jnp.broadcast_to(total, (step, 128)))
        ss_mine[c] = turned[0:8, :]
        ss_all[me, c] = turned[0:8, :]
        loop(n, lambda k: ss_copy(me, c, peer_mp(k)).start(), 1)

    def combine(c):
        def message(k):
            for up in (1, 0):
                s = n - 1 - k if up else k
                follows = (me >= 2) if up else (me <= n - 3)
                further = (s > me) if up else (s < me)
                last = (me == n - 2) if up else (me == 1)

                @pl.when(follows & (further | (s == me)))
                def _():
                    rs_copy(s, c, up).wait_recv()
                    value = part[s, rows_at(c), :] + landed[up, s, rows_at(c), :].astype(F32)

                    @pl.when((s == me) | last)
                    def _():
                        part[s, rows_at(c), :] = value

                    @pl.when((s != me) & jnp.logical_not(last))
                    def _():
                        send_out(s, c, up, value)

        loop(n - 2, message)
        finalize(c)

    @pl.when(jnp.logical_not(is_end))
    def _():
        pl.when(odd == 0)(forward_out_weights)
        other_weights(1)
        pl.when(is_edge)(lambda: other_weights(2))
        loop(n, own_share)
        pl.when(is_edge)(lambda: loop(chunks, originate))
        loop(chunks, combine)

    gain = post_v[...].astype(F32).reshape(1, feats)

    def normalize(c):
        def arrived(s):
            pl.when(s != me)(lambda: ss_copy(s, c, s).wait_recv())

        loop(n - 1, arrived, 1)

        @pl.when(is_end)
        def _():
            up = jnp.where(me == 0, 0, 1)
            rs_copy(me, c, up).wait_recv()
            stream_o[rows_at(c), :] = landed[up, me, rows_at(c), :]

        total = jnp.zeros((8, step), F32)
        for s in range(1, n - 1):
            total = total + ss_all[s, c]
        scale = jnp.transpose(lax.rsqrt(total / model + epsilon))[:, 0:1]
        stream = stream_o[rows_at(c), :].astype(F32)
        normed_o[rows_at(c), :] = (stream * scale * gain).astype(BF16)

    loop(chunks, normalize)

    loop(n, lambda k: gain_copy(me, peer_mp(k)).wait_send(), 1)

    def drain_tokens(s):
        def one(c):
            waited = (odd == 0) & (s == me) & is_end

            @pl.when((s <= me) & (me < n - 1) & jnp.logical_not(waited))
            def _():
                tok_copy(s, c, 1).wait_send()

            @pl.when((s >= me) & (me > 0) & jnp.logical_not(waited))
            def _():
                tok_copy(s, c, 0).wait_send()

            @pl.when(jnp.logical_not(is_end) & (s != me))
            def _():
                rs_copy(s, c, 1).wait_send()
                ss_copy(me, c, s).wait_send()

        loop(chunks, one)

    loop(n, drain_tokens)

    def drain_weights(which):
        weight_copy(which, d, partner, False).wait_send()

        def drain(k):
            weight_copy(which, d, same_core(k), False).wait_send()
            weight_copy(which, from_core(k), partner, True).wait_send()

        loop(half, drain, 1)

    drain_weights(0)
    pl.when(is_edge)(lambda: drain_weights(2))

    @pl.when(is_end)
    def _():
        cross_copy().wait_send()
        loop(chunks, lambda c: ctx_copy(c).wait_send())

    pl.when(jnp.logical_not(is_end))(lambda: drain_weights(1))


def publish(stream_i, normed_i, stream_o, normed_o, sems):
    copies = (
        pltpu.make_async_copy(stream_i, stream_o, sems.at[0]),
        pltpu.make_async_copy(normed_i, normed_o, sems.at[1]),
    )
    for copy in copies:
        copy.start()
    for copy in copies:
        copy.wait()


def on_device(n, groups, tokens, pre_gain, input_weight, output_weight, position_bias, post_gain):
    rows, feats = tokens.shape
    step = 128
    chunks = rows // step
    inner = input_weight.shape[2]
    model = n * feats
    wide = output_weight.shape[1] % 128 == 0
    if not wide:
        output_weight = output_weight.T
    dma, any_space = pltpu.SemaphoreType.DMA, pl.BlockSpec(memory_space=pl.ANY)
    vmem = pl.BlockSpec(memory_space=pltpu.VMEM)
    wo_shape = (inner, model) if wide else (model, inner)
    stream, normed = pl.pallas_call(
        functools.partial(kernel, n, groups, chunks, wide),
        out_shape=(pltpu.VMEM((rows, feats), BF16), pltpu.VMEM((rows, feats), BF16)),
        in_specs=[any_space] * 6,
        out_specs=[vmem] * 2,
        scratch_shapes=[
            pltpu.VMEM((n, rows, feats), BF16),
            pltpu.VMEM((n * feats,), BF16),
            pltpu.VMEM((feats,), BF16),
            pltpu.VMEM((3, model, inner), BF16),
            pltpu.VMEM(wo_shape, BF16),
            pltpu.VMEM(wo_shape, BF16),
            pltpu.VMEM(position_bias.shape, BF16),
            pltpu.VMEM((3, rows, inner), F32),
            pltpu.VMEM((rows, feats), F32),
            pltpu.VMEM((3, rows, inner), BF16),
            pltpu.VMEM((n, rows, feats), F32),
            pltpu.VMEM((n, rows, feats), BF16),
            pltpu.VMEM((2, n, rows, feats), BF16),
            pltpu.VMEM((rows, inner), BF16),
            pltpu.VMEM((rows, inner), BF16),
            pltpu.VMEM((chunks, 8, step), F32),
            pltpu.VMEM((n, chunks, 8, step), F32),
            dma((2, n, chunks)),
            dma((n, chunks)),
            dma((n,)),
            dma((n,)),
            dma((3, 2, groups)),
            dma((3, groups)),
            dma((chunks,)),
            dma((chunks,)),
            dma((n, chunks)),
            dma((2, n, chunks)),
            dma((n, chunks)),
            dma((n, chunks)),
            dma((6,)),
            pltpu.SemaphoreType.REGULAR((2,)),
        ],
        compiler_params=pltpu.CompilerParams(
            collective_id=0, has_side_effects=True, vmem_limit_bytes=56 * 1024 * 1024
        ),
    )(tokens, pre_gain, input_weight, output_weight, position_bias, post_gain)
    shape = jax.ShapeDtypeStruct((rows, feats), BF16)
    return pl.pallas_call(
        publish,
        out_shape=(shape, shape),
        in_specs=[vmem] * 2,
        out_specs=[any_space] * 2,
        scratch_shapes=[dma((2,))],
        compiler_params=pltpu.CompilerParams(vmem_limit_bytes=4 * 1024 * 1024),
    )(stream, normed)


def solution(mesh):
    return jax.shard_map(
        functools.partial(on_device, mesh.shape["mp"], mesh.shape["dp"]),
        mesh=mesh,
        in_specs=(
            P("dp", "mp"),
            P("mp"),
            P(None, "dp", "mp"),
            P("mp", "dp"),
            P("mp", None, None),
            P("mp"),
        ),
        out_specs=(P("dp", "mp"), P("dp", "mp")),
        check_vma=False,
    )
```

```python
import functools

import jax
import jax.numpy as jnp
from jax import lax
from jax.experimental import pallas as pl
from jax.experimental.pallas import tpu as pltpu
from jax.sharding import PartitionSpec as P

epsilon = 1e-06
F32, BF16 = jnp.float32, jnp.bfloat16
MESH = pl.DeviceIdType.MESH


def kernel(
    n,
    groups,
    chunks,
    wide,
    tok,
    pre,
    win,
    wout,
    bias,
    post,
    stream_o,
    normed_o,
    x_all,
    gain_all,
    post_v,
    w_all,
    wo_all,
    wo_end,
    bias_v,
    acc,
    square,
    qkv,
    part,
    out_buf,
    landed,
    ctx_buf,
    ctx_in,
    ss_mine,
    ss_all,
    ag_send,
    ag_recv,
    g_send,
    g_recv,
    w_send,
    w_recv,
    ctx_send,
    ctx_recv,
    rs_send,
    rs_recv,
    ss_send,
    ss_recv,
    local_sem,
    link_free,
):
    rows, feats = tok.shape
    step = rows // chunks
    heads, seq = bias.shape[0], bias.shape[1]
    inner = win.shape[2]
    head_dim = inner // heads
    model = n * feats
    wrows = win.shape[1]
    wcols = model // groups
    half = groups // 2
    me = lax.axis_index("mp")
    d = lax.axis_index("dp")
    odd = lax.rem(d, 2)
    pair = d // 2
    partner = d + 1 - 2 * odd
    is_end = (me == 0) | (me == n - 1)
    is_edge = (me == 1) | (me == n - 2)
    all_rows = pl.ds(0, rows)

    def rows_at(c):
        return pl.ds(pl.multiple_of(c * step, step), step)

    def feats_at(s):
        return pl.ds(pl.multiple_of(s * feats, feats), feats)

    def loop(count, body, start=0):
        def wrapped(i, carry):
            body(i)
            return carry

        lax.fori_loop(start, count, wrapped, 0)

    def remote(src, dst, send, recv, target):
        return pltpu.make_async_remote_copy(
            src_ref=src,
            dst_ref=dst,
            send_sem=send,
            recv_sem=recv,
            device_id=target,
            device_id_type=MESH,
        )

    def tok_copy(s, c, up):
        ref = x_all.at[s, rows_at(c)]
        return remote(ref, ref, ag_send.at[up, s, c], ag_recv.at[s, c], {"mp": me + 2 * up - 1})

    def gain_copy(origin, target):
        ref = gain_all.at[feats_at(origin)]
        return remote(ref, ref, g_send.at[target], g_recv.at[origin], {"mp": target})

    def w_slot(o):
        return w_all.at[:, pl.ds(pl.multiple_of(o * wrows, wrows), wrows), :]

    def o_slot(ref, o):
        block = pl.ds(pl.multiple_of(o * wcols, wcols), wcols)
        return ref.at[:, block] if wide else ref.at[block, :]

    def slot(which, o):
        return w_slot(o) if which == 0 else o_slot(wo_all if which == 1 else wo_end, o)

    def weight_copy(which, o, target, forward):
        ref = slot(which, o)
        send = w_send.at[which, 1, o] if forward else w_send.at[which, 0, target]
        return remote(ref, ref, send, w_recv.at[which, o], {"dp": target})

    def cross_copy():
        inwards = jnp.where(me == 0, 1, n - 2)
        return remote(
            o_slot(wo_all, d), o_slot(wo_end, d), w_send.at[2, 0, d], w_recv.at[2, d], {"mp": inwards}
        )

    def ctx_copy(c):
        inwards = jnp.where(me == 0, 1, n - 2)
        return remote(
            ctx_buf.at[rows_at(c)], ctx_in.at[rows_at(c)], ctx_send.at[c], ctx_recv.at[c], {"mp": inwards}
        )

    def rs_copy(s, c, up):
        return remote(
            out_buf.at[s, rows_at(c)],
            landed.at[up, s, rows_at(c)],
            rs_send.at[s, c],
            rs_recv.at[up, s, c],
            {"mp": me + 2 * up - 1},
        )

    def ss_copy(origin, c, target):
        return remote(
            ss_mine.at[c], ss_all.at[origin, c], ss_send.at[target, c], ss_recv.at[origin, c], {"mp": target}
        )

    local = (
        pltpu.make_async_copy(tok, x_all.at[me], local_sem.at[0]),
        pltpu.make_async_copy(pre, gain_all.at[feats_at(me)], local_sem.at[1]),
        pltpu.make_async_copy(win, w_slot(d), local_sem.at[2]),
        pltpu.make_async_copy(wout, o_slot(wo_all, d), local_sem.at[3]),
        pltpu.make_async_copy(post, post_v, local_sem.at[4]),
        pltpu.make_async_copy(bias, bias_v, local_sem.at[5]),
    )
    for copy in local:
        copy.start()

    def peer_mp(k):
        return lax.rem(me + k, n)

    def same_core(k):
        return 2 * lax.rem(pair + k, half) + odd

    def from_core(k):
        return 2 * lax.rem(pair + half - k, half) + odd

    barrier = pltpu.get_barrier_semaphore()

    def greet(target):
        pl.semaphore_signal(barrier, inc=1, device_id=target, device_id_type=MESH)

    loop(n, lambda k: greet({"mp": peer_mp(k)}), 1)
    loop(half, lambda k: greet({"dp": same_core(k)}), 1)
    greet({"dp": partner})
    acc[...] = jnp.zeros_like(acc)
    square[...] = jnp.zeros_like(square)
    for copy in local[:5]:
        copy.wait()
    pl.semaphore_wait(barrier, n - 1 + half - 1 + 1)

    def can_send(up):
        return (me < n - 1) if up else (me > 0)

    def send_own(up):
        @pl.when(can_send(up))
        def _():
            @pl.when(odd == 1)
            def _():
                pl.semaphore_wait(link_free.at[up], 1)

            loop(chunks, lambda c: tok_copy(me, c, up).start())

    def release(up):
        @pl.when(can_send(up))
        def _():
            pl.semaphore_signal(
                link_free.at[up], inc=1, device_id={"dp": partner}, device_id_type=MESH
            )

    def send_weights(which):
        weight_copy(which, d, partner, False).start()
        loop(half, lambda k: weight_copy(which, d, same_core(k), False).start(), 1)

    def forward_weights(which):
        def forward(k):
            o = from_core(k)
            weight_copy(which, o, partner, False).wait_recv()
            weight_copy(which, o, partner, True).start()

        loop(half, forward, 1)

    def other_weights(which):
        loop(half, lambda k: weight_copy(which, 2 * k + 1 - odd, partner, False).wait_recv())

    def pass_end_weights():
        @pl.when(is_edge)
        def _():
            weight_copy(2, d, partner, False).wait_recv()
            send_weights(2)

    def forward_out_weights():
        pl.when(jnp.logical_not(is_end))(lambda: forward_weights(1))
        pl.when(is_edge)(lambda: forward_weights(2))

    def take(up, j, use=None):
        s = me - j if up else me + j

        @pl.when((s >= 0) & (s < n))
        def _():
            def one(c):
                tok_copy(s, c, up).wait_recv()

                @pl.when(can_send(up))
                def _():
                    tok_copy(s, c, up).start()

                if use is not None:
                    use(s, c)

            loop(chunks, one)

    def accumulate(s, at):
        gain = gain_all[feats_at(s)].astype(F32).reshape(1, feats)
        x = x_all[s, at, :].astype(F32)
        square[at, :] += x * x
        xg = (x * gain).astype(BF16)
        for m in range(3):
            acc[m, at, :] += jnp.dot(xg, w_all[m, feats_at(s), :], preferred_element_type=F32)

    def both_ways(action):
        @pl.when(2 * me < n)
        def _():
            action(0)
            action(1)

        @pl.when(2 * me >= n)
        def _():
            action(1)
            action(0)

    def finish(c):
        total = jnp.sum(square[rows_at(c), :], axis=1, keepdims=True)
        inverse = lax.rsqrt(total / model + epsilon)
        for m in range(3):
            qkv[m, rows_at(c), :] = (acc[m, rows_at(c), :] * inverse).astype(BF16)

    def send_all_weights():
        send_weights(0)
        pl.when(is_end)(lambda: cross_copy().start())
        pl.when(jnp.logical_not(is_end))(lambda: send_weights(1))

    def wait_gains():
        loop(n, lambda k: gain_copy(peer_mp(k), peer_mp(k)).wait_recv(), 1)

    def gather_even():
        both_ways(send_own)
        send_all_weights()

        @pl.when(is_end)
        def _():
            up = jnp.where(me == 0, 1, 0)
            loop(chunks, lambda c: tok_copy(me, c, up).wait_send())
            both_ways(release)

        def hop(j):
            def one(c):
                def side(up):
                    s = me - j if up else me + j

                    @pl.when((s >= 0) & (s < n))
                    def _():
                        tok_copy(s, c, up).wait_recv()
                        pl.when(can_send(up))(lambda: tok_copy(s, c, up).start())

                both_ways(side)

            loop(chunks, one)

        loop(n, hop, 1)
        pl.when(jnp.logical_not(is_end))(lambda: both_ways(release))
        pass_end_weights()
        forward_weights(0)
        wait_gains()
        other_weights(0)
        loop(n, lambda s: accumulate(s, all_rows))
        loop(chunks, finish)

    def gather_odd():
        send_all_weights()
        both_ways(send_own)

        def toward(near):
            far = 1 - near
            reach = n - 1 - me if near else me
            loop(n, lambda j: take(near, j), 1)
            pass_end_weights()
            forward_weights(0)
            wait_gains()
            take(far, 1)
            other_weights(0)

            def known(s):
                pl.when((s <= me + 1) if near else (s >= me - 1))(lambda: accumulate(s, all_rows))

            loop(n, known)

            def later(j):
                @pl.when(j < reach)
                def _():
                    take(far, j)
                    accumulate(me + j if near else me - j, all_rows)

            def use(s, c):
                accumulate(s, rows_at(c))
                finish(c)

            loop(n, later, 2)
            pl.when(reach > 1)(lambda: take(far, reach, use))
            pl.when(reach <= 1)(lambda: loop(chunks, finish))

        pl.when(2 * me < n)(lambda: toward(1))
        pl.when(2 * me >= n)(lambda: toward(0))
        forward_out_weights()

    loop(n, lambda k: gain_copy(me, peer_mp(k)).start(), 1)
    pl.when(odd == 0)(gather_even)
    pl.when(odd == 1)(gather_odd)

    local[5].wait()

    lane_head = lax.broadcasted_iota(jnp.int32, (1, inner), 1) // head_dim
    contract = (((1,), (1,)), ((), ()))

    def attend(c):
        first = (c * step) // seq * seq
        keys_at = pl.ds(pl.multiple_of(first, seq), seq)
        bias_at = pl.ds(pl.multiple_of(c * step - first, step), step)
        q = qkv[0, rows_at(c), :]
        k = qkv[1, keys_at, :]
        v = qkv[2, keys_at, :]
        stacked = jnp.concatenate([jnp.where(lane_head == h, q, jnp.zeros_like(q)) for h in range(heads)], axis=0)
        scores = lax.dot_general(stacked, k, contract, preferred_element_type=F32)
        scores = scores + bias_v[:, bias_at, :].reshape(heads * step, seq).astype(F32)
        weights = jnp.exp(scores - jnp.max(scores, axis=1, keepdims=True))
        scale = 1.0 / jnp.sum(weights, axis=1, keepdims=True)
        mixed = jnp.dot(weights.astype(BF16), v, preferred_element_type=F32) * scale
        context = mixed[0:step]
        for h in range(1, heads):
            context = jnp.where(lane_head == h, mixed[h * step : (h + 1) * step], context)
        ctx_buf[rows_at(c), :] = context.astype(BF16)
        pl.when(is_end)(lambda: ctx_copy(c).start())

    loop(chunks, attend)

    def project_out(context, ref, s):
        block = feats_at(s)
        if wide:
            return jnp.dot(context, ref[:, block], preferred_element_type=F32)
        return lax.dot_general(context, ref[block, :], contract, preferred_element_type=F32)

    def send_out(s, c, up, value):
        out_buf[s, rows_at(c), :] = value.astype(BF16)
        rs_copy(s, c, up).start()

    def own_share(s):
        part[s] = project_out(ctx_buf[...], wo_all, s)

    def originate(c):
        ctx_copy(c).wait_recv()
        context = ctx_in[rows_at(c), :]

        def far(k):
            s = jnp.where(me == 1, n - 1 - k, k)
            value = part[s, rows_at(c), :] + project_out(context, wo_end, s)
            send_out(s, c, jnp.where(me == 1, 1, 0), value)

        def near(k):
            s = jnp.where(me == 1, k, n - 2 + k)
            part[s, rows_at(c), :] += project_out(context, wo_end, s)

        loop(n - 2, far)
        loop(2, near)

    def finished(s, c):
        value = x_all[s, rows_at(c), :].astype(F32) + part[s, rows_at(c), :]
        stream = value.astype(BF16)
        wide_stream = stream.astype(F32)
        return stream, wide_stream * wide_stream

    def finalize(c):
        stream, squares = finished(me, c)
        stream_o[rows_at(c), :] = stream
        part[me, rows_at(c), :] = squares

        @pl.when(is_edge)
        def _():
            end, up = jnp.where(me == 1, 0, n - 1), jnp.where(me == 1, 0, 1)
            stream_end, squares_end = finished(end, c)
            out_buf[end, rows_at(c), :] = stream_end
            rs_copy(end, c, up).start()
            part[me, rows_at(c), :] += squares_end

        total = jnp.sum(part[me, rows_at(c), :], axis=1, keepdims=True)
        turned = jnp.transpose(jnp.broadcast_to(total, (step, 128)))
        ss_mine[c] = turned[0:8, :]
        ss_all[me, c] = turned[0:8, :]
        loop(n, lambda k: ss_copy(me, c, peer_mp(k)).start(), 1)

    def combine(c):
        def message(k):
            for up in (1, 0):
                s = n - 1 - k if up else k
                follows = (me >= 2) if up else (me <= n - 3)
                further = (s > me) if up else (s < me)
                last = (me == n - 2) if up else (me == 1)

                @pl.when(follows & (further | (s == me)))
                def _():
                    rs_copy(s, c, up).wait_recv()
                    value = part[s, rows_at(c), :] + landed[up, s, rows_at(c), :].astype(F32)

                    @pl.when((s == me) | last)
                    def _():
                        part[s, rows_at(c), :] = value

                    @pl.when((s != me) & jnp.logical_not(last))
                    def _():
                        send_out(s, c, up, value)

        loop(n - 2, message)
        finalize(c)

    @pl.when(jnp.logical_not(is_end))
    def _():
        pl.when(odd == 0)(forward_out_weights)
        other_weights(1)
        pl.when(is_edge)(lambda: other_weights(2))
        loop(n, own_share)
        pl.when(is_edge)(lambda: loop(chunks, originate))
        loop(chunks, combine)

    gain = post_v[...].astype(F32).reshape(1, feats)

    def normalize(c):
        def arrived(s):
            pl.when(s != me)(lambda: ss_copy(s, c, s).wait_recv())

        loop(n - 1, arrived, 1)

        @pl.when(is_end)
        def _():
            up = jnp.where(me == 0, 0, 1)
            rs_copy(me, c, up).wait_recv()
            stream_o[rows_at(c), :] = landed[up, me, rows_at(c), :]

        total = jnp.zeros((8, step), F32)
        for s in range(1, n - 1):
            total = total + ss_all[s, c]
        scale = jnp.transpose(lax.rsqrt(total / model + epsilon))[:, 0:1]
        stream = stream_o[rows_at(c), :].astype(F32)
        normed_o[rows_at(c), :] = (stream * scale * gain).astype(BF16)

    loop(chunks, normalize)

    loop(n, lambda k: gain_copy(me, peer_mp(k)).wait_send(), 1)

    def drain_tokens(s):
        def one(c):
            waited = (odd == 0) & (s == me) & is_end

            @pl.when((s <= me) & (me < n - 1) & jnp.logical_not(waited))
            def _():
                tok_copy(s, c, 1).wait_send()

            @pl.when((s >= me) & (me > 0) & jnp.logical_not(waited))
            def _():
                tok_copy(s, c, 0).wait_send()

            @pl.when(jnp.logical_not(is_end) & (s != me))
            def _():
                rs_copy(s, c, 1).wait_send()
                ss_copy(me, c, s).wait_send()

        loop(chunks, one)

    loop(n, drain_tokens)

    def drain_weights(which):
        weight_copy(which, d, partner, False).wait_send()

        def drain(k):
            weight_copy(which, d, same_core(k), False).wait_send()
            weight_copy(which, from_core(k), partner, True).wait_send()

        loop(half, drain, 1)

    drain_weights(0)
    pl.when(is_edge)(lambda: drain_weights(2))

    @pl.when(is_end)
    def _():
        cross_copy().wait_send()
        loop(chunks, lambda c: ctx_copy(c).wait_send())

    pl.when(jnp.logical_not(is_end))(lambda: drain_weights(1))


def line_kernel(
    n,
    groups,
    chunks,
    tok,
    pre,
    win,
    wout,
    bias,
    post,
    stream_o,
    normed_o,
    x_all,
    gain_all,
    post_v,
    w_all,
    wo_own,
    wo_all,
    bias_v,
    acc,
    square,
    qkv,
    ctx_all,
    part,
    out_buf,
    landed,
    ss_mine,
    ss_all,
    ag_send,
    ag_recv,
    g_send,
    g_recv,
    w_send,
    w_recv,
    x_send,
    o_send,
    o_recv,
    ctx_send,
    ctx_recv,
    end_send,
    end_recv,
    ss_send,
    ss_recv,
    local_sem,
    link_free,
):
    rows, feats = tok.shape
    step = rows // chunks
    pieces = ag_recv.shape[1]
    piece = rows // pieces
    heads, seq = bias.shape[0], bias.shape[1]
    inner = win.shape[2]
    head_dim = inner // heads
    model = n * feats
    wrows = win.shape[1]
    wcols = model // groups
    half = groups // 2
    me = lax.axis_index("mp")
    d = lax.axis_index("dp")
    odd = lax.rem(d, 2)
    pair = d // 2
    partner = d + 1 - 2 * odd
    low = 2 * me < n
    is_end = (me == 0) | (me == n - 1)
    is_inner = jnp.logical_not(is_end)
    near_end, far_end = jnp.where(low, 0, n - 1), jnp.where(low, n - 1, 0)
    other_inner = n - 1 - me
    inwards = me + jnp.where(low, 1, -1)
    home = jnp.where(d < half, 1, n - 2)
    is_source = me == home
    all_rows = pl.ds(0, rows)

    def rows_at(c):
        return pl.ds(pl.multiple_of(c * step, step), step)

    def feats_at(s):
        return pl.ds(pl.multiple_of(s * feats, feats), feats)

    def loop(count, body, start=0):
        def wrapped(i, carry):
            body(i)
            return carry

        lax.fori_loop(start, count, wrapped, 0)

    def remote(src, dst, send, recv, target):
        return pltpu.make_async_remote_copy(
            src_ref=src,
            dst_ref=dst,
            send_sem=send,
            recv_sem=recv,
            device_id=target,
            device_id_type=MESH,
        )

    def tok_copy(s, c, up):
        ref = x_all.at[s, pl.ds(pl.multiple_of(c * piece, piece), piece)]
        return remote(ref, ref, ag_send.at[up, s, c], ag_recv.at[s, c], {"mp": me + 2 * up - 1})

    def gain_copy(origin, target):
        ref = gain_all.at[feats_at(origin)]
        return remote(ref, ref, g_send.at[target], g_recv.at[origin], {"mp": target})

    def w_slot(o):
        return w_all.at[:, pl.ds(pl.multiple_of(o * wrows, wrows), wrows), :]

    def w_copy(o, target, forward):
        send = w_send.at[1, o] if forward else w_send.at[0, target]
        return remote(w_slot(o), w_slot(o), send, w_recv.at[o], {"dp": target})

    def o_slot(z, o):
        return wo_all.at[z, :, pl.ds(pl.multiple_of(lax.rem(o, half) * wcols, wcols), wcols)]

    def o_copy(z, o, target, forward):
        send = o_send.at[1, z, o] if forward else o_send.at[0, z, target]
        return remote(o_slot(z, o), o_slot(z, o), send, o_recv.at[z, o], {"dp": target})

    def cross_copy():
        return remote(wo_own, o_slot(me, d), x_send.at[0], o_recv.at[me, d], {"mp": home})

    def ctx_copy(s, c):
        ref = ctx_all.at[s, rows_at(c)]
        return remote(ref, ref, ctx_send.at[s, c], ctx_recv.at[s, c], {"mp": inwards})

    def end_copy(c):
        return remote(
            out_buf.at[rows_at(c)], landed.at[rows_at(c)], end_send.at[c], end_recv.at[c], {"mp": near_end}
        )

    def ss_copy(origin, c, target):
        return remote(
            ss_mine.at[c], ss_all.at[origin, c], ss_send.at[target, c], ss_recv.at[origin, c], {"mp": target}
        )

    tok_in = pltpu.make_async_copy(tok, x_all.at[me], local_sem.at[0])
    win_in = pltpu.make_async_copy(win, w_slot(d), local_sem.at[1])
    pre_in = pltpu.make_async_copy(pre, gain_all.at[feats_at(me)], local_sem.at[2])
    post_in = pltpu.make_async_copy(post, post_v, local_sem.at[3])
    bias_in = pltpu.make_async_copy(bias, bias_v, local_sem.at[4])

    def wout_in(action):
        pl.when(is_source)(lambda: action(pltpu.make_async_copy(wout, o_slot(me, d), local_sem.at[5])))
        pl.when(jnp.logical_not(is_source))(
            lambda: action(pltpu.make_async_copy(wout, wo_own, local_sem.at[5]))
        )

    tok_in.start()
    win_in.start()
    pre_in.start()
    wout_in(lambda copy: copy.start())
    post_in.start()
    bias_in.start()

    def peer_mp(k):
        return lax.rem(me + k, n)

    def same_core(k):
        return 2 * lax.rem(pair + k, half) + odd

    def from_core(k):
        return 2 * lax.rem(pair + half - k, half) + odd

    barrier = pltpu.get_barrier_semaphore()

    def greet(target):
        pl.semaphore_signal(barrier, inc=1, device_id=target, device_id_type=MESH)

    loop(n, lambda k: greet({"mp": peer_mp(k)}), 1)
    loop(half, lambda k: greet({"dp": same_core(k)}), 1)
    greet({"dp": partner})
    acc[...] = jnp.zeros_like(acc)
    square[...] = jnp.zeros_like(square)
    tok_in.wait()
    pl.semaphore_wait(barrier, n - 1 + half - 1 + 1)

    def can_send(up):
        return (me < n - 1) if up else (me > 0)

    def send_own(up):
        @pl.when(can_send(up))
        def _():
            @pl.when(odd == 1)
            def _():
                pl.semaphore_wait(link_free.at[up], 1)

            loop(pieces, lambda c: tok_copy(me, c, up).start())

    def release(up):
        @pl.when(can_send(up))
        def _():
            pl.semaphore_signal(
                link_free.at[up], inc=1, device_id={"dp": partner}, device_id_type=MESH
            )

    def both_ways(action):
        @pl.when(low)
        def _():
            action(0)
            action(1)

        @pl.when(jnp.logical_not(low))
        def _():
            action(1)
            action(0)

    def in_plane(o):
        return (o < half) == (me == 1)

    def send_slice(z):
        o_copy(z, d, partner, False).start()
        loop(half, lambda k: o_copy(z, d, same_core(k), False).start(), 1)

    def relay_slice(z):
        @pl.when(is_source)
        def _():
            o_copy(z, d, partner, False).wait_recv()
            send_slice(z)

    def forward_slices(z):
        def forward(k):
            o = from_core(k)

            @pl.when(in_plane(o))
            def _():
                o_copy(z, o, partner, False).wait_recv()
                o_copy(z, o, partner, True).start()

        loop(half, forward, 1)

    def other_slices(z):
        def other(k):
            o = 2 * k + 1 - odd
            pl.when(in_plane(o))(lambda: o_copy(z, o, partner, False).wait_recv())

        loop(half, other)

    def send_weights():
        win_in.wait()
        w_copy(d, partner, False).start()
        loop(half, lambda k: w_copy(d, same_core(k), False).start(), 1)
        pre_in.wait()
        loop(n, lambda k: gain_copy(me, peer_mp(k)).start(), 1)
        wout_in(lambda copy: copy.wait())
        pl.when(is_source)(lambda: send_slice(me))

    def send_cross():
        pl.when(jnp.logical_not(is_source))(lambda: cross_copy().start())

    def forward_weights():
        def forward(k):
            o = from_core(k)
            w_copy(o, partner, False).wait_recv()
            w_copy(o, partner, True).start()

        loop(half, forward, 1)
        loop(n, lambda k: gain_copy(peer_mp(k), peer_mp(k)).wait_recv(), 1)

    def other_weights():
        loop(half, lambda k: w_copy(2 * k + 1 - odd, partner, False).wait_recv())

    def take(up, j, use=None):
        s = me - j if up else me + j

        @pl.when((s >= 0) & (s < n))
        def _():
            def one(c):
                tok_copy(s, c, up).wait_recv()
                pl.when(can_send(up))(lambda: tok_copy(s, c, up).start())

            if use is None:
                loop(pieces, one)
            else:
                per = pieces // chunks

                def block(c):
                    loop(per, lambda i: one(c * per + i))
                    use(s, c)

                loop(chunks, block)

    def accumulate(s, at):
        gain = gain_all[feats_at(s)].astype(F32).reshape(1, feats)
        x = x_all[s, at, :].astype(F32)
        square[at, :] += x * x
        xg = (x * gain).astype(BF16)
        for m in range(3):
            acc[m, at, :] += jnp.dot(xg, w_all[m, feats_at(s), :], preferred_element_type=F32)

    def finish(c):
        total = jnp.sum(square[rows_at(c), :], axis=1, keepdims=True)
        inverse = lax.rsqrt(total / model + epsilon)
        for m in range(3):
            qkv[m, rows_at(c), :] = (acc[m, rows_at(c), :] * inverse).astype(BF16)

    def gather_by_shard(near):
        far = 1 - near
        reach = n - 1 - me if near else me
        loop(n, lambda j: take(near, j), 1)
        pl.when(odd == 1)(send_cross)
        forward_weights()
        relay_slice(near_end)
        relay_slice(far_end)
        take(far, 1)
        other_weights()

        def known(s):
            pl.when((s <= me + 1) if near else (s >= me - 1))(lambda: accumulate(s, all_rows))

        loop(n, known)

        def later(j):
            @pl.when(j < reach)
            def _():
                take(far, j)
                accumulate(me + j if near else me - j, all_rows)

        def use(s, c):
            accumulate(s, rows_at(c))
            finish(c)

        loop(n, later, 2)
        take(far, reach, use)
        relay_slice(other_inner)

    def by_shard():
        pl.when(low)(lambda: gather_by_shard(1))
        pl.when(jnp.logical_not(low))(lambda: gather_by_shard(0))

    def gather_even():
        both_ways(send_own)
        send_weights()

        @pl.when(is_end)
        def _():
            up = jnp.where(me == 0, 1, 0)
            loop(pieces, lambda c: tok_copy(me, c, up).wait_send())
            both_ways(release)
            send_cross()
            by_shard()

        def hop(j):
            def one(c):
                def side(up):
                    s = me - j if up else me + j

                    @pl.when((s >= 0) & (s < n))
                    def _():
                        tok_copy(s, c, up).wait_recv()
                        pl.when(can_send(up))(lambda: tok_copy(s, c, up).start())

                both_ways(side)

            loop(pieces, one)

        @pl.when(is_inner)
        def _():
            hop(1)
            pl.when(low)(lambda: release(0))
            pl.when(jnp.logical_not(low))(lambda: release(1))
            loop(n - 1, hop, 2)
            pl.when(low)(lambda: release(1))
            pl.when(jnp.logical_not(low))(lambda: release(0))
            send_cross()
            forward_weights()
            relay_slice(near_end)
            relay_slice(far_end)
            other_weights()
            relay_slice(other_inner)
            loop(n, lambda s: accumulate(s, all_rows))
            loop(chunks, finish)

    def gather_odd():
        send_weights()
        both_ways(send_own)
        by_shard()

        @pl.when(is_inner)
        def _():
            forward_slices(me)
            forward_slices(near_end)
            forward_slices(far_end)

    pl.when(odd == 0)(gather_even)
    pl.when(odd == 1)(gather_odd)
    post_in.wait()
    bias_in.wait()

    lane_head = lax.broadcasted_iota(jnp.int32, (1, inner), 1) // head_dim
    contract = (((1,), (1,)), ((), ()))

    def attend(c):
        first = (c * step) // seq * seq
        keys_at = pl.ds(first, seq)
        bias_at = pl.ds(c * step - first, step)
        q = qkv[0, rows_at(c), :]
        k = qkv[1, keys_at, :]
        v = qkv[2, keys_at, :]
        stacked = jnp.concatenate([jnp.where(lane_head == h, q, jnp.zeros_like(q)) for h in range(heads)], axis=0)
        scores = lax.dot_general(stacked, k, contract, preferred_element_type=F32)
        scores = scores + bias_v[:, bias_at, :].reshape(heads * step, seq).astype(F32)
        weights = jnp.exp(scores - jnp.max(scores, axis=1, keepdims=True))
        scale = 1.0 / jnp.sum(weights, axis=1, keepdims=True)
        mixed = jnp.dot(weights.astype(BF16), v, preferred_element_type=F32) * scale
        context = mixed[0:step]
        for h in range(1, heads):
            context = jnp.where(lane_head == h, mixed[h * step : (h + 1) * step], context)
        ctx_all[me, rows_at(c), :] = context.astype(BF16)

    for c in range(0, chunks, 2):
        together = range(c, min(c + 2, chunks))
        for i in together:
            attend(i)
        for i in together:
            ctx_copy(me, i).start()

    def drain_line(s):
        @pl.when(s != me)
        def _():
            gain_copy(me, s).wait_send()

        def one(c):
            waited = (odd == 0) & (s == me) & is_end

            @pl.when((s <= me) & (me < n - 1) & jnp.logical_not(waited))
            def _():
                tok_copy(s, c, 1).wait_send()

            @pl.when((s >= me) & (me > 0) & jnp.logical_not(waited))
            def _():
                tok_copy(s, c, 0).wait_send()

        loop(pieces, one)

        @pl.when(is_source)
        def _():
            o_copy(s, d, partner, False).wait_send()
            loop(half, lambda k: o_copy(s, d, same_core(k), False).wait_send(), 1)

    def drain_early():
        loop(n, drain_line)
        w_copy(d, partner, False).wait_send()

        def drain_weights(k):
            w_copy(d, same_core(k), False).wait_send()
            w_copy(from_core(k), partner, True).wait_send()

        loop(half, drain_weights, 1)
        pl.when(jnp.logical_not(is_source))(lambda: cross_copy().wait_send())
        loop(chunks, lambda c: ctx_copy(me, c).wait_send())

    def project_out(s, at, first=False):
        value = jnp.dot(ctx_all[s, at, :], wo_all[s], preferred_element_type=F32)
        part[at, :] = value if first else part[at, :] + value

    def pass_on(c):
        ctx_copy(near_end, c).wait_recv()
        ctx_copy(near_end, c).start()

    def finalize(c):
        def block(s, at):
            stream = (x_all[s, rows_at(c), :].astype(F32) + part[rows_at(c), at]).astype(BF16)
            wide_stream = stream.astype(F32)
            return stream, wide_stream * wide_stream

        def both(own_at, end_at):
            stream_end, squares_end = block(near_end, end_at)
            out_buf[rows_at(c), :] = stream_end
            end_copy(c).start()
            stream, squares = block(me, own_at)
            stream_o[rows_at(c), :] = stream
            total = jnp.sum(squares + squares_end, axis=1, keepdims=True)
            turned = jnp.transpose(jnp.broadcast_to(total, (step, 128)))
            ss_mine[c] = turned[0:8, :]
            ss_all[me, c] = turned[0:8, :]

        pl.when(low)(lambda: both(pl.ds(feats, feats), pl.ds(0, feats)))
        pl.when(jnp.logical_not(low))(lambda: both(pl.ds(0, feats), pl.ds(feats, feats)))
        loop(n, lambda k: ss_copy(me, c, peer_mp(k)).start(), 1)

    pl.when(is_end)(drain_early)

    @pl.when(is_inner)
    def _():
        @pl.when(odd == 0)
        def _():
            forward_slices(me)
            forward_slices(near_end)

        pl.when(odd == 1)(lambda: forward_slices(other_inner))

        loop(chunks, pass_on)
        @pl.when(odd == 0)
        def _():
            forward_slices(far_end)
            forward_slices(other_inner)

        loop(n, other_slices)
        project_out(me, all_rows, True)
        drain_early()
        loop(chunks, lambda c: ctx_copy(other_inner, c).wait_recv())
        project_out(other_inner, all_rows)

        project_out(near_end, all_rows)

        def last(c):
            ctx_copy(far_end, c).wait_recv()
            project_out(far_end, rows_at(c))
            finalize(c)

        loop(chunks, last)

    gain = post_v[...].astype(F32).reshape(1, feats)

    def normalize(c):
        def arrived(s):
            pl.when(s != me)(lambda: ss_copy(s, c, s).wait_recv())

        loop(n - 1, arrived, 1)

        @pl.when(is_end)
        def _():
            end_copy(c).wait_recv()
            stream_o[rows_at(c), :] = landed[rows_at(c), :]

        total = ss_all[1, c] + ss_all[n - 2, c]
        scale = jnp.transpose(lax.rsqrt(total / model + epsilon))[:, 0:1]
        stream = stream_o[rows_at(c), :].astype(F32)
        normed_o[rows_at(c), :] = (stream * scale * gain).astype(BF16)

    loop(chunks, normalize)

    def drain_late(c):
        ctx_copy(near_end, c).wait_send()
        end_copy(c).wait_send()
        loop(n, lambda k: ss_copy(me, c, peer_mp(k)).wait_send(), 1)

    def drain_slices(z):
        def forwarded(k):
            o = from_core(k)
            pl.when(in_plane(o))(lambda: o_copy(z, o, partner, True).wait_send())

        loop(half, forwarded, 1)

    @pl.when(is_inner)
    def _():
        loop(chunks, drain_late)
        loop(n, drain_slices)


def publish(stream_i, normed_i, stream_o, normed_o, sems):
    copies = (
        pltpu.make_async_copy(stream_i, stream_o, sems.at[0]),
        pltpu.make_async_copy(normed_i, normed_o, sems.at[1]),
    )
    for copy in copies:
        copy.start()
    for copy in copies:
        copy.wait()


def on_device(n, groups, tokens, pre_gain, input_weight, output_weight, position_bias, post_gain):
    rows, feats = tokens.shape
    step = 128
    chunks = rows // step
    inner = input_weight.shape[2]
    model = n * feats
    wide = output_weight.shape[1] % 128 == 0
    if not wide:
        output_weight = output_weight.T
    dma, any_space = pltpu.SemaphoreType.DMA, pl.BlockSpec(memory_space=pl.ANY)
    vmem = pl.BlockSpec(memory_space=pltpu.VMEM)
    if wide and n - 2 == 2:
        pieces = rows // 64
        body = functools.partial(line_kernel, n, groups, chunks)
        scratch = [
            pltpu.VMEM((n, rows, feats), BF16),
            pltpu.VMEM((n * feats,), BF16),
            pltpu.VMEM((feats,), BF16),
            pltpu.VMEM((3, model, inner), BF16),
            pltpu.VMEM(output_weight.shape, BF16),
            pltpu.VMEM((n, inner, 2 * feats), BF16),
            pltpu.VMEM(position_bias.shape, BF16),
            pltpu.VMEM((3, rows, inner), F32),
            pltpu.VMEM((rows, feats), F32),
            pltpu.VMEM((3, rows, inner), BF16),
            pltpu.VMEM((n, rows, inner), BF16),
            pltpu.VMEM((rows, 2 * feats), F32),
            pltpu.VMEM((rows, feats), BF16),
            pltpu.VMEM((rows, feats), BF16),
            pltpu.VMEM((chunks, 8, step), F32),
            pltpu.VMEM((n, chunks, 8, step), F32),
            dma((2, n, pieces)),
            dma((n, pieces)),
            dma((n,)),
            dma((n,)),
            dma((2, groups)),
            dma((groups,)),
            dma((1,)),
            dma((2, n, groups)),
            dma((n, groups)),
            dma((n, chunks)),
            dma((n, chunks)),
            dma((chunks,)),
            dma((chunks,)),
            dma((n, chunks)),
            dma((n, chunks)),
            dma((6,)),
            pltpu.SemaphoreType.REGULAR((2,)),
        ]
    else:
        body = functools.partial(kernel, n, groups, chunks, wide)
        wo_shape = (inner, model) if wide else (model, inner)
        scratch = [
            pltpu.VMEM((n, rows, feats), BF16),
            pltpu.VMEM((n * feats,), BF16),
            pltpu.VMEM((feats,), BF16),
            pltpu.VMEM((3, model, inner), BF16),
            pltpu.VMEM(wo_shape, BF16),
            pltpu.VMEM(wo_shape, BF16),
            pltpu.VMEM(position_bias.shape, BF16),
            pltpu.VMEM((3, rows, inner), F32),
            pltpu.VMEM((rows, feats), F32),
            pltpu.VMEM((3, rows, inner), BF16),
            pltpu.VMEM((n, rows, feats), F32),
            pltpu.VMEM((n, rows, feats), BF16),
            pltpu.VMEM((2, n, rows, feats), BF16),
            pltpu.VMEM((rows, inner), BF16),
            pltpu.VMEM((rows, inner), BF16),
            pltpu.VMEM((chunks, 8, step), F32),
            pltpu.VMEM((n, chunks, 8, step), F32),
            dma((2, n, chunks)),
            dma((n, chunks)),
            dma((n,)),
            dma((n,)),
            dma((3, 2, groups)),
            dma((3, groups)),
            dma((chunks,)),
            dma((chunks,)),
            dma((n, chunks)),
            dma((2, n, chunks)),
            dma((n, chunks)),
            dma((n, chunks)),
            dma((6,)),
            pltpu.SemaphoreType.REGULAR((2,)),
        ]
    stream, normed = pl.pallas_call(
        body,
        out_shape=(pltpu.VMEM((rows, feats), BF16), pltpu.VMEM((rows, feats), BF16)),
        in_specs=[any_space] * 6,
        out_specs=[vmem] * 2,
        scratch_shapes=scratch,
        compiler_params=pltpu.CompilerParams(
            collective_id=0, has_side_effects=True, vmem_limit_bytes=56 * 1024 * 1024
        ),
    )(tokens, pre_gain, input_weight, output_weight, position_bias, post_gain)
    shape = jax.ShapeDtypeStruct((rows, feats), BF16)
    return pl.pallas_call(
        publish,
        out_shape=(shape, shape),
        in_specs=[vmem] * 2,
        out_specs=[any_space] * 2,
        scratch_shapes=[dma((2,))],
        compiler_params=pltpu.CompilerParams(vmem_limit_bytes=4 * 1024 * 1024),
    )(stream, normed)


def solution(mesh):
    return jax.shard_map(
        functools.partial(on_device, mesh.shape["mp"], mesh.shape["dp"]),
        mesh=mesh,
        in_specs=(
            P("dp", "mp"),
            P("mp"),
            P(None, "dp", "mp"),
            P("mp", "dp"),
            P("mp", None, None),
            P("mp"),
        ),
        out_specs=(P("dp", "mp"), P("dp", "mp")),
        check_vma=False,
    )
```

```python
import functools

import jax
import jax.numpy as jnp
from jax import lax
from jax.experimental import pallas as pl
from jax.experimental.pallas import tpu as pltpu
from jax.sharding import PartitionSpec as P

epsilon = 1e-06
F32, BF16 = jnp.float32, jnp.bfloat16
MESH = pl.DeviceIdType.MESH


def kernel(
    n,
    groups,
    chunks,
    wide,
    tok,
    pre,
    win,
    wout,
    bias,
    post,
    stream_o,
    normed_o,
    x_all,
    gain_all,
    post_v,
    w_all,
    wo_all,
    wo_end,
    bias_v,
    acc,
    square,
    qkv,
    part,
    out_buf,
    landed,
    ctx_buf,
    ctx_in,
    ss_mine,
    ss_all,
    ag_send,
    ag_recv,
    g_send,
    g_recv,
    w_send,
    w_recv,
    ctx_send,
    ctx_recv,
    rs_send,
    rs_recv,
    ss_send,
    ss_recv,
    local_sem,
    link_free,
):
    rows, feats = tok.shape
    step = rows // chunks
    heads, seq = bias.shape[0], bias.shape[1]
    inner = win.shape[2]
    head_dim = inner // heads
    model = n * feats
    wrows = win.shape[1]
    wcols = model // groups
    half = groups // 2
    me = lax.axis_index("mp")
    d = lax.axis_index("dp")
    odd = lax.rem(d, 2)
    pair = d // 2
    partner = d + 1 - 2 * odd
    is_end = (me == 0) | (me == n - 1)
    is_edge = (me == 1) | (me == n - 2)
    all_rows = pl.ds(0, rows)

    def rows_at(c):
        return pl.ds(pl.multiple_of(c * step, step), step)

    def feats_at(s):
        return pl.ds(pl.multiple_of(s * feats, feats), feats)

    def loop(count, body, start=0):
        def wrapped(i, carry):
            body(i)
            return carry

        lax.fori_loop(start, count, wrapped, 0)

    def remote(src, dst, send, recv, target):
        return pltpu.make_async_remote_copy(
            src_ref=src,
            dst_ref=dst,
            send_sem=send,
            recv_sem=recv,
            device_id=target,
            device_id_type=MESH,
        )

    def tok_copy(s, c, up):
        ref = x_all.at[s, rows_at(c)]
        return remote(ref, ref, ag_send.at[up, s, c], ag_recv.at[s, c], {"mp": me + 2 * up - 1})

    def gain_copy(origin, target):
        ref = gain_all.at[feats_at(origin)]
        return remote(ref, ref, g_send.at[target], g_recv.at[origin], {"mp": target})

    def w_slot(o):
        return w_all.at[:, pl.ds(pl.multiple_of(o * wrows, wrows), wrows), :]

    def o_slot(ref, o):
        block = pl.ds(pl.multiple_of(o * wcols, wcols), wcols)
        return ref.at[:, block] if wide else ref.at[block, :]

    def slot(which, o):
        return w_slot(o) if which == 0 else o_slot(wo_all if which == 1 else wo_end, o)

    def weight_copy(which, o, target, forward):
        ref = slot(which, o)
        send = w_send.at[which, 1, o] if forward else w_send.at[which, 0, target]
        return remote(ref, ref, send, w_recv.at[which, o], {"dp": target})

    def cross_copy():
        inwards = jnp.where(me == 0, 1, n - 2)
        return remote(
            o_slot(wo_all, d), o_slot(wo_end, d), w_send.at[2, 0, d], w_recv.at[2, d], {"mp": inwards}
        )

    def ctx_copy(c):
        inwards = jnp.where(me == 0, 1, n - 2)
        return remote(
            ctx_buf.at[rows_at(c)], ctx_in.at[rows_at(c)], ctx_send.at[c], ctx_recv.at[c], {"mp": inwards}
        )

    def rs_copy(s, c, up):
        return remote(
            out_buf.at[s, rows_at(c)],
            landed.at[up, s, rows_at(c)],
            rs_send.at[s, c],
            rs_recv.at[up, s, c],
            {"mp": me + 2 * up - 1},
        )

    def ss_copy(origin, c, target):
        return remote(
            ss_mine.at[c], ss_all.at[origin, c], ss_send.at[target, c], ss_recv.at[origin, c], {"mp": target}
        )

    local = (
        pltpu.make_async_copy(tok, x_all.at[me], local_sem.at[0]),
        pltpu.make_async_copy(pre, gain_all.at[feats_at(me)], local_sem.at[1]),
        pltpu.make_async_copy(win, w_slot(d), local_sem.at[2]),
        pltpu.make_async_copy(wout, o_slot(wo_all, d), local_sem.at[3]),
        pltpu.make_async_copy(post, post_v, local_sem.at[4]),
        pltpu.make_async_copy(bias, bias_v, local_sem.at[5]),
    )
    for copy in local:
        copy.start()

    def peer_mp(k):
        return lax.rem(me + k, n)

    def same_core(k):
        return 2 * lax.rem(pair + k, half) + odd

    def from_core(k):
        return 2 * lax.rem(pair + half - k, half) + odd

    barrier = pltpu.get_barrier_semaphore()

    def greet(target):
        pl.semaphore_signal(barrier, inc=1, device_id=target, device_id_type=MESH)

    loop(n, lambda k: greet({"mp": peer_mp(k)}), 1)
    loop(half, lambda k: greet({"dp": same_core(k)}), 1)
    greet({"dp": partner})
    acc[...] = jnp.zeros_like(acc)
    square[...] = jnp.zeros_like(square)
    for copy in local[:5]:
        copy.wait()
    pl.semaphore_wait(barrier, n - 1 + half - 1 + 1)

    def can_send(up):
        return (me < n - 1) if up else (me > 0)

    def send_own(up):
        @pl.when(can_send(up))
        def _():
            @pl.when(odd == 1)
            def _():
                pl.semaphore_wait(link_free.at[up], 1)

            loop(chunks, lambda c: tok_copy(me, c, up).start())

    def release(up):
        @pl.when(can_send(up))
        def _():
            pl.semaphore_signal(
                link_free.at[up], inc=1, device_id={"dp": partner}, device_id_type=MESH
            )

    def send_weights(which):
        weight_copy(which, d, partner, False).start()
        loop(half, lambda k: weight_copy(which, d, same_core(k), False).start(), 1)

    def forward_weights(which):
        def forward(k):
            o = from_core(k)
            weight_copy(which, o, partner, False).wait_recv()
            weight_copy(which, o, partner, True).start()

        loop(half, forward, 1)

    def other_weights(which):
        loop(half, lambda k: weight_copy(which, 2 * k + 1 - odd, partner, False).wait_recv())

    def pass_end_weights():
        @pl.when(is_edge)
        def _():
            weight_copy(2, d, partner, False).wait_recv()
            send_weights(2)

    def forward_out_weights():
        pl.when(jnp.logical_not(is_end))(lambda: forward_weights(1))
        pl.when(is_edge)(lambda: forward_weights(2))

    def take(up, j, use=None):
        s = me - j if up else me + j

        @pl.when((s >= 0) & (s < n))
        def _():
            def one(c):
                tok_copy(s, c, up).wait_recv()

                @pl.when(can_send(up))
                def _():
                    tok_copy(s, c, up).start()

                if use is not None:
                    use(s, c)

            loop(chunks, one)

    def accumulate(s, at):
        gain = gain_all[feats_at(s)].astype(F32).reshape(1, feats)
        x = x_all[s, at, :].astype(F32)
        square[at, :] += x * x
        xg = (x * gain).astype(BF16)
        for m in range(3):
            acc[m, at, :] += jnp.dot(xg, w_all[m, feats_at(s), :], preferred_element_type=F32)

    def both_ways(action):
        @pl.when(2 * me < n)
        def _():
            action(0)
            action(1)

        @pl.when(2 * me >= n)
        def _():
            action(1)
            action(0)

    def finish(c):
        total = jnp.sum(square[rows_at(c), :], axis=1, keepdims=True)
        inverse = lax.rsqrt(total / model + epsilon)
        for m in range(3):
            qkv[m, rows_at(c), :] = (acc[m, rows_at(c), :] * inverse).astype(BF16)

    def send_all_weights():
        send_weights(0)
        pl.when(is_end)(lambda: cross_copy().start())
        pl.when(jnp.logical_not(is_end))(lambda: send_weights(1))

    def wait_gains():
        loop(n, lambda k: gain_copy(peer_mp(k), peer_mp(k)).wait_recv(), 1)

    def gather_even():
        both_ways(send_own)
        send_all_weights()

        @pl.when(is_end)
        def _():
            up = jnp.where(me == 0, 1, 0)
            loop(chunks, lambda c: tok_copy(me, c, up).wait_send())
            both_ways(release)

        def hop(j):
            def one(c):
                def side(up):
                    s = me - j if up else me + j

                    @pl.when((s >= 0) & (s < n))
                    def _():
                        tok_copy(s, c, up).wait_recv()
                        pl.when(can_send(up))(lambda: tok_copy(s, c, up).start())

                both_ways(side)

            loop(chunks, one)

        loop(n, hop, 1)
        pl.when(jnp.logical_not(is_end))(lambda: both_ways(release))
        pass_end_weights()
        forward_weights(0)
        wait_gains()
        other_weights(0)
        loop(n, lambda s: accumulate(s, all_rows))
        loop(chunks, finish)

    def gather_odd():
        send_all_weights()
        both_ways(send_own)

        def toward(near):
            far = 1 - near
            reach = n - 1 - me if near else me
            loop(n, lambda j: take(near, j), 1)
            pass_end_weights()
            forward_weights(0)
            wait_gains()
            take(far, 1)
            other_weights(0)

            def known(s):
                pl.when((s <= me + 1) if near else (s >= me - 1))(lambda: accumulate(s, all_rows))

            loop(n, known)

            def later(j):
                @pl.when(j < reach)
                def _():
                    take(far, j)
                    accumulate(me + j if near else me - j, all_rows)

            def use(s, c):
                accumulate(s, rows_at(c))
                finish(c)

            loop(n, later, 2)
            pl.when(reach > 1)(lambda: take(far, reach, use))
            pl.when(reach <= 1)(lambda: loop(chunks, finish))

        pl.when(2 * me < n)(lambda: toward(1))
        pl.when(2 * me >= n)(lambda: toward(0))
        forward_out_weights()

    loop(n, lambda k: gain_copy(me, peer_mp(k)).start(), 1)
    pl.when(odd == 0)(gather_even)
    pl.when(odd == 1)(gather_odd)

    local[5].wait()

    lane_head = lax.broadcasted_iota(jnp.int32, (1, inner), 1) // head_dim
    contract = (((1,), (1,)), ((), ()))

    def attend(c):
        first = (c * step) // seq * seq
        keys_at = pl.ds(pl.multiple_of(first, seq), seq)
        bias_at = pl.ds(pl.multiple_of(c * step - first, step), step)
        q = qkv[0, rows_at(c), :]
        k = qkv[1, keys_at, :]
        v = qkv[2, keys_at, :]
        stacked = jnp.concatenate([jnp.where(lane_head == h, q, jnp.zeros_like(q)) for h in range(heads)], axis=0)
        scores = lax.dot_general(stacked, k, contract, preferred_element_type=F32)
        scores = scores + bias_v[:, bias_at, :].reshape(heads * step, seq).astype(F32)
        weights = jnp.exp(scores - jnp.max(scores, axis=1, keepdims=True))
        scale = 1.0 / jnp.sum(weights, axis=1, keepdims=True)
        mixed = jnp.dot(weights.astype(BF16), v, preferred_element_type=F32) * scale
        context = mixed[0:step]
        for h in range(1, heads):
            context = jnp.where(lane_head == h, mixed[h * step : (h + 1) * step], context)
        ctx_buf[rows_at(c), :] = context.astype(BF16)
        pl.when(is_end)(lambda: ctx_copy(c).start())

    loop(chunks, attend)

    def project_out(context, ref, s):
        block = feats_at(s)
        if wide:
            return jnp.dot(context, ref[:, block], preferred_element_type=F32)
        return lax.dot_general(context, ref[block, :], contract, preferred_element_type=F32)

    def send_out(s, c, up, value):
        out_buf[s, rows_at(c), :] = value.astype(BF16)
        rs_copy(s, c, up).start()

    def own_share(s):
        part[s] = project_out(ctx_buf[...], wo_all, s)

    def originate(c):
        ctx_copy(c).wait_recv()
        context = ctx_in[rows_at(c), :]

        def far(k):
            s = jnp.where(me == 1, n - 1 - k, k)
            value = part[s, rows_at(c), :] + project_out(context, wo_end, s)
            send_out(s, c, jnp.where(me == 1, 1, 0), value)

        def near(k):
            s = jnp.where(me == 1, k, n - 2 + k)
            part[s, rows_at(c), :] += project_out(context, wo_end, s)

        loop(n - 2, far)
        loop(2, near)

    def finished(s, c):
        value = x_all[s, rows_at(c), :].astype(F32) + part[s, rows_at(c), :]
        stream = value.astype(BF16)
        wide_stream = stream.astype(F32)
        return stream, wide_stream * wide_stream

    def finalize(c):
        stream, squares = finished(me, c)
        stream_o[rows_at(c), :] = stream
        part[me, rows_at(c), :] = squares

        @pl.when(is_edge)
        def _():
            end, up = jnp.where(me == 1, 0, n - 1), jnp.where(me == 1, 0, 1)
            stream_end, squares_end = finished(end, c)
            out_buf[end, rows_at(c), :] = stream_end
            rs_copy(end, c, up).start()
            part[me, rows_at(c), :] += squares_end

        total = jnp.sum(part[me, rows_at(c), :], axis=1, keepdims=True)
        turned = jnp.transpose(jnp.broadcast_to(total, (step, 128)))
        ss_mine[c] = turned[0:8, :]
        ss_all[me, c] = turned[0:8, :]
        loop(n, lambda k: ss_copy(me, c, peer_mp(k)).start(), 1)

    def combine(c):
        def message(k):
            for up in (1, 0):
                s = n - 1 - k if up else k
                follows = (me >= 2) if up else (me <= n - 3)
                further = (s > me) if up else (s < me)
                last = (me == n - 2) if up else (me == 1)

                @pl.when(follows & (further | (s == me)))
                def _():
                    rs_copy(s, c, up).wait_recv()
                    value = part[s, rows_at(c), :] + landed[up, s, rows_at(c), :].astype(F32)

                    @pl.when((s == me) | last)
                    def _():
                        part[s, rows_at(c), :] = value

                    @pl.when((s != me) & jnp.logical_not(last))
                    def _():
                        send_out(s, c, up, value)

        loop(n - 2, message)
        finalize(c)

    @pl.when(jnp.logical_not(is_end))
    def _():
        pl.when(odd == 0)(forward_out_weights)
        other_weights(1)
        pl.when(is_edge)(lambda: other_weights(2))
        loop(n, own_share)
        pl.when(is_edge)(lambda: loop(chunks, originate))
        loop(chunks, combine)

    gain = post_v[...].astype(F32).reshape(1, feats)

    def normalize(c):
        def arrived(s):
            pl.when(s != me)(lambda: ss_copy(s, c, s).wait_recv())

        loop(n - 1, arrived, 1)

        @pl.when(is_end)
        def _():
            up = jnp.where(me == 0, 0, 1)
            rs_copy(me, c, up).wait_recv()
            stream_o[rows_at(c), :] = landed[up, me, rows_at(c), :]

        total = jnp.zeros((8, step), F32)
        for s in range(1, n - 1):
            total = total + ss_all[s, c]
        scale = jnp.transpose(lax.rsqrt(total / model + epsilon))[:, 0:1]
        stream = stream_o[rows_at(c), :].astype(F32)
        normed_o[rows_at(c), :] = (stream * scale * gain).astype(BF16)

    loop(chunks, normalize)

    loop(n, lambda k: gain_copy(me, peer_mp(k)).wait_send(), 1)

    def drain_tokens(s):
        def one(c):
            waited = (odd == 0) & (s == me) & is_end

            @pl.when((s <= me) & (me < n - 1) & jnp.logical_not(waited))
            def _():
                tok_copy(s, c, 1).wait_send()

            @pl.when((s >= me) & (me > 0) & jnp.logical_not(waited))
            def _():
                tok_copy(s, c, 0).wait_send()

            @pl.when(jnp.logical_not(is_end) & (s != me))
            def _():
                rs_copy(s, c, 1).wait_send()
                ss_copy(me, c, s).wait_send()

        loop(chunks, one)

    loop(n, drain_tokens)

    def drain_weights(which):
        weight_copy(which, d, partner, False).wait_send()

        def drain(k):
            weight_copy(which, d, same_core(k), False).wait_send()
            weight_copy(which, from_core(k), partner, True).wait_send()

        loop(half, drain, 1)

    drain_weights(0)
    pl.when(is_edge)(lambda: drain_weights(2))

    @pl.when(is_end)
    def _():
        cross_copy().wait_send()
        loop(chunks, lambda c: ctx_copy(c).wait_send())

    pl.when(jnp.logical_not(is_end))(lambda: drain_weights(1))


def line_kernel(
    n,
    groups,
    chunks,
    tok,
    pre,
    win,
    wout,
    bias,
    post,
    stream_o,
    normed_o,
    x_all,
    gain_all,
    post_v,
    w_all,
    wo_own,
    wo_all,
    bias_v,
    acc,
    square,
    qkv,
    ctx_all,
    part,
    out_buf,
    landed,
    ss_mine,
    ss_all,
    ag_send,
    ag_recv,
    g_send,
    g_recv,
    w_send,
    w_recv,
    x_send,
    o_send,
    o_recv,
    ctx_send,
    ctx_recv,
    end_send,
    end_recv,
    ss_send,
    ss_recv,
    local_sem,
    link_free,
):
    rows, feats = tok.shape
    step = rows // chunks
    pieces = ag_recv.shape[1]
    piece = rows // pieces
    heads, seq = bias.shape[0], bias.shape[1]
    inner = win.shape[2]
    head_dim = inner // heads
    model = n * feats
    wrows = win.shape[1]
    wcols = model // groups
    half = groups // 2
    me = lax.axis_index("mp")
    d = lax.axis_index("dp")
    odd = lax.rem(d, 2)
    pair = d // 2
    partner = d + 1 - 2 * odd
    low = 2 * me < n
    is_end = (me == 0) | (me == n - 1)
    is_inner = jnp.logical_not(is_end)
    near_end, far_end = jnp.where(low, 0, n - 1), jnp.where(low, n - 1, 0)
    other_inner = n - 1 - me
    inwards = me + jnp.where(low, 1, -1)
    home = jnp.where(d < half, 1, n - 2)
    is_source = me == home
    late_cross = is_end & (home == inwards) & (odd == 1)
    all_rows = pl.ds(0, rows)

    def rows_at(c):
        return pl.ds(pl.multiple_of(c * step, step), step)

    def feats_at(s):
        return pl.ds(pl.multiple_of(s * feats, feats), feats)

    def loop(count, body, start=0):
        def wrapped(i, carry):
            body(i)
            return carry

        lax.fori_loop(start, count, wrapped, 0)

    def remote(src, dst, send, recv, target):
        return pltpu.make_async_remote_copy(
            src_ref=src,
            dst_ref=dst,
            send_sem=send,
            recv_sem=recv,
            device_id=target,
            device_id_type=MESH,
        )

    def tok_copy(s, c, up):
        ref = x_all.at[s, pl.ds(pl.multiple_of(c * piece, piece), piece)]
        return remote(ref, ref, ag_send.at[up, s, c], ag_recv.at[s, c], {"mp": me + 2 * up - 1})

    def gain_copy(origin, target):
        ref = gain_all.at[feats_at(origin)]
        return remote(ref, ref, g_send.at[target], g_recv.at[origin], {"mp": target})

    def w_slot(o):
        return w_all.at[:, pl.ds(pl.multiple_of(o * wrows, wrows), wrows), :]

    def w_copy(o, target, forward):
        send = w_send.at[1, o] if forward else w_send.at[0, target]
        return remote(w_slot(o), w_slot(o), send, w_recv.at[o], {"dp": target})

    def o_slot(z, o):
        return wo_all.at[z, lax.rem(o, half)]

    def o_copy(z, o, target, forward):
        send = o_send.at[1, z, o] if forward else o_send.at[0, z, target]
        return remote(o_slot(z, o), o_slot(z, o), send, o_recv.at[z, o], {"dp": target})

    def cross_copy():
        return remote(wo_own, o_slot(me, d), x_send.at[0], o_recv.at[me, d], {"mp": home})

    def ctx_copy(s, c):
        ref = ctx_all.at[s, rows_at(c)]
        return remote(ref, ref, ctx_send.at[s, c], ctx_recv.at[s, c], {"mp": inwards})

    def end_copy(c):
        return remote(
            out_buf.at[rows_at(c)], landed.at[rows_at(c)], end_send.at[c], end_recv.at[c], {"mp": near_end}
        )

    def ss_copy(origin, c, target):
        return remote(
            ss_mine.at[c], ss_all.at[origin, c], ss_send.at[target, c], ss_recv.at[origin, c], {"mp": target}
        )

    tok_in = pltpu.make_async_copy(tok, x_all.at[me], local_sem.at[0])
    win_in = pltpu.make_async_copy(win, w_slot(d), local_sem.at[1])
    pre_in = pltpu.make_async_copy(pre, gain_all.at[feats_at(me)], local_sem.at[2])
    post_in = pltpu.make_async_copy(post, post_v, local_sem.at[3])
    bias_in = pltpu.make_async_copy(bias, bias_v, local_sem.at[4])

    def wout_in(action):
        pl.when(is_source)(lambda: action(pltpu.make_async_copy(wout, o_slot(me, d), local_sem.at[5])))
        pl.when(jnp.logical_not(is_source))(
            lambda: action(pltpu.make_async_copy(wout, wo_own, local_sem.at[5]))
        )

    tok_in.start()
    win_in.start()
    pre_in.start()
    wout_in(lambda copy: copy.start())

    def peer_mp(k):
        return lax.rem(me + k, n)

    def same_core(k):
        return 2 * lax.rem(pair + k, half) + odd

    def from_core(k):
        return 2 * lax.rem(pair + half - k, half) + odd

    barrier = pltpu.get_barrier_semaphore()

    def greet(target):
        pl.semaphore_signal(barrier, inc=1, device_id=target, device_id_type=MESH)

    loop(n, lambda k: greet({"mp": peer_mp(k)}), 1)
    loop(half, lambda k: greet({"dp": same_core(k)}), 1)
    greet({"dp": partner})
    acc[...] = jnp.zeros_like(acc)
    square[...] = jnp.zeros_like(square)
    tok_in.wait()
    post_in.start()
    bias_in.start()
    pl.semaphore_wait(barrier, n - 1 + half - 1 + 1)

    def can_send(up):
        return (me < n - 1) if up else (me > 0)

    def send_own(up):
        @pl.when(can_send(up))
        def _():
            @pl.when(odd == 1)
            def _():
                pl.semaphore_wait(link_free.at[up], 1)

            loop(pieces, lambda c: tok_copy(me, c, up).start())

    def release(up):
        @pl.when(can_send(up))
        def _():
            pl.semaphore_signal(
                link_free.at[up], inc=1, device_id={"dp": partner}, device_id_type=MESH
            )

    def both_ways(action):
        @pl.when(low)
        def _():
            action(0)
            action(1)

        @pl.when(jnp.logical_not(low))
        def _():
            action(1)
            action(0)

    def in_plane(o):
        return (o < half) == (me == 1)

    def send_slice(z):
        o_copy(z, d, partner, False).start()
        loop(half, lambda k: o_copy(z, d, same_core(k), False).start(), 1)

    def relay_slice(z):
        @pl.when(is_source)
        def _():
            o_copy(z, d, partner, False).wait_recv()
            send_slice(z)

    def forward_slices(z):
        def forward(k):
            o = from_core(k)

            @pl.when(in_plane(o))
            def _():
                o_copy(z, o, partner, False).wait_recv()
                o_copy(z, o, partner, True).start()

        loop(half, forward, 1)

    def other_slices(z):
        def other(k):
            o = 2 * k + 1 - odd
            pl.when(in_plane(o))(lambda: o_copy(z, o, partner, False).wait_recv())

        loop(half, other)

    def send_weights():
        win_in.wait()
        w_copy(d, partner, False).start()
        loop(half, lambda k: w_copy(d, same_core(k), False).start(), 1)
        pre_in.wait()
        loop(n, lambda k: gain_copy(me, peer_mp(k)).start(), 1)
        wout_in(lambda copy: copy.wait())
        pl.when(is_source)(lambda: send_slice(me))
        pl.when(jnp.logical_not(is_source | late_cross))(lambda: cross_copy().start())

    def forward_weights():
        def forward(k):
            o = from_core(k)
            w_copy(o, partner, False).wait_recv()
            w_copy(o, partner, True).start()

        loop(half, forward, 1)
        loop(n, lambda k: gain_copy(peer_mp(k), peer_mp(k)).wait_recv(), 1)

    def other_weights():
        loop(half, lambda k: w_copy(2 * k + 1 - odd, partner, False).wait_recv())

    def take(up, j, use=None):
        s = me - j if up else me + j

        @pl.when((s >= 0) & (s < n))
        def _():
            def one(c):
                tok_copy(s, c, up).wait_recv()
                pl.when(can_send(up))(lambda: tok_copy(s, c, up).start())

            if use is None:
                loop(pieces, one)
            else:
                per = pieces // chunks

                def block(c):
                    loop(per, lambda i: one(c * per + i))
                    use(s, c)

                loop(chunks, block)

    def accumulate(s, at):
        gain = gain_all[feats_at(s)].astype(F32).reshape(1, feats)
        x = x_all[s, at, :].astype(F32)
        square[at, :] += x * x
        xg = (x * gain).astype(BF16)
        for m in range(3):
            acc[m, at, :] += jnp.dot(xg, w_all[m, feats_at(s), :], preferred_element_type=F32)

    def finish(c):
        total = jnp.sum(square[rows_at(c), :], axis=1, keepdims=True)
        inverse = lax.rsqrt(total / model + epsilon)
        for m in range(3):
            qkv[m, rows_at(c), :] = (acc[m, rows_at(c), :] * inverse).astype(BF16)

    def gather_by_shard(near):
        far = 1 - near
        reach = n - 1 - me if near else me
        loop(n, lambda j: take(near, j), 1)
        pl.when(late_cross)(lambda: cross_copy().start())
        forward_weights()
        relay_slice(near_end)
        relay_slice(far_end)
        relay_slice(other_inner)
        take(far, 1)
        other_weights()

        def known(s):
            pl.when((s <= me + 1) if near else (s >= me - 1))(lambda: accumulate(s, all_rows))

        loop(n, known)

        def later(j):
            @pl.when(j < reach)
            def _():
                take(far, j)
                accumulate(me + j if near else me - j, all_rows)

        def use(s, c):
            accumulate(s, rows_at(c))
            finish(c)

        loop(n, later, 2)
        take(far, reach, use)

    def by_shard():
        pl.when(low)(lambda: gather_by_shard(1))
        pl.when(jnp.logical_not(low))(lambda: gather_by_shard(0))

    def gather_even():
        both_ways(send_own)
        send_weights()

        @pl.when(is_end)
        def _():
            up = jnp.where(me == 0, 1, 0)
            loop(pieces, lambda c: tok_copy(me, c, up).wait_send())
            both_ways(release)
            by_shard()

        def hop(j, start=0, stop=pieces):
            def one(c):
                def side(up):
                    s = me - j if up else me + j

                    @pl.when((s >= 0) & (s < n))
                    def _():
                        tok_copy(s, c, up).wait_recv()
                        pl.when(can_send(up))(lambda: tok_copy(s, c, up).start())

                both_ways(side)

            loop(stop, one, start)

        @pl.when(is_inner)
        def _():
            hop(1)
            pl.when(low)(lambda: release(0))
            pl.when(jnp.logical_not(low))(lambda: release(1))
            hop(2, 0, pieces // 2)
            pl.when(low)(lambda: release(1))
            pl.when(jnp.logical_not(low))(lambda: release(0))
            hop(2, pieces // 2)
            forward_weights()
            relay_slice(near_end)
            relay_slice(far_end)
            relay_slice(other_inner)
            other_weights()
            loop(n, lambda s: accumulate(s, all_rows))
            loop(chunks, finish)
            forward_slices(me)

    def gather_odd():
        send_weights()
        both_ways(send_own)
        by_shard()

        @pl.when(is_inner)
        def _():
            forward_slices(me)
            forward_slices(near_end)
            forward_slices(far_end)

    pl.when(odd == 0)(gather_even)
    pl.when(odd == 1)(gather_odd)
    post_in.wait()
    bias_in.wait()

    lane_head = lax.broadcasted_iota(jnp.int32, (1, inner), 1) // head_dim
    contract = (((1,), (1,)), ((), ()))

    def attend(c):
        first = (c * step) // seq * seq
        keys_at = pl.ds(first, seq)
        bias_at = pl.ds(c * step - first, step)
        q = qkv[0, rows_at(c), :]
        k = qkv[1, keys_at, :]
        v = qkv[2, keys_at, :]
        stacked = jnp.concatenate([jnp.where(lane_head == h, q, jnp.zeros_like(q)) for h in range(heads)], axis=0)
        scores = lax.dot_general(stacked, k, contract, preferred_element_type=F32)
        scores = scores + bias_v[:, bias_at, :].reshape(heads * step, seq).astype(F32)
        weights = jnp.exp(scores - jnp.max(scores, axis=1, keepdims=True))
        scale = 1.0 / jnp.sum(weights, axis=1, keepdims=True)
        mixed = jnp.dot(weights.astype(BF16), v, preferred_element_type=F32) * scale
        context = mixed[0:step]
        for h in range(1, heads):
            context = jnp.where(lane_head == h, mixed[h * step : (h + 1) * step], context)
        ctx_all[me, rows_at(c), :] = context.astype(BF16)

    for c in range(0, chunks, 2):
        together = range(c, min(c + 2, chunks))
        for i in together:
            attend(i)
        for i in together:
            ctx_copy(me, i).start()

    def drain_line(s):
        @pl.when(s != me)
        def _():
            gain_copy(me, s).wait_send()

        def one(c):
            waited = (odd == 0) & (s == me) & is_end

            @pl.when((s <= me) & (me < n - 1) & jnp.logical_not(waited))
            def _():
                tok_copy(s, c, 1).wait_send()

            @pl.when((s >= me) & (me > 0) & jnp.logical_not(waited))
            def _():
                tok_copy(s, c, 0).wait_send()

        loop(pieces, one)

        @pl.when(is_source)
        def _():
            o_copy(s, d, partner, False).wait_send()
            loop(half, lambda k: o_copy(s, d, same_core(k), False).wait_send(), 1)

    def drain_early():
        loop(n, drain_line)
        w_copy(d, partner, False).wait_send()

        def drain_weights(k):
            w_copy(d, same_core(k), False).wait_send()
            w_copy(from_core(k), partner, True).wait_send()

        loop(half, drain_weights, 1)
        pl.when(jnp.logical_not(is_source))(lambda: cross_copy().wait_send())
        loop(chunks, lambda c: ctx_copy(me, c).wait_send())

    def project_out(s, at, first=False):
        weight = jnp.concatenate([wo_all[s, i] for i in range(wo_all.shape[1])], axis=1)
        value = jnp.dot(ctx_all[s, at, :], weight, preferred_element_type=F32)
        part[at, :] = value if first else part[at, :] + value

    def pass_on(c):
        ctx_copy(near_end, c).wait_recv()
        ctx_copy(near_end, c).start()

    def finalize(c):
        def block(s, at):
            stream = (x_all[s, rows_at(c), :].astype(F32) + part[rows_at(c), at]).astype(BF16)
            wide_stream = stream.astype(F32)
            return stream, wide_stream * wide_stream

        def both(own_at, end_at):
            stream_end, squares_end = block(near_end, end_at)
            out_buf[rows_at(c), :] = stream_end
            end_copy(c).start()
            stream, squares = block(me, own_at)
            stream_o[rows_at(c), :] = stream
            total = jnp.sum(squares + squares_end, axis=1, keepdims=True)
            turned = jnp.transpose(jnp.broadcast_to(total, (step, 128)))
            ss_mine[c] = turned[0:8, :]
            ss_all[me, c] = turned[0:8, :]

        pl.when(low)(lambda: both(pl.ds(feats, feats), pl.ds(0, feats)))
        pl.when(jnp.logical_not(low))(lambda: both(pl.ds(0, feats), pl.ds(feats, feats)))
        loop(n, lambda k: ss_copy(me, c, peer_mp(k)).start(), 1)

    pl.when(is_end)(drain_early)

    @pl.when(is_inner)
    def _():
        @pl.when(odd == 0)
        def _():
            forward_slices(near_end)
            forward_slices(far_end)

        pl.when(odd == 1)(lambda: forward_slices(other_inner))
        other_slices(me)
        project_out(me, all_rows, True)
        other_slices(near_end)
        def near(c):
            pass_on(c)
            project_out(near_end, rows_at(c))

        loop(chunks // 2, near)
        pl.when(odd == 0)(lambda: forward_slices(other_inner))
        loop(chunks, near, chunks // 2)
        other_slices(other_inner)
        loop(chunks, lambda c: ctx_copy(other_inner, c).wait_recv())
        project_out(other_inner, all_rows)
        other_slices(far_end)

        def last(c):
            ctx_copy(far_end, c).wait_recv()
            project_out(far_end, rows_at(c))
            finalize(c)

        loop(chunks, last)

    gain = post_v[...].astype(F32).reshape(1, feats)

    def normalize(c):
        def arrived(s):
            pl.when(s != me)(lambda: ss_copy(s, c, s).wait_recv())

        loop(n - 1, arrived, 1)

        @pl.when(is_end)
        def _():
            end_copy(c).wait_recv()
            stream_o[rows_at(c), :] = landed[rows_at(c), :]

        total = ss_all[1, c] + ss_all[n - 2, c]
        scale = jnp.transpose(lax.rsqrt(total / model + epsilon))[:, 0:1]
        stream = stream_o[rows_at(c), :].astype(F32)
        normed_o[rows_at(c), :] = (stream * scale * gain).astype(BF16)

    loop(chunks, normalize)

    def drain_late(c):
        ctx_copy(near_end, c).wait_send()
        end_copy(c).wait_send()
        loop(n, lambda k: ss_copy(me, c, peer_mp(k)).wait_send(), 1)

    def drain_slices(z):
        def forwarded(k):
            o = from_core(k)
            pl.when(in_plane(o))(lambda: o_copy(z, o, partner, True).wait_send())

        loop(half, forwarded, 1)

    @pl.when(is_inner)
    def _():
        drain_early()
        loop(chunks, drain_late)
        loop(n, drain_slices)


def publish(stream_i, normed_i, stream_o, normed_o, sems):
    copies = (
        pltpu.make_async_copy(stream_i, stream_o, sems.at[0]),
        pltpu.make_async_copy(normed_i, normed_o, sems.at[1]),
    )
    for copy in copies:
        copy.start()
    for copy in copies:
        copy.wait()


def on_device(n, groups, tokens, pre_gain, input_weight, output_weight, position_bias, post_gain):
    rows, feats = tokens.shape
    step = 128
    chunks = rows // step
    inner = input_weight.shape[2]
    model = n * feats
    wide = output_weight.shape[1] % 128 == 0
    if not wide:
        output_weight = output_weight.T
    dma, any_space = pltpu.SemaphoreType.DMA, pl.BlockSpec(memory_space=pl.ANY)
    vmem = pl.BlockSpec(memory_space=pltpu.VMEM)
    if wide and n - 2 == 2:
        pieces = rows // 64
        body = functools.partial(line_kernel, n, groups, chunks)
        scratch = [
            pltpu.VMEM((n, rows, feats), BF16),
            pltpu.VMEM((n * feats,), BF16),
            pltpu.VMEM((feats,), BF16),
            pltpu.VMEM((3, model, inner), BF16),
            pltpu.VMEM(output_weight.shape, BF16),
            pltpu.VMEM((n, groups // 2, inner, output_weight.shape[1]), BF16),
            pltpu.VMEM(position_bias.shape, BF16),
            pltpu.VMEM((3, rows, inner), F32),
            pltpu.VMEM((rows, feats), F32),
            pltpu.VMEM((3, rows, inner), BF16),
            pltpu.VMEM((n, rows, inner), BF16),
            pltpu.VMEM((rows, 2 * feats), F32),
            pltpu.VMEM((rows, feats), BF16),
            pltpu.VMEM((rows, feats), BF16),
            pltpu.VMEM((chunks, 8, step), F32),
            pltpu.VMEM((n, chunks, 8, step), F32),
            dma((2, n, pieces)),
            dma((n, pieces)),
            dma((n,)),
            dma((n,)),
            dma((2, groups)),
            dma((groups,)),
            dma((1,)),
            dma((2, n, groups)),
            dma((n, groups)),
            dma((n, chunks)),
            dma((n, chunks)),
            dma((chunks,)),
            dma((chunks,)),
            dma((n, chunks)),
            dma((n, chunks)),
            dma((6,)),
            pltpu.SemaphoreType.REGULAR((2,)),
        ]
    else:
        body = functools.partial(kernel, n, groups, chunks, wide)
        wo_shape = (inner, model) if wide else (model, inner)
        scratch = [
            pltpu.VMEM((n, rows, feats), BF16),
            pltpu.VMEM((n * feats,), BF16),
            pltpu.VMEM((feats,), BF16),
            pltpu.VMEM((3, model, inner), BF16),
            pltpu.VMEM(wo_shape, BF16),
            pltpu.VMEM(wo_shape, BF16),
            pltpu.VMEM(position_bias.shape, BF16),
            pltpu.VMEM((3, rows, inner), F32),
            pltpu.VMEM((rows, feats), F32),
            pltpu.VMEM((3, rows, inner), BF16),
            pltpu.VMEM((n, rows, feats), F32),
            pltpu.VMEM((n, rows, feats), BF16),
            pltpu.VMEM((2, n, rows, feats), BF16),
            pltpu.VMEM((rows, inner), BF16),
            pltpu.VMEM((rows, inner), BF16),
            pltpu.VMEM((chunks, 8, step), F32),
            pltpu.VMEM((n, chunks, 8, step), F32),
            dma((2, n, chunks)),
            dma((n, chunks)),
            dma((n,)),
            dma((n,)),
            dma((3, 2, groups)),
            dma((3, groups)),
            dma((chunks,)),
            dma((chunks,)),
            dma((n, chunks)),
            dma((2, n, chunks)),
            dma((n, chunks)),
            dma((n, chunks)),
            dma((6,)),
            pltpu.SemaphoreType.REGULAR((2,)),
        ]
    stream, normed = pl.pallas_call(
        body,
        out_shape=(pltpu.VMEM((rows, feats), BF16), pltpu.VMEM((rows, feats), BF16)),
        in_specs=[any_space] * 6,
        out_specs=[vmem] * 2,
        scratch_shapes=scratch,
        compiler_params=pltpu.CompilerParams(
            collective_id=0, has_side_effects=True, vmem_limit_bytes=56 * 1024 * 1024
        ),
    )(tokens, pre_gain, input_weight, output_weight, position_bias, post_gain)
    shape = jax.ShapeDtypeStruct((rows, feats), BF16)
    return pl.pallas_call(
        publish,
        out_shape=(shape, shape),
        in_specs=[vmem] * 2,
        out_specs=[any_space] * 2,
        scratch_shapes=[dma((2,))],
        compiler_params=pltpu.CompilerParams(vmem_limit_bytes=4 * 1024 * 1024),
    )(stream, normed)


def solution(mesh):
    return jax.shard_map(
        functools.partial(on_device, mesh.shape["mp"], mesh.shape["dp"]),
        mesh=mesh,
        in_specs=(
            P("dp", "mp"),
            P("mp"),
            P(None, "dp", "mp"),
            P("mp", "dp"),
            P("mp", None, None),
            P("mp"),
        ),
        out_specs=(P("dp", "mp"), P("dp", "mp")),
        check_vma=False,
    )
```

```python
import functools

import jax
import jax.numpy as jnp
from jax import lax
from jax.experimental import pallas as pl
from jax.experimental.pallas import tpu as pltpu
from jax.sharding import PartitionSpec as P

epsilon = 1e-06
F32, BF16 = jnp.float32, jnp.bfloat16
MESH = pl.DeviceIdType.MESH


def kernel(
    n,
    groups,
    chunks,
    wide,
    tok,
    pre,
    win,
    wout,
    bias,
    post,
    stream_o,
    normed_o,
    x_all,
    gain_all,
    post_v,
    w_all,
    wo_all,
    wo_end,
    bias_v,
    acc,
    square,
    qkv,
    part,
    out_buf,
    landed,
    ctx_buf,
    ctx_in,
    ss_mine,
    ss_all,
    ag_send,
    ag_recv,
    g_send,
    g_recv,
    w_send,
    w_recv,
    ctx_send,
    ctx_recv,
    rs_send,
    rs_recv,
    ss_send,
    ss_recv,
    local_sem,
    link_free,
):
    rows, feats = tok.shape
    step = rows // chunks
    heads, seq = bias.shape[0], bias.shape[1]
    inner = win.shape[2]
    head_dim = inner // heads
    model = n * feats
    wrows = win.shape[1]
    wcols = model // groups
    half = groups // 2
    me = lax.axis_index("mp")
    d = lax.axis_index("dp")
    odd = lax.rem(d, 2)
    pair = d // 2
    partner = d + 1 - 2 * odd
    is_end = (me == 0) | (me == n - 1)
    is_edge = (me == 1) | (me == n - 2)
    all_rows = pl.ds(0, rows)

    def rows_at(c):
        return pl.ds(pl.multiple_of(c * step, step), step)

    def feats_at(s):
        return pl.ds(pl.multiple_of(s * feats, feats), feats)

    def loop(count, body, start=0):
        def wrapped(i, carry):
            body(i)
            return carry

        lax.fori_loop(start, count, wrapped, 0)

    def remote(src, dst, send, recv, target):
        return pltpu.make_async_remote_copy(
            src_ref=src,
            dst_ref=dst,
            send_sem=send,
            recv_sem=recv,
            device_id=target,
            device_id_type=MESH,
        )

    def tok_copy(s, c, up):
        ref = x_all.at[s, rows_at(c)]
        return remote(ref, ref, ag_send.at[up, s, c], ag_recv.at[s, c], {"mp": me + 2 * up - 1})

    def gain_copy(origin, target):
        ref = gain_all.at[feats_at(origin)]
        return remote(ref, ref, g_send.at[target], g_recv.at[origin], {"mp": target})

    def w_slot(o):
        return w_all.at[:, pl.ds(pl.multiple_of(o * wrows, wrows), wrows), :]

    def o_slot(ref, o):
        block = pl.ds(pl.multiple_of(o * wcols, wcols), wcols)
        return ref.at[:, block] if wide else ref.at[block, :]

    def slot(which, o):
        return w_slot(o) if which == 0 else o_slot(wo_all if which == 1 else wo_end, o)

    def weight_copy(which, o, target, forward):
        ref = slot(which, o)
        send = w_send.at[which, 1, o] if forward else w_send.at[which, 0, target]
        return remote(ref, ref, send, w_recv.at[which, o], {"dp": target})

    def cross_copy():
        inwards = jnp.where(me == 0, 1, n - 2)
        return remote(
            o_slot(wo_all, d), o_slot(wo_end, d), w_send.at[2, 0, d], w_recv.at[2, d], {"mp": inwards}
        )

    def ctx_copy(c):
        inwards = jnp.where(me == 0, 1, n - 2)
        return remote(
            ctx_buf.at[rows_at(c)], ctx_in.at[rows_at(c)], ctx_send.at[c], ctx_recv.at[c], {"mp": inwards}
        )

    def rs_copy(s, c, up):
        return remote(
            out_buf.at[s, rows_at(c)],
            landed.at[up, s, rows_at(c)],
            rs_send.at[s, c],
            rs_recv.at[up, s, c],
            {"mp": me + 2 * up - 1},
        )

    def ss_copy(origin, c, target):
        return remote(
            ss_mine.at[c], ss_all.at[origin, c], ss_send.at[target, c], ss_recv.at[origin, c], {"mp": target}
        )

    local = (
        pltpu.make_async_copy(tok, x_all.at[me], local_sem.at[0]),
        pltpu.make_async_copy(pre, gain_all.at[feats_at(me)], local_sem.at[1]),
        pltpu.make_async_copy(win, w_slot(d), local_sem.at[2]),
        pltpu.make_async_copy(wout, o_slot(wo_all, d), local_sem.at[3]),
        pltpu.make_async_copy(post, post_v, local_sem.at[4]),
        pltpu.make_async_copy(bias, bias_v, local_sem.at[5]),
    )
    for copy in local:
        copy.start()

    def peer_mp(k):
        return lax.rem(me + k, n)

    def same_core(k):
        return 2 * lax.rem(pair + k, half) + odd

    def from_core(k):
        return 2 * lax.rem(pair + half - k, half) + odd

    barrier = pltpu.get_barrier_semaphore()

    def greet(target):
        pl.semaphore_signal(barrier, inc=1, device_id=target, device_id_type=MESH)

    loop(n, lambda k: greet({"mp": peer_mp(k)}), 1)
    loop(half, lambda k: greet({"dp": same_core(k)}), 1)
    greet({"dp": partner})
    acc[...] = jnp.zeros_like(acc)
    square[...] = jnp.zeros_like(square)
    for copy in local[:5]:
        copy.wait()
    pl.semaphore_wait(barrier, n - 1 + half - 1 + 1)

    def can_send(up):
        return (me < n - 1) if up else (me > 0)

    def send_own(up):
        @pl.when(can_send(up))
        def _():
            @pl.when(odd == 1)
            def _():
                pl.semaphore_wait(link_free.at[up], 1)

            loop(chunks, lambda c: tok_copy(me, c, up).start())

    def release(up):
        @pl.when(can_send(up))
        def _():
            pl.semaphore_signal(
                link_free.at[up], inc=1, device_id={"dp": partner}, device_id_type=MESH
            )

    def send_weights(which):
        weight_copy(which, d, partner, False).start()
        loop(half, lambda k: weight_copy(which, d, same_core(k), False).start(), 1)

    def forward_weights(which):
        def forward(k):
            o = from_core(k)
            weight_copy(which, o, partner, False).wait_recv()
            weight_copy(which, o, partner, True).start()

        loop(half, forward, 1)

    def other_weights(which):
        loop(half, lambda k: weight_copy(which, 2 * k + 1 - odd, partner, False).wait_recv())

    def pass_end_weights():
        @pl.when(is_edge)
        def _():
            weight_copy(2, d, partner, False).wait_recv()
            send_weights(2)

    def forward_out_weights():
        pl.when(jnp.logical_not(is_end))(lambda: forward_weights(1))
        pl.when(is_edge)(lambda: forward_weights(2))

    def take(up, j, use=None):
        s = me - j if up else me + j

        @pl.when((s >= 0) & (s < n))
        def _():
            def one(c):
                tok_copy(s, c, up).wait_recv()

                @pl.when(can_send(up))
                def _():
                    tok_copy(s, c, up).start()

                if use is not None:
                    use(s, c)

            loop(chunks, one)

    def accumulate(s, at):
        gain = gain_all[feats_at(s)].astype(F32).reshape(1, feats)
        x = x_all[s, at, :].astype(F32)
        square[at, :] += x * x
        xg = (x * gain).astype(BF16)
        for m in range(3):
            acc[m, at, :] += jnp.dot(xg, w_all[m, feats_at(s), :], preferred_element_type=F32)

    def both_ways(action):
        @pl.when(2 * me < n)
        def _():
            action(0)
            action(1)

        @pl.when(2 * me >= n)
        def _():
            action(1)
            action(0)

    def finish(c):
        total = jnp.sum(square[rows_at(c), :], axis=1, keepdims=True)
        inverse = lax.rsqrt(total / model + epsilon)
        for m in range(3):
            qkv[m, rows_at(c), :] = (acc[m, rows_at(c), :] * inverse).astype(BF16)

    def send_all_weights():
        send_weights(0)
        pl.when(is_end)(lambda: cross_copy().start())
        pl.when(jnp.logical_not(is_end))(lambda: send_weights(1))

    def wait_gains():
        loop(n, lambda k: gain_copy(peer_mp(k), peer_mp(k)).wait_recv(), 1)

    def gather_even():
        both_ways(send_own)
        send_all_weights()

        @pl.when(is_end)
        def _():
            up = jnp.where(me == 0, 1, 0)
            loop(chunks, lambda c: tok_copy(me, c, up).wait_send())
            both_ways(release)

        def hop(j):
            def one(c):
                def side(up):
                    s = me - j if up else me + j

                    @pl.when((s >= 0) & (s < n))
                    def _():
                        tok_copy(s, c, up).wait_recv()
                        pl.when(can_send(up))(lambda: tok_copy(s, c, up).start())

                both_ways(side)

            loop(chunks, one)

        loop(n, hop, 1)
        pl.when(jnp.logical_not(is_end))(lambda: both_ways(release))
        pass_end_weights()
        forward_weights(0)
        wait_gains()
        other_weights(0)
        loop(n, lambda s: accumulate(s, all_rows))
        loop(chunks, finish)

    def gather_odd():
        send_all_weights()
        both_ways(send_own)

        def toward(near):
            far = 1 - near
            reach = n - 1 - me if near else me
            loop(n, lambda j: take(near, j), 1)
            pass_end_weights()
            forward_weights(0)
            wait_gains()
            take(far, 1)
            other_weights(0)

            def known(s):
                pl.when((s <= me + 1) if near else (s >= me - 1))(lambda: accumulate(s, all_rows))

            loop(n, known)

            def later(j):
                @pl.when(j < reach)
                def _():
                    take(far, j)
                    accumulate(me + j if near else me - j, all_rows)

            def use(s, c):
                accumulate(s, rows_at(c))
                finish(c)

            loop(n, later, 2)
            pl.when(reach > 1)(lambda: take(far, reach, use))
            pl.when(reach <= 1)(lambda: loop(chunks, finish))

        pl.when(2 * me < n)(lambda: toward(1))
        pl.when(2 * me >= n)(lambda: toward(0))
        forward_out_weights()

    loop(n, lambda k: gain_copy(me, peer_mp(k)).start(), 1)
    pl.when(odd == 0)(gather_even)
    pl.when(odd == 1)(gather_odd)

    local[5].wait()

    lane_head = lax.broadcasted_iota(jnp.int32, (1, inner), 1) // head_dim
    contract = (((1,), (1,)), ((), ()))

    def attend(c):
        first = (c * step) // seq * seq
        keys_at = pl.ds(pl.multiple_of(first, seq), seq)
        bias_at = pl.ds(pl.multiple_of(c * step - first, step), step)
        q = qkv[0, rows_at(c), :]
        k = qkv[1, keys_at, :]
        v = qkv[2, keys_at, :]
        stacked = jnp.concatenate([jnp.where(lane_head == h, q, jnp.zeros_like(q)) for h in range(heads)], axis=0)
        scores = lax.dot_general(stacked, k, contract, preferred_element_type=F32)
        scores = scores + bias_v[:, bias_at, :].reshape(heads * step, seq).astype(F32)
        weights = jnp.exp(scores - jnp.max(scores, axis=1, keepdims=True))
        scale = 1.0 / jnp.sum(weights, axis=1, keepdims=True)
        mixed = jnp.dot(weights.astype(BF16), v, preferred_element_type=F32) * scale
        context = mixed[0:step]
        for h in range(1, heads):
            context = jnp.where(lane_head == h, mixed[h * step : (h + 1) * step], context)
        ctx_buf[rows_at(c), :] = context.astype(BF16)
        pl.when(is_end)(lambda: ctx_copy(c).start())

    loop(chunks, attend)

    def project_out(context, ref, s):
        block = feats_at(s)
        if wide:
            return jnp.dot(context, ref[:, block], preferred_element_type=F32)
        return lax.dot_general(context, ref[block, :], contract, preferred_element_type=F32)

    def send_out(s, c, up, value):
        out_buf[s, rows_at(c), :] = value.astype(BF16)
        rs_copy(s, c, up).start()

    def own_share(s):
        part[s] = project_out(ctx_buf[...], wo_all, s)

    def originate(c):
        ctx_copy(c).wait_recv()
        context = ctx_in[rows_at(c), :]

        def far(k):
            s = jnp.where(me == 1, n - 1 - k, k)
            value = part[s, rows_at(c), :] + project_out(context, wo_end, s)
            send_out(s, c, jnp.where(me == 1, 1, 0), value)

        def near(k):
            s = jnp.where(me == 1, k, n - 2 + k)
            part[s, rows_at(c), :] += project_out(context, wo_end, s)

        loop(n - 2, far)
        loop(2, near)

    def finished(s, c):
        value = x_all[s, rows_at(c), :].astype(F32) + part[s, rows_at(c), :]
        stream = value.astype(BF16)
        wide_stream = stream.astype(F32)
        return stream, wide_stream * wide_stream

    def finalize(c):
        stream, squares = finished(me, c)
        stream_o[rows_at(c), :] = stream
        part[me, rows_at(c), :] = squares

        @pl.when(is_edge)
        def _():
            end, up = jnp.where(me == 1, 0, n - 1), jnp.where(me == 1, 0, 1)
            stream_end, squares_end = finished(end, c)
            out_buf[end, rows_at(c), :] = stream_end
            rs_copy(end, c, up).start()
            part[me, rows_at(c), :] += squares_end

        total = jnp.sum(part[me, rows_at(c), :], axis=1, keepdims=True)
        turned = jnp.transpose(jnp.broadcast_to(total, (step, 128)))
        ss_mine[c] = turned[0:8, :]
        ss_all[me, c] = turned[0:8, :]
        loop(n, lambda k: ss_copy(me, c, peer_mp(k)).start(), 1)

    def combine(c):
        def message(k):
            for up in (1, 0):
                s = n - 1 - k if up else k
                follows = (me >= 2) if up else (me <= n - 3)
                further = (s > me) if up else (s < me)
                last = (me == n - 2) if up else (me == 1)

                @pl.when(follows & (further | (s == me)))
                def _():
                    rs_copy(s, c, up).wait_recv()
                    value = part[s, rows_at(c), :] + landed[up, s, rows_at(c), :].astype(F32)

                    @pl.when((s == me) | last)
                    def _():
                        part[s, rows_at(c), :] = value

                    @pl.when((s != me) & jnp.logical_not(last))
                    def _():
                        send_out(s, c, up, value)

        loop(n - 2, message)
        finalize(c)

    @pl.when(jnp.logical_not(is_end))
    def _():
        pl.when(odd == 0)(forward_out_weights)
        other_weights(1)
        pl.when(is_edge)(lambda: other_weights(2))
        loop(n, own_share)
        pl.when(is_edge)(lambda: loop(chunks, originate))
        loop(chunks, combine)

    gain = post_v[...].astype(F32).reshape(1, feats)

    def normalize(c):
        def arrived(s):
            pl.when(s != me)(lambda: ss_copy(s, c, s).wait_recv())

        loop(n - 1, arrived, 1)

        @pl.when(is_end)
        def _():
            up = jnp.where(me == 0, 0, 1)
            rs_copy(me, c, up).wait_recv()
            stream_o[rows_at(c), :] = landed[up, me, rows_at(c), :]

        total = jnp.zeros((8, step), F32)
        for s in range(1, n - 1):
            total = total + ss_all[s, c]
        scale = jnp.transpose(lax.rsqrt(total / model + epsilon))[:, 0:1]
        stream = stream_o[rows_at(c), :].astype(F32)
        normed_o[rows_at(c), :] = (stream * scale * gain).astype(BF16)

    loop(chunks, normalize)

    loop(n, lambda k: gain_copy(me, peer_mp(k)).wait_send(), 1)

    def drain_tokens(s):
        def one(c):
            waited = (odd == 0) & (s == me) & is_end

            @pl.when((s <= me) & (me < n - 1) & jnp.logical_not(waited))
            def _():
                tok_copy(s, c, 1).wait_send()

            @pl.when((s >= me) & (me > 0) & jnp.logical_not(waited))
            def _():
                tok_copy(s, c, 0).wait_send()

            @pl.when(jnp.logical_not(is_end) & (s != me))
            def _():
                rs_copy(s, c, 1).wait_send()
                ss_copy(me, c, s).wait_send()

        loop(chunks, one)

    loop(n, drain_tokens)

    def drain_weights(which):
        weight_copy(which, d, partner, False).wait_send()

        def drain(k):
            weight_copy(which, d, same_core(k), False).wait_send()
            weight_copy(which, from_core(k), partner, True).wait_send()

        loop(half, drain, 1)

    drain_weights(0)
    pl.when(is_edge)(lambda: drain_weights(2))

    @pl.when(is_end)
    def _():
        cross_copy().wait_send()
        loop(chunks, lambda c: ctx_copy(c).wait_send())

    pl.when(jnp.logical_not(is_end))(lambda: drain_weights(1))


def line_kernel(
    n,
    groups,
    chunks,
    tok,
    pre,
    win,
    wout,
    bias,
    post,
    stream_o,
    normed_o,
    x_all,
    gain_all,
    post_v,
    w_all,
    wo_own,
    wo_all,
    bias_v,
    acc,
    square,
    qkv,
    ctx_all,
    part,
    out_buf,
    landed,
    ss_mine,
    ss_all,
    ag_send,
    ag_recv,
    g_send,
    g_recv,
    w_send,
    w_recv,
    x_send,
    o_send,
    o_recv,
    ctx_send,
    ctx_recv,
    end_send,
    end_recv,
    ss_send,
    ss_recv,
    local_sem,
    link_free,
):
    rows, feats = tok.shape
    step = rows // chunks
    pieces = ag_recv.shape[1]
    piece = rows // pieces
    heads, seq = bias.shape[0], bias.shape[1]
    inner = win.shape[2]
    head_dim = inner // heads
    model = n * feats
    wrows = win.shape[1]
    wcols = model // groups
    half = groups // 2
    me = lax.axis_index("mp")
    d = lax.axis_index("dp")
    odd = lax.rem(d, 2)
    pair = d // 2
    partner = d + 1 - 2 * odd
    low = 2 * me < n
    is_end = (me == 0) | (me == n - 1)
    is_inner = jnp.logical_not(is_end)
    near_end, far_end = jnp.where(low, 0, n - 1), jnp.where(low, n - 1, 0)
    other_inner = n - 1 - me
    inwards = me + jnp.where(low, 1, -1)
    home = jnp.where(d < half, 1, n - 2)
    is_source = me == home
    late_cross = is_end & (home == inwards) & (odd == 1)
    all_rows = pl.ds(0, rows)

    def rows_at(c):
        return pl.ds(pl.multiple_of(c * step, step), step)

    def feats_at(s):
        return pl.ds(pl.multiple_of(s * feats, feats), feats)

    def loop(count, body, start=0):
        def wrapped(i, carry):
            body(i)
            return carry

        lax.fori_loop(start, count, wrapped, 0)

    def remote(src, dst, send, recv, target):
        return pltpu.make_async_remote_copy(
            src_ref=src,
            dst_ref=dst,
            send_sem=send,
            recv_sem=recv,
            device_id=target,
            device_id_type=MESH,
        )

    def tok_copy(s, c, up):
        ref = x_all.at[s, pl.ds(pl.multiple_of(c * piece, piece), piece)]
        return remote(ref, ref, ag_send.at[up, s], ag_recv.at[s, c], {"mp": me + 2 * up - 1})

    def sent(ref, sem):
        remote(ref, ref, sem, ctx_recv.at[0, 0], {"mp": inwards}).wait_send()

    def tokens_sent(s, up):
        sent(x_all.at[s], ag_send.at[up, s])

    def gain_copy(origin, target):
        ref = gain_all.at[feats_at(origin)]
        return remote(ref, ref, g_send.at[0], g_recv.at[0], {"mp": target})

    def all_gains():
        ref = gain_all.at[pl.ds(0, (n - 1) * feats)]
        return remote(ref, ref, g_send.at[0], g_recv.at[0], {"mp": inwards})

    def w_slot(o):
        return w_all.at[:, pl.ds(pl.multiple_of(o * wrows, wrows), wrows), :]

    def w_copy(o, target, forward):
        send = w_send.at[1 if forward else 0]
        return remote(w_slot(o), w_slot(o), send, w_recv.at[o], {"dp": target})

    def o_slot(z, o):
        return wo_all.at[z, lax.rem(o, half)]

    def o_copy(z, o, target, forward):
        send = o_send.at[1 if forward else 0, z]
        return remote(o_slot(z, o), o_slot(z, o), send, o_recv.at[z, lax.rem(o, half)], {"dp": target})

    def cross_copy():
        return remote(wo_own, o_slot(me, d), x_send.at[0], o_recv.at[me, lax.rem(d, half)], {"mp": home})

    def ctx_copy(s, c):
        ref = ctx_all.at[s, rows_at(c)]
        return remote(ref, ref, ctx_send.at[jnp.where(s == me, 0, 1)], ctx_recv.at[s, c], {"mp": inwards})

    def end_copy(c):
        return remote(
            out_buf.at[rows_at(c)], landed.at[rows_at(c)], end_send.at[0], end_recv.at[c], {"mp": near_end}
        )

    def ss_copy(origin, c, target):
        return remote(
            ss_mine.at[c], ss_all.at[origin, c], ss_send.at[0], ss_recv.at[jnp.where(origin == 1, 0, 1), c], {"mp": target}
        )

    tok_in = pltpu.make_async_copy(tok, x_all.at[me], local_sem.at[0])
    win_in = pltpu.make_async_copy(win, w_slot(d), local_sem.at[1])
    pre_in = pltpu.make_async_copy(pre, gain_all.at[feats_at(me)], local_sem.at[2])
    post_in = pltpu.make_async_copy(post, post_v, local_sem.at[3])
    bias_in = pltpu.make_async_copy(bias, bias_v, local_sem.at[4])

    def wout_in(action):
        pl.when(is_source)(lambda: action(pltpu.make_async_copy(wout, o_slot(me, d), local_sem.at[5])))
        pl.when(jnp.logical_not(is_source))(
            lambda: action(pltpu.make_async_copy(wout, wo_own, local_sem.at[5]))
        )

    tok_in.start()
    win_in.start()
    pre_in.start()
    wout_in(lambda copy: copy.start())

    def peer_mp(k):
        return lax.rem(me + k, n)

    def same_core(k):
        return 2 * lax.rem(pair + k, half) + odd

    def from_core(k):
        return 2 * lax.rem(pair + half - k, half) + odd

    barrier = pltpu.get_barrier_semaphore()

    def greet(target):
        pl.semaphore_signal(barrier, inc=1, device_id=target, device_id_type=MESH)

    loop(n, lambda k: greet({"mp": peer_mp(k)}), 1)
    loop(half, lambda k: greet({"dp": same_core(k)}), 1)
    greet({"dp": partner})
    acc[...] = jnp.zeros_like(acc)
    square[...] = jnp.zeros_like(square)
    tok_in.wait()
    post_in.start()
    bias_in.start()
    pl.semaphore_wait(barrier, n - 1 + half - 1 + 1)

    def can_send(up):
        return (me < n - 1) if up else (me > 0)

    def send_own(up):
        @pl.when(can_send(up))
        def _():
            @pl.when(odd == 1)
            def _():
                pl.semaphore_wait(link_free.at[up], 1)

            loop(pieces, lambda c: tok_copy(me, c, up).start())

    def release(up):
        @pl.when(can_send(up))
        def _():
            pl.semaphore_signal(
                link_free.at[up], inc=1, device_id={"dp": partner}, device_id_type=MESH
            )

    def both_ways(action):
        @pl.when(low)
        def _():
            action(0)
            action(1)

        @pl.when(jnp.logical_not(low))
        def _():
            action(1)
            action(0)

    def in_plane(o):
        return (o < half) == (me == 1)

    def send_slice(z):
        o_copy(z, d, partner, False).start()
        loop(half, lambda k: o_copy(z, d, same_core(k), False).start(), 1)

    def relay_slice(z):
        @pl.when(is_source)
        def _():
            o_copy(z, d, partner, False).wait_recv()
            send_slice(z)

    def forward_slices(z):
        def forward(k):
            o = from_core(k)

            @pl.when(in_plane(o))
            def _():
                o_copy(z, o, partner, False).wait_recv()
                o_copy(z, o, partner, True).start()

        loop(half, forward, 1)

    def other_slices(z):
        def other(k):
            o = 2 * k + 1 - odd
            pl.when(in_plane(o))(lambda: o_copy(z, o, partner, False).wait_recv())

        loop(half, other)

    def send_weights():
        win_in.wait()
        w_copy(d, partner, False).start()
        loop(half, lambda k: w_copy(d, same_core(k), False).start(), 1)
        pre_in.wait()
        loop(n, lambda k: gain_copy(me, peer_mp(k)).start(), 1)
        wout_in(lambda copy: copy.wait())
        pl.when(is_source)(lambda: send_slice(me))
        pl.when(jnp.logical_not(is_source | late_cross))(lambda: cross_copy().start())

    def forward_weights():
        def forward(k):
            o = from_core(k)
            w_copy(o, partner, False).wait_recv()
            w_copy(o, partner, True).start()

        loop(half, forward, 1)
        all_gains().wait_recv()

    def other_weights():
        loop(half, lambda k: w_copy(2 * k + 1 - odd, partner, False).wait_recv())

    def take(up, j, use=None):
        s = me - j if up else me + j

        @pl.when((s >= 0) & (s < n))
        def _():
            def one(c):
                tok_copy(s, c, up).wait_recv()
                pl.when(can_send(up))(lambda: tok_copy(s, c, up).start())

            if use is None:
                loop(pieces, one)
            else:
                per = pieces // chunks

                def block(c):
                    loop(per, lambda i: one(c * per + i))
                    use(s, c)

                loop(chunks, block)

    def accumulate(s, at):
        gain = gain_all[feats_at(s)].astype(F32).reshape(1, feats)
        x = x_all[s, at, :].astype(F32)
        square[at, :] += x * x
        xg = (x * gain).astype(BF16)
        for m in range(3):
            acc[m, at, :] += jnp.dot(xg, w_all[m, feats_at(s), :], preferred_element_type=F32)

    def finish(c):
        total = jnp.sum(square[rows_at(c), :], axis=1, keepdims=True)
        inverse = lax.rsqrt(total / model + epsilon)
        for m in range(3):
            qkv[m, rows_at(c), :] = (acc[m, rows_at(c), :] * inverse).astype(BF16)

    def gather_by_shard(near):
        far = 1 - near
        reach = n - 1 - me if near else me
        loop(n, lambda j: take(near, j), 1)
        pl.when(late_cross)(lambda: cross_copy().start())
        forward_weights()
        relay_slice(near_end)
        relay_slice(far_end)
        relay_slice(other_inner)
        take(far, 1)
        other_weights()

        def known(s):
            pl.when((s <= me + 1) if near else (s >= me - 1))(lambda: accumulate(s, all_rows))

        loop(n, known)

        def later(j):
            @pl.when(j < reach)
            def _():
                take(far, j)
                accumulate(me + j if near else me - j, all_rows)

        def use(s, c):
            accumulate(s, rows_at(c))
            finish(c)

        loop(n, later, 2)
        take(far, reach, use)

    def by_shard():
        pl.when(low)(lambda: gather_by_shard(1))
        pl.when(jnp.logical_not(low))(lambda: gather_by_shard(0))

    def gather_even():
        both_ways(send_own)
        send_weights()

        @pl.when(is_end)
        def _():
            up = jnp.where(me == 0, 1, 0)
            tokens_sent(me, up)
            both_ways(release)
            by_shard()

        def hop(j, start=0, stop=pieces):
            def one(c):
                def side(up):
                    s = me - j if up else me + j

                    @pl.when((s >= 0) & (s < n))
                    def _():
                        tok_copy(s, c, up).wait_recv()
                        pl.when(can_send(up))(lambda: tok_copy(s, c, up).start())

                both_ways(side)

            loop(stop, one, start)

        @pl.when(is_inner)
        def _():
            hop(1)
            pl.when(low)(lambda: release(0))
            pl.when(jnp.logical_not(low))(lambda: release(1))
            hop(2, 0, pieces // 2)
            pl.when(low)(lambda: release(1))
            pl.when(jnp.logical_not(low))(lambda: release(0))
            hop(2, pieces // 2)
            forward_weights()
            relay_slice(near_end)
            relay_slice(far_end)
            relay_slice(other_inner)
            other_weights()
            loop(n, lambda s: accumulate(s, all_rows))
            loop(chunks, finish)
            forward_slices(me)

    def gather_odd():
        send_weights()
        both_ways(send_own)
        by_shard()

        @pl.when(is_inner)
        def _():
            forward_slices(me)
            forward_slices(near_end)
            forward_slices(far_end)

    pl.when(odd == 0)(gather_even)
    pl.when(odd == 1)(gather_odd)
    post_in.wait()
    bias_in.wait()

    lane_head = lax.broadcasted_iota(jnp.int32, (1, inner), 1) // head_dim
    contract = (((1,), (1,)), ((), ()))

    def attend(c):
        first = (c * step) // seq * seq
        keys_at = pl.ds(first, seq)
        bias_at = pl.ds(c * step - first, step)
        q = qkv[0, rows_at(c), :]
        k = qkv[1, keys_at, :]
        v = qkv[2, keys_at, :]
        stacked = jnp.concatenate([jnp.where(lane_head == h, q, jnp.zeros_like(q)) for h in range(heads)], axis=0)
        scores = lax.dot_general(stacked, k, contract, preferred_element_type=F32)
        scores = scores + bias_v[:, bias_at, :].reshape(heads * step, seq).astype(F32)
        weights = jnp.exp(scores - jnp.max(scores, axis=1, keepdims=True))
        scale = 1.0 / jnp.sum(weights, axis=1, keepdims=True)
        mixed = jnp.dot(weights.astype(BF16), v, preferred_element_type=F32) * scale
        context = mixed[0:step]
        for h in range(1, heads):
            context = jnp.where(lane_head == h, mixed[h * step : (h + 1) * step], context)
        ctx_all[me, rows_at(c), :] = context.astype(BF16)

    for c in range(0, chunks, 2):
        together = range(c, min(c + 2, chunks))
        for i in together:
            attend(i)
        for i in together:
            ctx_copy(me, i).start()

    def drain_line(s):
        waited = (odd == 0) & (s == me) & is_end

        @pl.when((s <= me) & (me < n - 1) & jnp.logical_not(waited))
        def _():
            tokens_sent(s, 1)

        @pl.when((s >= me) & (me > 0) & jnp.logical_not(waited))
        def _():
            tokens_sent(s, 0)

        @pl.when(is_source)
        def _():
            sent(wo_all.at[s], o_send.at[0, s])

    def drain_early():
        all_gains().wait_send()
        loop(n, drain_line)
        sent(w_all.at[:, pl.ds(0, half * wrows), :], w_send.at[0])
        sent(w_all.at[:, pl.ds(0, (half - 1) * wrows), :], w_send.at[1])
        pl.when(jnp.logical_not(is_source))(lambda: cross_copy().wait_send())
        sent(ctx_all.at[me], ctx_send.at[0])

    def project_out(s, at, first=False):
        weight = jnp.concatenate([wo_all[s, i] for i in range(wo_all.shape[1])], axis=1)
        value = jnp.dot(ctx_all[s, at, :], weight, preferred_element_type=F32)
        part[at, :] = value if first else part[at, :] + value

    def pass_on(c):
        ctx_copy(near_end, c).wait_recv()
        ctx_copy(near_end, c).start()

    def finalize(c):
        def block(s, at):
            stream = (x_all[s, rows_at(c), :].astype(F32) + part[rows_at(c), at]).astype(BF16)
            wide_stream = stream.astype(F32)
            return stream, wide_stream * wide_stream

        def both(own_at, end_at):
            stream_end, squares_end = block(near_end, end_at)
            out_buf[rows_at(c), :] = stream_end
            end_copy(c).start()
            stream, squares = block(me, own_at)
            stream_o[rows_at(c), :] = stream
            total = jnp.sum(squares + squares_end, axis=1, keepdims=True)
            turned = jnp.transpose(jnp.broadcast_to(total, (step, 128)))
            ss_mine[c] = turned[0:8, :]
            ss_all[me, c] = turned[0:8, :]

        pl.when(low)(lambda: both(pl.ds(feats, feats), pl.ds(0, feats)))
        pl.when(jnp.logical_not(low))(lambda: both(pl.ds(0, feats), pl.ds(feats, feats)))
        loop(n, lambda k: ss_copy(me, c, peer_mp(k)).start(), 1)

    pl.when(is_end)(drain_early)

    @pl.when(is_inner)
    def _():
        @pl.when(odd == 0)
        def _():
            forward_slices(near_end)
            forward_slices(far_end)

        pl.when(odd == 1)(lambda: forward_slices(other_inner))
        other_slices(me)
        project_out(me, all_rows, True)
        other_slices(near_end)
        def near(c):
            pass_on(c)
            project_out(near_end, rows_at(c))

        loop(chunks // 2, near)
        pl.when(odd == 0)(lambda: forward_slices(other_inner))
        loop(chunks, near, chunks // 2)
        other_slices(other_inner)
        loop(chunks, lambda c: ctx_copy(other_inner, c).wait_recv())
        project_out(other_inner, all_rows)
        other_slices(far_end)

        def last(c):
            ctx_copy(far_end, c).wait_recv()
            project_out(far_end, rows_at(c))
            finalize(c)

        loop(chunks, last)

    gain = post_v[...].astype(F32).reshape(1, feats)

    def normalize(c):
        def arrived(s):
            pl.when(s != me)(lambda: ss_copy(s, c, s).wait_recv())

        loop(n - 1, arrived, 1)

        @pl.when(is_end)
        def _():
            end_copy(c).wait_recv()
            stream_o[rows_at(c), :] = landed[rows_at(c), :]

        total = ss_all[1, c] + ss_all[n - 2, c]
        scale = jnp.transpose(lax.rsqrt(total / model + epsilon))[:, 0:1]
        stream = stream_o[rows_at(c), :].astype(F32)
        normed_o[rows_at(c), :] = (stream * scale * gain).astype(BF16)

    loop(chunks, normalize)

    def drain_slices(z):
        spreads = is_source
        pl.when(spreads)(lambda: sent(wo_all.at[z, pl.ds(0, half // 2 - 1)], o_send.at[1, z]))
        pl.when(jnp.logical_not(spreads))(lambda: sent(wo_all.at[z, pl.ds(0, half // 2)], o_send.at[1, z]))

    @pl.when(is_inner)
    def _():
        drain_early()
        sent(ctx_all.at[near_end], ctx_send.at[1])
        sent(out_buf, end_send.at[0])
        sent(ss_all.at[pl.ds(0, n - 1)], ss_send.at[0])
        loop(n, drain_slices)


def publish(stream_i, normed_i, stream_o, normed_o, sems):
    copies = (
        pltpu.make_async_copy(stream_i, stream_o, sems.at[0]),
        pltpu.make_async_copy(normed_i, normed_o, sems.at[1]),
    )
    for copy in copies:
        copy.start()
    for copy in copies:
        copy.wait()


def on_device(n, groups, tokens, pre_gain, input_weight, output_weight, position_bias, post_gain):
    rows, feats = tokens.shape
    step = 128
    chunks = rows // step
    inner = input_weight.shape[2]
    model = n * feats
    wide = output_weight.shape[1] % 128 == 0
    if not wide:
        output_weight = output_weight.T
    dma, any_space = pltpu.SemaphoreType.DMA, pl.BlockSpec(memory_space=pl.ANY)
    vmem = pl.BlockSpec(memory_space=pltpu.VMEM)
    if wide and n - 2 == 2:
        pieces = rows // 64
        body = functools.partial(line_kernel, n, groups, chunks)
        scratch = [
            pltpu.VMEM((n, rows, feats), BF16),
            pltpu.VMEM((n * feats,), BF16),
            pltpu.VMEM((feats,), BF16),
            pltpu.VMEM((3, model, inner), BF16),
            pltpu.VMEM(output_weight.shape, BF16),
            pltpu.VMEM((n, groups // 2, inner, output_weight.shape[1]), BF16),
            pltpu.VMEM(position_bias.shape, BF16),
            pltpu.VMEM((3, rows, inner), F32),
            pltpu.VMEM((rows, feats), F32),
            pltpu.VMEM((3, rows, inner), BF16),
            pltpu.VMEM((n, rows, inner), BF16),
            pltpu.VMEM((rows, 2 * feats), F32),
            pltpu.VMEM((rows, feats), BF16),
            pltpu.VMEM((rows, feats), BF16),
            pltpu.VMEM((chunks, 8, step), F32),
            pltpu.VMEM((n, chunks, 8, step), F32),
            dma((2, n)),
            dma((n, pieces)),
            dma((1,)),
            dma((1,)),
            dma((2,)),
            dma((groups,)),
            dma((1,)),
            dma((2, n)),
            dma((n, groups // 2)),
            dma((2,)),
            dma((n, chunks)),
            dma((1,)),
            dma((chunks,)),
            dma((1,)),
            dma((2, chunks)),
            dma((6,)),
            pltpu.SemaphoreType.REGULAR((2,)),
        ]
    else:
        body = functools.partial(kernel, n, groups, chunks, wide)
        wo_shape = (inner, model) if wide else (model, inner)
        scratch = [
            pltpu.VMEM((n, rows, feats), BF16),
            pltpu.VMEM((n * feats,), BF16),
            pltpu.VMEM((feats,), BF16),
            pltpu.VMEM((3, model, inner), BF16),
            pltpu.VMEM(wo_shape, BF16),
            pltpu.VMEM(wo_shape, BF16),
            pltpu.VMEM(position_bias.shape, BF16),
            pltpu.VMEM((3, rows, inner), F32),
            pltpu.VMEM((rows, feats), F32),
            pltpu.VMEM((3, rows, inner), BF16),
            pltpu.VMEM((n, rows, feats), F32),
            pltpu.VMEM((n, rows, feats), BF16),
            pltpu.VMEM((2, n, rows, feats), BF16),
            pltpu.VMEM((rows, inner), BF16),
            pltpu.VMEM((rows, inner), BF16),
            pltpu.VMEM((chunks, 8, step), F32),
            pltpu.VMEM((n, chunks, 8, step), F32),
            dma((2, n, chunks)),
            dma((n, chunks)),
            dma((n,)),
            dma((n,)),
            dma((3, 2, groups)),
            dma((3, groups)),
            dma((chunks,)),
            dma((chunks,)),
            dma((n, chunks)),
            dma((2, n, chunks)),
            dma((n, chunks)),
            dma((n, chunks)),
            dma((6,)),
            pltpu.SemaphoreType.REGULAR((2,)),
        ]
    stream, normed = pl.pallas_call(
        body,
        out_shape=(pltpu.VMEM((rows, feats), BF16), pltpu.VMEM((rows, feats), BF16)),
        in_specs=[any_space] * 6,
        out_specs=[vmem] * 2,
        scratch_shapes=scratch,
        compiler_params=pltpu.CompilerParams(
            collective_id=0, has_side_effects=True, vmem_limit_bytes=56 * 1024 * 1024
        ),
    )(tokens, pre_gain, input_weight, output_weight, position_bias, post_gain)
    shape = jax.ShapeDtypeStruct((rows, feats), BF16)
    return pl.pallas_call(
        publish,
        out_shape=(shape, shape),
        in_specs=[vmem] * 2,
        out_specs=[any_space] * 2,
        scratch_shapes=[dma((2,))],
        compiler_params=pltpu.CompilerParams(vmem_limit_bytes=4 * 1024 * 1024),
    )(stream, normed)


def solution(mesh):
    return jax.shard_map(
        functools.partial(on_device, mesh.shape["mp"], mesh.shape["dp"]),
        mesh=mesh,
        in_specs=(
            P("dp", "mp"),
            P("mp"),
            P(None, "dp", "mp"),
            P("mp", "dp"),
            P("mp", None, None),
            P("mp"),
        ),
        out_specs=(P("dp", "mp"), P("dp", "mp")),
        check_vma=False,
    )
```

```python
import functools

import jax
import jax.numpy as jnp
from jax import lax
from jax.experimental import pallas as pl
from jax.experimental.pallas import tpu as pltpu
from jax.sharding import PartitionSpec as P

epsilon = 1e-06
F32, BF16 = jnp.float32, jnp.bfloat16
MESH = pl.DeviceIdType.MESH


def kernel(
    n,
    groups,
    chunks,
    wide,
    tok,
    pre,
    win,
    wout,
    bias,
    post,
    stream_o,
    normed_o,
    x_all,
    gain_all,
    post_v,
    w_all,
    wo_all,
    wo_end,
    bias_v,
    acc,
    square,
    qkv,
    part,
    out_buf,
    landed,
    ctx_buf,
    ctx_in,
    ss_mine,
    ss_all,
    ag_send,
    ag_recv,
    g_send,
    g_recv,
    w_send,
    w_recv,
    ctx_send,
    ctx_recv,
    rs_send,
    rs_recv,
    ss_send,
    ss_recv,
    local_sem,
    link_free,
):
    rows, feats = tok.shape
    step = rows // chunks
    heads, seq = bias.shape[0], bias.shape[1]
    inner = win.shape[2]
    head_dim = inner // heads
    model = n * feats
    wrows = win.shape[1]
    wcols = model // groups
    half = groups // 2
    me = lax.axis_index("mp")
    d = lax.axis_index("dp")
    odd = lax.rem(d, 2)
    pair = d // 2
    partner = d + 1 - 2 * odd
    is_end = (me == 0) | (me == n - 1)
    is_edge = (me == 1) | (me == n - 2)
    all_rows = pl.ds(0, rows)

    def rows_at(c):
        return pl.ds(pl.multiple_of(c * step, step), step)

    def feats_at(s):
        return pl.ds(pl.multiple_of(s * feats, feats), feats)

    def loop(count, body, start=0):
        def wrapped(i, carry):
            body(i)
            return carry

        lax.fori_loop(start, count, wrapped, 0)

    def remote(src, dst, send, recv, target):
        return pltpu.make_async_remote_copy(
            src_ref=src,
            dst_ref=dst,
            send_sem=send,
            recv_sem=recv,
            device_id=target,
            device_id_type=MESH,
        )

    def tok_copy(s, c, up):
        ref = x_all.at[s, rows_at(c)]
        return remote(ref, ref, ag_send.at[up, s, c], ag_recv.at[s, c], {"mp": me + 2 * up - 1})

    def gain_copy(origin, target):
        ref = gain_all.at[feats_at(origin)]
        return remote(ref, ref, g_send.at[target], g_recv.at[origin], {"mp": target})

    def w_slot(o):
        return w_all.at[:, pl.ds(pl.multiple_of(o * wrows, wrows), wrows), :]

    def o_slot(ref, o):
        block = pl.ds(pl.multiple_of(o * wcols, wcols), wcols)
        return ref.at[:, block] if wide else ref.at[block, :]

    def slot(which, o):
        return w_slot(o) if which == 0 else o_slot(wo_all if which == 1 else wo_end, o)

    def weight_copy(which, o, target, forward):
        ref = slot(which, o)
        send = w_send.at[which, 1, o] if forward else w_send.at[which, 0, target]
        return remote(ref, ref, send, w_recv.at[which, o], {"dp": target})

    def cross_copy():
        inwards = jnp.where(me == 0, 1, n - 2)
        return remote(
            o_slot(wo_all, d), o_slot(wo_end, d), w_send.at[2, 0, d], w_recv.at[2, d], {"mp": inwards}
        )

    def ctx_copy(c):
        inwards = jnp.where(me == 0, 1, n - 2)
        return remote(
            ctx_buf.at[rows_at(c)], ctx_in.at[rows_at(c)], ctx_send.at[c], ctx_recv.at[c], {"mp": inwards}
        )

    def rs_copy(s, c, up):
        return remote(
            out_buf.at[s, rows_at(c)],
            landed.at[up, s, rows_at(c)],
            rs_send.at[s, c],
            rs_recv.at[up, s, c],
            {"mp": me + 2 * up - 1},
        )

    def ss_copy(origin, c, target):
        return remote(
            ss_mine.at[c], ss_all.at[origin, c], ss_send.at[target, c], ss_recv.at[origin, c], {"mp": target}
        )

    local = (
        pltpu.make_async_copy(tok, x_all.at[me], local_sem.at[0]),
        pltpu.make_async_copy(pre, gain_all.at[feats_at(me)], local_sem.at[1]),
        pltpu.make_async_copy(win, w_slot(d), local_sem.at[2]),
        pltpu.make_async_copy(wout, o_slot(wo_all, d), local_sem.at[3]),
        pltpu.make_async_copy(post, post_v, local_sem.at[4]),
        pltpu.make_async_copy(bias, bias_v, local_sem.at[5]),
    )
    for copy in local:
        copy.start()

    def peer_mp(k):
        return lax.rem(me + k, n)

    def same_core(k):
        return 2 * lax.rem(pair + k, half) + odd

    def from_core(k):
        return 2 * lax.rem(pair + half - k, half) + odd

    barrier = pltpu.get_barrier_semaphore()

    def greet(target):
        pl.semaphore_signal(barrier, inc=1, device_id=target, device_id_type=MESH)

    loop(n, lambda k: greet({"mp": peer_mp(k)}), 1)
    loop(half, lambda k: greet({"dp": same_core(k)}), 1)
    greet({"dp": partner})
    acc[...] = jnp.zeros_like(acc)
    square[...] = jnp.zeros_like(square)
    for copy in local[:5]:
        copy.wait()
    pl.semaphore_wait(barrier, n - 1 + half - 1 + 1)

    def can_send(up):
        return (me < n - 1) if up else (me > 0)

    def send_own(up):
        @pl.when(can_send(up))
        def _():
            @pl.when(odd == 1)
            def _():
                pl.semaphore_wait(link_free.at[up], 1)

            loop(chunks, lambda c: tok_copy(me, c, up).start())

    def release(up):
        @pl.when(can_send(up))
        def _():
            pl.semaphore_signal(
                link_free.at[up], inc=1, device_id={"dp": partner}, device_id_type=MESH
            )

    def send_weights(which):
        weight_copy(which, d, partner, False).start()
        loop(half, lambda k: weight_copy(which, d, same_core(k), False).start(), 1)

    def forward_weights(which):
        def forward(k):
            o = from_core(k)
            weight_copy(which, o, partner, False).wait_recv()
            weight_copy(which, o, partner, True).start()

        loop(half, forward, 1)

    def other_weights(which):
        loop(half, lambda k: weight_copy(which, 2 * k + 1 - odd, partner, False).wait_recv())

    def pass_end_weights():
        @pl.when(is_edge)
        def _():
            weight_copy(2, d, partner, False).wait_recv()
            send_weights(2)

    def forward_out_weights():
        pl.when(jnp.logical_not(is_end))(lambda: forward_weights(1))
        pl.when(is_edge)(lambda: forward_weights(2))

    def take(up, j, use=None):
        s = me - j if up else me + j

        @pl.when((s >= 0) & (s < n))
        def _():
            def one(c):
                tok_copy(s, c, up).wait_recv()

                @pl.when(can_send(up))
                def _():
                    tok_copy(s, c, up).start()

                if use is not None:
                    use(s, c)

            loop(chunks, one)

    def accumulate(s, at):
        gain = gain_all[feats_at(s)].astype(F32).reshape(1, feats)
        x = x_all[s, at, :].astype(F32)
        square[at, :] += x * x
        xg = (x * gain).astype(BF16)
        for m in range(3):
            acc[m, at, :] += jnp.dot(xg, w_all[m, feats_at(s), :], preferred_element_type=F32)

    def both_ways(action):
        @pl.when(2 * me < n)
        def _():
            action(0)
            action(1)

        @pl.when(2 * me >= n)
        def _():
            action(1)
            action(0)

    def finish(c):
        total = jnp.sum(square[rows_at(c), :], axis=1, keepdims=True)
        inverse = lax.rsqrt(total / model + epsilon)
        for m in range(3):
            qkv[m, rows_at(c), :] = (acc[m, rows_at(c), :] * inverse).astype(BF16)

    def send_all_weights():
        send_weights(0)
        pl.when(is_end)(lambda: cross_copy().start())
        pl.when(jnp.logical_not(is_end))(lambda: send_weights(1))

    def wait_gains():
        loop(n, lambda k: gain_copy(peer_mp(k), peer_mp(k)).wait_recv(), 1)

    def gather_even():
        both_ways(send_own)
        send_all_weights()

        @pl.when(is_end)
        def _():
            up = jnp.where(me == 0, 1, 0)
            loop(chunks, lambda c: tok_copy(me, c, up).wait_send())
            both_ways(release)

        def hop(j):
            def one(c):
                def side(up):
                    s = me - j if up else me + j

                    @pl.when((s >= 0) & (s < n))
                    def _():
                        tok_copy(s, c, up).wait_recv()
                        pl.when(can_send(up))(lambda: tok_copy(s, c, up).start())

                both_ways(side)

            loop(chunks, one)

        loop(n, hop, 1)
        pl.when(jnp.logical_not(is_end))(lambda: both_ways(release))
        pass_end_weights()
        forward_weights(0)
        wait_gains()
        other_weights(0)
        loop(n, lambda s: accumulate(s, all_rows))
        loop(chunks, finish)

    def gather_odd():
        send_all_weights()
        both_ways(send_own)

        def toward(near):
            far = 1 - near
            reach = n - 1 - me if near else me
            loop(n, lambda j: take(near, j), 1)
            pass_end_weights()
            forward_weights(0)
            wait_gains()
            take(far, 1)
            other_weights(0)

            def known(s):
                pl.when((s <= me + 1) if near else (s >= me - 1))(lambda: accumulate(s, all_rows))

            loop(n, known)

            def later(j):
                @pl.when(j < reach)
                def _():
                    take(far, j)
                    accumulate(me + j if near else me - j, all_rows)

            def use(s, c):
                accumulate(s, rows_at(c))
                finish(c)

            loop(n, later, 2)
            pl.when(reach > 1)(lambda: take(far, reach, use))
            pl.when(reach <= 1)(lambda: loop(chunks, finish))

        pl.when(2 * me < n)(lambda: toward(1))
        pl.when(2 * me >= n)(lambda: toward(0))
        forward_out_weights()

    loop(n, lambda k: gain_copy(me, peer_mp(k)).start(), 1)
    pl.when(odd == 0)(gather_even)
    pl.when(odd == 1)(gather_odd)

    local[5].wait()

    lane_head = lax.broadcasted_iota(jnp.int32, (1, inner), 1) // head_dim
    contract = (((1,), (1,)), ((), ()))

    def attend(c):
        first = (c * step) // seq * seq
        keys_at = pl.ds(pl.multiple_of(first, seq), seq)
        bias_at = pl.ds(pl.multiple_of(c * step - first, step), step)
        q = qkv[0, rows_at(c), :]
        k = qkv[1, keys_at, :]
        v = qkv[2, keys_at, :]
        stacked = jnp.concatenate([jnp.where(lane_head == h, q, jnp.zeros_like(q)) for h in range(heads)], axis=0)
        scores = lax.dot_general(stacked, k, contract, preferred_element_type=F32)
        scores = scores + bias_v[:, bias_at, :].reshape(heads * step, seq).astype(F32)
        weights = jnp.exp(scores - jnp.max(scores, axis=1, keepdims=True))
        scale = 1.0 / jnp.sum(weights, axis=1, keepdims=True)
        mixed = jnp.dot(weights.astype(BF16), v, preferred_element_type=F32) * scale
        context = mixed[0:step]
        for h in range(1, heads):
            context = jnp.where(lane_head == h, mixed[h * step : (h + 1) * step], context)
        ctx_buf[rows_at(c), :] = context.astype(BF16)
        pl.when(is_end)(lambda: ctx_copy(c).start())

    loop(chunks, attend)

    def project_out(context, ref, s):
        block = feats_at(s)
        if wide:
            return jnp.dot(context, ref[:, block], preferred_element_type=F32)
        return lax.dot_general(context, ref[block, :], contract, preferred_element_type=F32)

    def send_out(s, c, up, value):
        out_buf[s, rows_at(c), :] = value.astype(BF16)
        rs_copy(s, c, up).start()

    def own_share(s):
        part[s] = project_out(ctx_buf[...], wo_all, s)

    def originate(c):
        ctx_copy(c).wait_recv()
        context = ctx_in[rows_at(c), :]

        def far(k):
            s = jnp.where(me == 1, n - 1 - k, k)
            value = part[s, rows_at(c), :] + project_out(context, wo_end, s)
            send_out(s, c, jnp.where(me == 1, 1, 0), value)

        def near(k):
            s = jnp.where(me == 1, k, n - 2 + k)
            part[s, rows_at(c), :] += project_out(context, wo_end, s)

        loop(n - 2, far)
        loop(2, near)

    def finished(s, c):
        value = x_all[s, rows_at(c), :].astype(F32) + part[s, rows_at(c), :]
        stream = value.astype(BF16)
        wide_stream = stream.astype(F32)
        return stream, wide_stream * wide_stream

    def finalize(c):
        stream, squares = finished(me, c)
        stream_o[rows_at(c), :] = stream
        part[me, rows_at(c), :] = squares

        @pl.when(is_edge)
        def _():
            end, up = jnp.where(me == 1, 0, n - 1), jnp.where(me == 1, 0, 1)
            stream_end, squares_end = finished(end, c)
            out_buf[end, rows_at(c), :] = stream_end
            rs_copy(end, c, up).start()
            part[me, rows_at(c), :] += squares_end

        total = jnp.sum(part[me, rows_at(c), :], axis=1, keepdims=True)
        turned = jnp.transpose(jnp.broadcast_to(total, (step, 128)))
        ss_mine[c] = turned[0:8, :]
        ss_all[me, c] = turned[0:8, :]
        loop(n, lambda k: ss_copy(me, c, peer_mp(k)).start(), 1)

    def combine(c):
        def message(k):
            for up in (1, 0):
                s = n - 1 - k if up else k
                follows = (me >= 2) if up else (me <= n - 3)
                further = (s > me) if up else (s < me)
                last = (me == n - 2) if up else (me == 1)

                @pl.when(follows & (further | (s == me)))
                def _():
                    rs_copy(s, c, up).wait_recv()
                    value = part[s, rows_at(c), :] + landed[up, s, rows_at(c), :].astype(F32)

                    @pl.when((s == me) | last)
                    def _():
                        part[s, rows_at(c), :] = value

                    @pl.when((s != me) & jnp.logical_not(last))
                    def _():
                        send_out(s, c, up, value)

        loop(n - 2, message)
        finalize(c)

    @pl.when(jnp.logical_not(is_end))
    def _():
        pl.when(odd == 0)(forward_out_weights)
        other_weights(1)
        pl.when(is_edge)(lambda: other_weights(2))
        loop(n, own_share)
        pl.when(is_edge)(lambda: loop(chunks, originate))
        loop(chunks, combine)

    gain = post_v[...].astype(F32).reshape(1, feats)

    def normalize(c):
        def arrived(s):
            pl.when(s != me)(lambda: ss_copy(s, c, s).wait_recv())

        loop(n - 1, arrived, 1)

        @pl.when(is_end)
        def _():
            up = jnp.where(me == 0, 0, 1)
            rs_copy(me, c, up).wait_recv()
            stream_o[rows_at(c), :] = landed[up, me, rows_at(c), :]

        total = jnp.zeros((8, step), F32)
        for s in range(1, n - 1):
            total = total + ss_all[s, c]
        scale = jnp.transpose(lax.rsqrt(total / model + epsilon))[:, 0:1]
        stream = stream_o[rows_at(c), :].astype(F32)
        normed_o[rows_at(c), :] = (stream * scale * gain).astype(BF16)

    loop(chunks, normalize)

    loop(n, lambda k: gain_copy(me, peer_mp(k)).wait_send(), 1)

    def drain_tokens(s):
        def one(c):
            waited = (odd == 0) & (s == me) & is_end

            @pl.when((s <= me) & (me < n - 1) & jnp.logical_not(waited))
            def _():
                tok_copy(s, c, 1).wait_send()

            @pl.when((s >= me) & (me > 0) & jnp.logical_not(waited))
            def _():
                tok_copy(s, c, 0).wait_send()

            @pl.when(jnp.logical_not(is_end) & (s != me))
            def _():
                rs_copy(s, c, 1).wait_send()
                ss_copy(me, c, s).wait_send()

        loop(chunks, one)

    loop(n, drain_tokens)

    def drain_weights(which):
        weight_copy(which, d, partner, False).wait_send()

        def drain(k):
            weight_copy(which, d, same_core(k), False).wait_send()
            weight_copy(which, from_core(k), partner, True).wait_send()

        loop(half, drain, 1)

    drain_weights(0)
    pl.when(is_edge)(lambda: drain_weights(2))

    @pl.when(is_end)
    def _():
        cross_copy().wait_send()
        loop(chunks, lambda c: ctx_copy(c).wait_send())

    pl.when(jnp.logical_not(is_end))(lambda: drain_weights(1))


def line_kernel(
    n,
    groups,
    chunks,
    tok,
    pre,
    win,
    wout,
    bias,
    post,
    stream_o,
    normed_o,
    x_all,
    gain_all,
    post_v,
    w_all,
    wo_own,
    wo_all,
    bias_v,
    acc,
    square,
    qkv,
    ctx_all,
    part,
    out_buf,
    landed,
    ss_mine,
    ss_all,
    ag_send,
    ag_recv,
    g_send,
    g_recv,
    w_send,
    w_recv,
    x_send,
    o_send,
    o_recv,
    ctx_send,
    ctx_recv,
    end_send,
    end_recv,
    ss_send,
    ss_recv,
    local_sem,
    link_free,
):
    rows, feats = tok.shape
    step = rows // chunks
    pieces = ag_recv.shape[1]
    piece = rows // pieces
    heads, seq = bias.shape[0], bias.shape[1]
    inner = win.shape[2]
    head_dim = inner // heads
    model = n * feats
    wrows = win.shape[1]
    wcols = model // groups
    half = groups // 2
    me = lax.axis_index("mp")
    d = lax.axis_index("dp")
    odd = lax.rem(d, 2)
    pair = d // 2
    partner = d + 1 - 2 * odd
    low = 2 * me < n
    is_end = (me == 0) | (me == n - 1)
    is_inner = jnp.logical_not(is_end)
    near_end, far_end = jnp.where(low, 0, n - 1), jnp.where(low, n - 1, 0)
    other_inner = n - 1 - me
    inwards = me + jnp.where(low, 1, -1)
    home = jnp.where(d < half, 1, n - 2)
    is_source = me == home
    late_cross = is_end & (home == inwards) & (odd == 1)
    all_rows = pl.ds(0, rows)

    def rows_at(c):
        return pl.ds(pl.multiple_of(c * step, step), step)

    def feats_at(s):
        return pl.ds(pl.multiple_of(s * feats, feats), feats)

    def loop(count, body, start=0):
        def wrapped(i, carry):
            body(i)
            return carry

        lax.fori_loop(start, count, wrapped, 0)

    def remote(src, dst, send, recv, target):
        return pltpu.make_async_remote_copy(
            src_ref=src,
            dst_ref=dst,
            send_sem=send,
            recv_sem=recv,
            device_id=target,
            device_id_type=MESH,
        )

    def tok_copy(s, c, up):
        ref = x_all.at[s, pl.ds(pl.multiple_of(c * piece, piece), piece)]
        return remote(ref, ref, ag_send.at[up, s], ag_recv.at[s, c], {"mp": me + 2 * up - 1})

    def sent(ref, sem):
        remote(ref, ref, sem, ctx_recv.at[0], {"mp": inwards}).wait_send()

    def tokens_sent(s, up):
        sent(x_all.at[s], ag_send.at[up, s])

    def gain_copy(origin, target):
        ref = gain_all.at[feats_at(origin)]
        return remote(ref, ref, g_send.at[0], g_recv.at[0], {"mp": target})

    def all_gains():
        ref = gain_all.at[pl.ds(0, (n - 1) * feats)]
        return remote(ref, ref, g_send.at[0], g_recv.at[0], {"mp": inwards})

    def w_slot(o):
        return w_all.at[:, pl.ds(pl.multiple_of(o * wrows, wrows), wrows), :]

    def w_copy(o, target, forward):
        send = w_send.at[1 if forward else 0]
        return remote(w_slot(o), w_slot(o), send, w_recv.at[o], {"dp": target})

    def o_slot(z, o):
        return wo_all.at[z, lax.rem(o, half)]

    def o_copy(z, o, target, forward):
        send = o_send.at[1 if forward else 0]
        return remote(o_slot(z, o), o_slot(z, o), send, o_recv.at[z, lax.rem(o, half)], {"dp": target})

    def cross_copy():
        return remote(wo_own, o_slot(me, d), x_send.at[0], o_recv.at[me, lax.rem(d, half)], {"mp": home})

    def ctx_place(s, c):
        return jnp.where(s == 0, c, jnp.where(s == n - 1, chunks + c, 2 * chunks))

    def ctx_copy(s, c):
        ref = ctx_all.at[s, rows_at(c)]
        return remote(ref, ref, ctx_send.at[jnp.where(s == me, 0, 1)], ctx_recv.at[ctx_place(s, c)], {"mp": inwards})

    def end_copy(c):
        return remote(
            out_buf.at[rows_at(c)], landed.at[rows_at(c)], end_send.at[0], end_recv.at[c], {"mp": near_end}
        )

    def ss_copy(origin, c, target):
        return remote(
            ss_mine.at[c], ss_all.at[origin, c], ss_send.at[0], ss_recv.at[jnp.where(origin == 1, 0, 1), c], {"mp": target}
        )

    tok_in = pltpu.make_async_copy(tok, x_all.at[me], local_sem.at[0])
    win_in = pltpu.make_async_copy(win, w_slot(d), local_sem.at[1])
    pre_in = pltpu.make_async_copy(pre, gain_all.at[feats_at(me)], local_sem.at[2])
    post_in = pltpu.make_async_copy(post, post_v, local_sem.at[3])
    bias_in = pltpu.make_async_copy(bias, bias_v, local_sem.at[4])

    def wout_in(action):
        pl.when(is_source)(lambda: action(pltpu.make_async_copy(wout, o_slot(me, d), local_sem.at[5])))
        pl.when(jnp.logical_not(is_source))(
            lambda: action(pltpu.make_async_copy(wout, wo_own, local_sem.at[5]))
        )

    tok_in.start()
    win_in.start()
    pre_in.start()
    wout_in(lambda copy: copy.start())

    def peer_mp(k):
        return lax.rem(me + k, n)

    def same_core(k):
        return 2 * lax.rem(pair + k, half) + odd

    def from_core(k):
        return 2 * lax.rem(pair + half - k, half) + odd

    barrier = pltpu.get_barrier_semaphore()

    def greet(target):
        pl.semaphore_signal(barrier, inc=1, device_id=target, device_id_type=MESH)

    loop(n, lambda k: greet({"mp": peer_mp(k)}), 1)
    loop(half, lambda k: greet({"dp": same_core(k)}), 1)
    greet({"dp": partner})
    acc[...] = jnp.zeros_like(acc)
    square[...] = jnp.zeros_like(square)
    tok_in.wait()
    post_in.start()
    bias_in.start()
    pl.semaphore_wait(barrier, n - 1 + half - 1 + 1)

    def can_send(up):
        return (me < n - 1) if up else (me > 0)

    def send_own(up):
        @pl.when(can_send(up))
        def _():
            @pl.when(odd == 1)
            def _():
                pl.semaphore_wait(link_free.at[up], 1)

            loop(pieces, lambda c: tok_copy(me, c, up).start())

    def release(up):
        @pl.when(can_send(up))
        def _():
            pl.semaphore_signal(
                link_free.at[up], inc=1, device_id={"dp": partner}, device_id_type=MESH
            )

    def both_ways(action):
        @pl.when(low)
        def _():
            action(0)
            action(1)

        @pl.when(jnp.logical_not(low))
        def _():
            action(1)
            action(0)

    def in_plane(o):
        return (o < half) == (me == 1)

    def send_slice(z):
        o_copy(z, d, partner, False).start()
        loop(half, lambda k: o_copy(z, d, same_core(k), False).start(), 1)

    def relay_slice(z):
        @pl.when(is_source)
        def _():
            o_copy(z, d, partner, False).wait_recv()
            send_slice(z)

    def forward_slices(z):
        def forward(k):
            o = from_core(k)

            @pl.when(in_plane(o))
            def _():
                o_copy(z, o, partner, False).wait_recv()
                o_copy(z, o, partner, True).start()

        loop(half, forward, 1)

    def other_slices(z):
        def other(k):
            o = 2 * k + 1 - odd
            pl.when(in_plane(o))(lambda: o_copy(z, o, partner, False).wait_recv())

        loop(half, other)

    def send_weights():
        win_in.wait()
        w_copy(d, partner, False).start()
        loop(half, lambda k: w_copy(d, same_core(k), False).start(), 1)
        pre_in.wait()
        loop(n, lambda k: gain_copy(me, peer_mp(k)).start(), 1)
        wout_in(lambda copy: copy.wait())
        pl.when(is_source)(lambda: send_slice(me))
        pl.when(jnp.logical_not(is_source | late_cross))(lambda: cross_copy().start())

    def forward_weights():
        def forward(k):
            o = from_core(k)
            w_copy(o, partner, False).wait_recv()
            w_copy(o, partner, True).start()

        loop(half, forward, 1)
        all_gains().wait_recv()

    def other_weights():
        loop(half, lambda k: w_copy(2 * k + 1 - odd, partner, False).wait_recv())

    def take(up, j, use=None):
        s = me - j if up else me + j

        @pl.when((s >= 0) & (s < n))
        def _():
            def one(c):
                tok_copy(s, c, up).wait_recv()
                pl.when(can_send(up))(lambda: tok_copy(s, c, up).start())

            if use is None:
                loop(pieces, one)
            else:
                per = pieces // chunks

                def block(c):
                    loop(per, lambda i: one(c * per + i))
                    use(s, c)

                loop(chunks, block)

    def accumulate(s, at):
        gain = gain_all[feats_at(s)].astype(F32).reshape(1, feats)
        x = x_all[s, at, :].astype(F32)
        square[at, :] += x * x
        xg = (x * gain).astype(BF16)
        for m in range(3):
            acc[m, at, :] += jnp.dot(xg, w_all[m, feats_at(s), :], preferred_element_type=F32)

    def finish(c):
        total = jnp.sum(square[rows_at(c), :], axis=1, keepdims=True)
        inverse = lax.rsqrt(total / model + epsilon)
        for m in range(3):
            qkv[m, rows_at(c), :] = (acc[m, rows_at(c), :] * inverse).astype(BF16)

    def gather_by_shard(near):
        far = 1 - near
        reach = n - 1 - me if near else me
        loop(n, lambda j: take(near, j), 1)
        pl.when(late_cross)(lambda: cross_copy().start())
        forward_weights()
        relay_slice(near_end)
        relay_slice(far_end)
        relay_slice(other_inner)
        take(far, 1)
        other_weights()

        def known(s):
            pl.when((s <= me + 1) if near else (s >= me - 1))(lambda: accumulate(s, all_rows))

        loop(n, known)

        def later(j):
            @pl.when(j < reach)
            def _():
                take(far, j)
                accumulate(me + j if near else me - j, all_rows)

        def use(s, c):
            accumulate(s, rows_at(c))
            finish(c)

        loop(n, later, 2)
        take(far, reach, use)

    def by_shard():
        pl.when(low)(lambda: gather_by_shard(1))
        pl.when(jnp.logical_not(low))(lambda: gather_by_shard(0))

    def gather_even():
        both_ways(send_own)
        send_weights()

        @pl.when(is_end)
        def _():
            up = jnp.where(me == 0, 1, 0)
            tokens_sent(me, up)
            both_ways(release)
            by_shard()

        def hop(j, start=0, stop=pieces):
            def one(c):
                def side(up):
                    s = me - j if up else me + j

                    @pl.when((s >= 0) & (s < n))
                    def _():
                        tok_copy(s, c, up).wait_recv()
                        pl.when(can_send(up))(lambda: tok_copy(s, c, up).start())

                both_ways(side)

            loop(stop, one, start)

        @pl.when(is_inner)
        def _():
            hop(1)
            pl.when(low)(lambda: release(0))
            pl.when(jnp.logical_not(low))(lambda: release(1))
            hop(2, 0, pieces // 2)
            pl.when(low)(lambda: release(1))
            pl.when(jnp.logical_not(low))(lambda: release(0))
            hop(2, pieces // 2)
            forward_weights()
            relay_slice(near_end)
            relay_slice(far_end)
            relay_slice(other_inner)
            other_weights()
            loop(n, lambda s: accumulate(s, all_rows))
            loop(chunks, finish)
            forward_slices(me)

    def gather_odd():
        send_weights()
        both_ways(send_own)
        by_shard()

        @pl.when(is_inner)
        def _():
            forward_slices(me)
            forward_slices(near_end)
            forward_slices(far_end)

    pl.when(odd == 0)(gather_even)
    pl.when(odd == 1)(gather_odd)
    post_in.wait()
    bias_in.wait()

    lane_head = lax.broadcasted_iota(jnp.int32, (1, inner), 1) // head_dim
    contract = (((1,), (1,)), ((), ()))

    def attend(c):
        first = (c * step) // seq * seq
        keys_at = pl.ds(first, seq)
        bias_at = pl.ds(c * step - first, step)
        q = qkv[0, rows_at(c), :]
        k = qkv[1, keys_at, :]
        v = qkv[2, keys_at, :]
        stacked = jnp.concatenate([jnp.where(lane_head == h, q, jnp.zeros_like(q)) for h in range(heads)], axis=0)
        scores = lax.dot_general(stacked, k, contract, preferred_element_type=F32)
        scores = scores + bias_v[:, bias_at, :].reshape(heads * step, seq).astype(F32)
        weights = jnp.exp(scores - jnp.max(scores, axis=1, keepdims=True))
        scale = 1.0 / jnp.sum(weights, axis=1, keepdims=True)
        mixed = jnp.dot(weights.astype(BF16), v, preferred_element_type=F32) * scale
        context = mixed[0:step]
        for h in range(1, heads):
            context = jnp.where(lane_head == h, mixed[h * step : (h + 1) * step], context)
        ctx_all[me, rows_at(c), :] = context.astype(BF16)

    for c in range(0, chunks, 2):
        together = range(c, min(c + 2, chunks))
        for i in together:
            attend(i)
        for i in together:
            ctx_copy(me, i).start()

    def drain_line(s):
        waited = (odd == 0) & (s == me) & is_end

        @pl.when((s <= me) & (me < n - 1) & jnp.logical_not(waited))
        def _():
            tokens_sent(s, 1)

        @pl.when((s >= me) & (me > 0) & jnp.logical_not(waited))
        def _():
            tokens_sent(s, 0)

    def drain_early():
        all_gains().wait_send()
        loop(n, drain_line)
        sent(w_all.at[:, pl.ds(0, half * wrows), :], w_send.at[0])
        sent(w_all.at[:, pl.ds(0, (half - 1) * wrows), :], w_send.at[1])
        pl.when(jnp.logical_not(is_source))(lambda: cross_copy().wait_send())
        sent(ctx_all.at[me], ctx_send.at[0])

    def project_out(s, at, first=False):
        weight = jnp.concatenate([wo_all[s, i] for i in range(wo_all.shape[1])], axis=1)
        value = jnp.dot(ctx_all[s, at, :], weight, preferred_element_type=F32)
        part[at, :] = value if first else part[at, :] + value

    def pass_on(c):
        ctx_copy(near_end, c).wait_recv()
        ctx_copy(near_end, c).start()

    def finalize(c):
        def block(s, at):
            stream = (x_all[s, rows_at(c), :].astype(F32) + part[rows_at(c), at]).astype(BF16)
            wide_stream = stream.astype(F32)
            return stream, wide_stream * wide_stream

        def both(own_at, end_at):
            stream_end, squares_end = block(near_end, end_at)
            out_buf[rows_at(c), :] = stream_end
            end_copy(c).start()
            stream, squares = block(me, own_at)
            stream_o[rows_at(c), :] = stream
            total = jnp.sum(squares + squares_end, axis=1, keepdims=True)
            turned = jnp.transpose(jnp.broadcast_to(total, (step, 128)))
            ss_mine[c] = turned[0:8, :]
            ss_all[me, c] = turned[0:8, :]

        pl.when(low)(lambda: both(pl.ds(feats, feats), pl.ds(0, feats)))
        pl.when(jnp.logical_not(low))(lambda: both(pl.ds(0, feats), pl.ds(feats, feats)))
        loop(n, lambda k: ss_copy(me, c, peer_mp(k)).start(), 1)

    pl.when(is_end)(drain_early)

    @pl.when(is_inner)
    def _():
        @pl.when(odd == 0)
        def _():
            forward_slices(near_end)
            forward_slices(far_end)

        pl.when(odd == 1)(lambda: forward_slices(other_inner))
        other_slices(me)
        project_out(me, all_rows, True)
        other_slices(near_end)
        def near(c):
            pass_on(c)
            project_out(near_end, rows_at(c))

        loop(chunks // 2, near)
        pl.when(odd == 0)(lambda: forward_slices(other_inner))
        loop(chunks, near, chunks // 2)
        other_slices(other_inner)
        ref = ctx_all.at[other_inner]
        remote(ref, ref, ctx_send.at[0], ctx_recv.at[2 * chunks], {"mp": inwards}).wait_recv()
        project_out(other_inner, all_rows)
        other_slices(far_end)

        def last(c):
            ctx_copy(far_end, c).wait_recv()
            project_out(far_end, rows_at(c))
            finalize(c)

        loop(chunks, last)

    gain = post_v[...].astype(F32).reshape(1, feats)

    def normalize(c):
        def arrived(s):
            pl.when(s != me)(lambda: ss_copy(s, c, s).wait_recv())

        loop(n - 1, arrived, 1)

        @pl.when(is_end)
        def _():
            end_copy(c).wait_recv()
            stream_o[rows_at(c), :] = landed[rows_at(c), :]

        total = ss_all[1, c] + ss_all[n - 2, c]
        scale = jnp.transpose(lax.rsqrt(total / model + epsilon))[:, 0:1]
        stream = stream_o[rows_at(c), :].astype(F32)
        normed_o[rows_at(c), :] = (stream * scale * gain).astype(BF16)

    loop(chunks, normalize)

    @pl.when(is_inner)
    def _():
        drain_early()
        sent(ctx_all.at[near_end], ctx_send.at[1])
        sent(out_buf, end_send.at[0])
        sent(ss_all.at[pl.ds(0, n - 1)], ss_send.at[0])
        few, many = pl.ds(0, half // 2 - 1), pl.ds(0, half // 2)
        pl.when(is_source)(lambda: sent(wo_all, o_send.at[0]))
        pl.when(is_source)(lambda: sent(wo_all.at[:, few], o_send.at[1]))
        pl.when(jnp.logical_not(is_source))(lambda: sent(wo_all.at[:, many], o_send.at[1]))


def publish(stream_i, normed_i, stream_o, normed_o, sems):
    copies = (
        pltpu.make_async_copy(stream_i, stream_o, sems.at[0]),
        pltpu.make_async_copy(normed_i, normed_o, sems.at[1]),
    )
    for copy in copies:
        copy.start()
    for copy in copies:
        copy.wait()


def on_device(n, groups, tokens, pre_gain, input_weight, output_weight, position_bias, post_gain):
    rows, feats = tokens.shape
    step = 128
    chunks = rows // step
    inner = input_weight.shape[2]
    model = n * feats
    wide = output_weight.shape[1] % 128 == 0
    if not wide:
        output_weight = output_weight.T
    dma, any_space = pltpu.SemaphoreType.DMA, pl.BlockSpec(memory_space=pl.ANY)
    vmem = pl.BlockSpec(memory_space=pltpu.VMEM)
    if wide and n - 2 == 2:
        pieces = rows // 64
        body = functools.partial(line_kernel, n, groups, chunks)
        scratch = [
            pltpu.VMEM((n, rows, feats), BF16),
            pltpu.VMEM((n * feats,), BF16),
            pltpu.VMEM((feats,), BF16),
            pltpu.VMEM((3, model, inner), BF16),
            pltpu.VMEM(output_weight.shape, BF16),
            pltpu.VMEM((n, groups // 2, inner, output_weight.shape[1]), BF16),
            pltpu.VMEM(position_bias.shape, BF16),
            pltpu.VMEM((3, rows, inner), F32),
            pltpu.VMEM((rows, feats), F32),
            pltpu.VMEM((3, rows, inner), BF16),
            pltpu.VMEM((n, rows, inner), BF16),
            pltpu.VMEM((rows, 2 * feats), F32),
            pltpu.VMEM((rows, feats), BF16),
            pltpu.VMEM((rows, feats), BF16),
            pltpu.VMEM((chunks, 8, step), F32),
            pltpu.VMEM((n, chunks, 8, step), F32),
            dma((2, n)),
            dma((n, pieces)),
            dma((1,)),
            dma((1,)),
            dma((2,)),
            dma((groups,)),
            dma((1,)),
            dma((2,)),
            dma((n, groups // 2)),
            dma((2,)),
            dma((2 * chunks + 1,)),
            dma((1,)),
            dma((chunks,)),
            dma((1,)),
            dma((2, chunks)),
            dma((6,)),
            pltpu.SemaphoreType.REGULAR((2,)),
        ]
    else:
        body = functools.partial(kernel, n, groups, chunks, wide)
        wo_shape = (inner, model) if wide else (model, inner)
        scratch = [
            pltpu.VMEM((n, rows, feats), BF16),
            pltpu.VMEM((n * feats,), BF16),
            pltpu.VMEM((feats,), BF16),
            pltpu.VMEM((3, model, inner), BF16),
            pltpu.VMEM(wo_shape, BF16),
            pltpu.VMEM(wo_shape, BF16),
            pltpu.VMEM(position_bias.shape, BF16),
            pltpu.VMEM((3, rows, inner), F32),
            pltpu.VMEM((rows, feats), F32),
            pltpu.VMEM((3, rows, inner), BF16),
            pltpu.VMEM((n, rows, feats), F32),
            pltpu.VMEM((n, rows, feats), BF16),
            pltpu.VMEM((2, n, rows, feats), BF16),
            pltpu.VMEM((rows, inner), BF16),
            pltpu.VMEM((rows, inner), BF16),
            pltpu.VMEM((chunks, 8, step), F32),
            pltpu.VMEM((n, chunks, 8, step), F32),
            dma((2, n, chunks)),
            dma((n, chunks)),
            dma((n,)),
            dma((n,)),
            dma((3, 2, groups)),
            dma((3, groups)),
            dma((chunks,)),
            dma((chunks,)),
            dma((n, chunks)),
            dma((2, n, chunks)),
            dma((n, chunks)),
            dma((n, chunks)),
            dma((6,)),
            pltpu.SemaphoreType.REGULAR((2,)),
        ]
    stream, normed = pl.pallas_call(
        body,
        out_shape=(pltpu.VMEM((rows, feats), BF16), pltpu.VMEM((rows, feats), BF16)),
        in_specs=[any_space] * 6,
        out_specs=[vmem] * 2,
        scratch_shapes=scratch,
        compiler_params=pltpu.CompilerParams(
            collective_id=0, has_side_effects=True, vmem_limit_bytes=56 * 1024 * 1024
        ),
    )(tokens, pre_gain, input_weight, output_weight, position_bias, post_gain)
    shape = jax.ShapeDtypeStruct((rows, feats), BF16)
    return pl.pallas_call(
        publish,
        out_shape=(shape, shape),
        in_specs=[vmem] * 2,
        out_specs=[any_space] * 2,
        scratch_shapes=[dma((2,))],
        compiler_params=pltpu.CompilerParams(vmem_limit_bytes=4 * 1024 * 1024),
    )(stream, normed)


def solution(mesh):
    return jax.shard_map(
        functools.partial(on_device, mesh.shape["mp"], mesh.shape["dp"]),
        mesh=mesh,
        in_specs=(
            P("dp", "mp"),
            P("mp"),
            P(None, "dp", "mp"),
            P("mp", "dp"),
            P("mp", None, None),
            P("mp"),
        ),
        out_specs=(P("dp", "mp"), P("dp", "mp")),
        check_vma=False,
    )
```

```python
import functools

import jax
import jax.numpy as jnp
from jax import lax
from jax.experimental import pallas as pl
from jax.experimental.pallas import tpu as pltpu
from jax.sharding import PartitionSpec as P

epsilon = 1e-06
F32, BF16 = jnp.float32, jnp.bfloat16
MESH = pl.DeviceIdType.MESH


def kernel(
    n,
    groups,
    chunks,
    wide,
    tok,
    pre,
    win,
    wout,
    bias,
    post,
    stream_o,
    normed_o,
    x_all,
    gain_all,
    post_v,
    w_all,
    wo_all,
    wo_end,
    bias_v,
    acc,
    square,
    qkv,
    part,
    out_buf,
    landed,
    ctx_buf,
    ctx_in,
    ss_mine,
    ss_all,
    ag_send,
    ag_recv,
    g_send,
    g_recv,
    w_send,
    w_recv,
    ctx_send,
    ctx_recv,
    rs_send,
    rs_recv,
    ss_send,
    ss_recv,
    local_sem,
    link_free,
):
    rows, feats = tok.shape
    step = rows // chunks
    heads, seq = bias.shape[0], bias.shape[1]
    inner = win.shape[2]
    head_dim = inner // heads
    model = n * feats
    wrows = win.shape[1]
    wcols = model // groups
    half = groups // 2
    me = lax.axis_index("mp")
    d = lax.axis_index("dp")
    odd = lax.rem(d, 2)
    pair = d // 2
    partner = d + 1 - 2 * odd
    is_end = (me == 0) | (me == n - 1)
    is_edge = (me == 1) | (me == n - 2)
    all_rows = pl.ds(0, rows)

    def rows_at(c):
        return pl.ds(pl.multiple_of(c * step, step), step)

    def feats_at(s):
        return pl.ds(pl.multiple_of(s * feats, feats), feats)

    def loop(count, body, start=0):
        def wrapped(i, carry):
            body(i)
            return carry

        lax.fori_loop(start, count, wrapped, 0)

    def remote(src, dst, send, recv, target):
        return pltpu.make_async_remote_copy(
            src_ref=src,
            dst_ref=dst,
            send_sem=send,
            recv_sem=recv,
            device_id=target,
            device_id_type=MESH,
        )

    def tok_copy(s, c, up):
        ref = x_all.at[s, rows_at(c)]
        return remote(ref, ref, ag_send.at[up, s, c], ag_recv.at[s, c], {"mp": me + 2 * up - 1})

    def gain_copy(origin, target):
        ref = gain_all.at[feats_at(origin)]
        return remote(ref, ref, g_send.at[target], g_recv.at[origin], {"mp": target})

    def w_slot(o):
        return w_all.at[:, pl.ds(pl.multiple_of(o * wrows, wrows), wrows), :]

    def o_slot(ref, o):
        block = pl.ds(pl.multiple_of(o * wcols, wcols), wcols)
        return ref.at[:, block] if wide else ref.at[block, :]

    def slot(which, o):
        return w_slot(o) if which == 0 else o_slot(wo_all if which == 1 else wo_end, o)

    def weight_copy(which, o, target, forward):
        ref = slot(which, o)
        send = w_send.at[which, 1, o] if forward else w_send.at[which, 0, target]
        return remote(ref, ref, send, w_recv.at[which, o], {"dp": target})

    def cross_copy():
        inwards = jnp.where(me == 0, 1, n - 2)
        return remote(
            o_slot(wo_all, d), o_slot(wo_end, d), w_send.at[2, 0, d], w_recv.at[2, d], {"mp": inwards}
        )

    def ctx_copy(c):
        inwards = jnp.where(me == 0, 1, n - 2)
        return remote(
            ctx_buf.at[rows_at(c)], ctx_in.at[rows_at(c)], ctx_send.at[c], ctx_recv.at[c], {"mp": inwards}
        )

    def rs_copy(s, c, up):
        return remote(
            out_buf.at[s, rows_at(c)],
            landed.at[up, s, rows_at(c)],
            rs_send.at[s, c],
            rs_recv.at[up, s, c],
            {"mp": me + 2 * up - 1},
        )

    def ss_copy(origin, c, target):
        return remote(
            ss_mine.at[c], ss_all.at[origin, c], ss_send.at[target, c], ss_recv.at[origin, c], {"mp": target}
        )

    local = (
        pltpu.make_async_copy(tok, x_all.at[me], local_sem.at[0]),
        pltpu.make_async_copy(pre, gain_all.at[feats_at(me)], local_sem.at[1]),
        pltpu.make_async_copy(win, w_slot(d), local_sem.at[2]),
        pltpu.make_async_copy(wout, o_slot(wo_all, d), local_sem.at[3]),
        pltpu.make_async_copy(post, post_v, local_sem.at[4]),
        pltpu.make_async_copy(bias, bias_v, local_sem.at[5]),
    )
    for copy in local:
        copy.start()

    def peer_mp(k):
        return lax.rem(me + k, n)

    def same_core(k):
        return 2 * lax.rem(pair + k, half) + odd

    def from_core(k):
        return 2 * lax.rem(pair + half - k, half) + odd

    barrier = pltpu.get_barrier_semaphore()

    def greet(target):
        pl.semaphore_signal(barrier, inc=1, device_id=target, device_id_type=MESH)

    loop(n, lambda k: greet({"mp": peer_mp(k)}), 1)
    loop(half, lambda k: greet({"dp": same_core(k)}), 1)
    greet({"dp": partner})
    acc[...] = jnp.zeros_like(acc)
    square[...] = jnp.zeros_like(square)
    for copy in local[:5]:
        copy.wait()
    pl.semaphore_wait(barrier, n - 1 + half - 1 + 1)

    def can_send(up):
        return (me < n - 1) if up else (me > 0)

    def send_own(up):
        @pl.when(can_send(up))
        def _():
            @pl.when(odd == 1)
            def _():
                pl.semaphore_wait(link_free.at[up], 1)

            loop(chunks, lambda c: tok_copy(me, c, up).start())

    def release(up):
        @pl.when(can_send(up))
        def _():
            pl.semaphore_signal(
                link_free.at[up], inc=1, device_id={"dp": partner}, device_id_type=MESH
            )

    def send_weights(which):
        weight_copy(which, d, partner, False).start()
        loop(half, lambda k: weight_copy(which, d, same_core(k), False).start(), 1)

    def forward_weights(which):
        def forward(k):
            o = from_core(k)
            weight_copy(which, o, partner, False).wait_recv()
            weight_copy(which, o, partner, True).start()

        loop(half, forward, 1)

    def other_weights(which):
        loop(half, lambda k: weight_copy(which, 2 * k + 1 - odd, partner, False).wait_recv())

    def pass_end_weights():
        @pl.when(is_edge)
        def _():
            weight_copy(2, d, partner, False).wait_recv()
            send_weights(2)

    def forward_out_weights():
        pl.when(jnp.logical_not(is_end))(lambda: forward_weights(1))
        pl.when(is_edge)(lambda: forward_weights(2))

    def take(up, j, use=None):
        s = me - j if up else me + j

        @pl.when((s >= 0) & (s < n))
        def _():
            def one(c):
                tok_copy(s, c, up).wait_recv()

                @pl.when(can_send(up))
                def _():
                    tok_copy(s, c, up).start()

                if use is not None:
                    use(s, c)

            loop(chunks, one)

    def accumulate(s, at):
        gain = gain_all[feats_at(s)].astype(F32).reshape(1, feats)
        x = x_all[s, at, :].astype(F32)
        square[at, :] += x * x
        xg = (x * gain).astype(BF16)
        for m in range(3):
            acc[m, at, :] += jnp.dot(xg, w_all[m, feats_at(s), :], preferred_element_type=F32)

    def both_ways(action):
        @pl.when(2 * me < n)
        def _():
            action(0)
            action(1)

        @pl.when(2 * me >= n)
        def _():
            action(1)
            action(0)

    def finish(c):
        total = jnp.sum(square[rows_at(c), :], axis=1, keepdims=True)
        inverse = lax.rsqrt(total / model + epsilon)
        for m in range(3):
            qkv[m, rows_at(c), :] = (acc[m, rows_at(c), :] * inverse).astype(BF16)

    def send_all_weights():
        send_weights(0)
        pl.when(is_end)(lambda: cross_copy().start())
        pl.when(jnp.logical_not(is_end))(lambda: send_weights(1))

    def wait_gains():
        loop(n, lambda k: gain_copy(peer_mp(k), peer_mp(k)).wait_recv(), 1)

    def gather_even():
        both_ways(send_own)
        send_all_weights()

        @pl.when(is_end)
        def _():
            up = jnp.where(me == 0, 1, 0)
            loop(chunks, lambda c: tok_copy(me, c, up).wait_send())
            both_ways(release)

        def hop(j):
            def one(c):
                def side(up):
                    s = me - j if up else me + j

                    @pl.when((s >= 0) & (s < n))
                    def _():
                        tok_copy(s, c, up).wait_recv()
                        pl.when(can_send(up))(lambda: tok_copy(s, c, up).start())

                both_ways(side)

            loop(chunks, one)

        loop(n, hop, 1)
        pl.when(jnp.logical_not(is_end))(lambda: both_ways(release))
        pass_end_weights()
        forward_weights(0)
        wait_gains()
        other_weights(0)
        loop(n, lambda s: accumulate(s, all_rows))
        loop(chunks, finish)

    def gather_odd():
        send_all_weights()
        both_ways(send_own)

        def toward(near):
            far = 1 - near
            reach = n - 1 - me if near else me
            loop(n, lambda j: take(near, j), 1)
            pass_end_weights()
            forward_weights(0)
            wait_gains()
            take(far, 1)
            other_weights(0)

            def known(s):
                pl.when((s <= me + 1) if near else (s >= me - 1))(lambda: accumulate(s, all_rows))

            loop(n, known)

            def later(j):
                @pl.when(j < reach)
                def _():
                    take(far, j)
                    accumulate(me + j if near else me - j, all_rows)

            def use(s, c):
                accumulate(s, rows_at(c))
                finish(c)

            loop(n, later, 2)
            pl.when(reach > 1)(lambda: take(far, reach, use))
            pl.when(reach <= 1)(lambda: loop(chunks, finish))

        pl.when(2 * me < n)(lambda: toward(1))
        pl.when(2 * me >= n)(lambda: toward(0))
        forward_out_weights()

    loop(n, lambda k: gain_copy(me, peer_mp(k)).start(), 1)
    pl.when(odd == 0)(gather_even)
    pl.when(odd == 1)(gather_odd)

    local[5].wait()

    lane_head = lax.broadcasted_iota(jnp.int32, (1, inner), 1) // head_dim
    contract = (((1,), (1,)), ((), ()))

    def attend(c):
        first = (c * step) // seq * seq
        keys_at = pl.ds(pl.multiple_of(first, seq), seq)
        bias_at = pl.ds(pl.multiple_of(c * step - first, step), step)
        q = qkv[0, rows_at(c), :]
        k = qkv[1, keys_at, :]
        v = qkv[2, keys_at, :]
        stacked = jnp.concatenate([jnp.where(lane_head == h, q, jnp.zeros_like(q)) for h in range(heads)], axis=0)
        scores = lax.dot_general(stacked, k, contract, preferred_element_type=F32)
        scores = scores + bias_v[:, bias_at, :].reshape(heads * step, seq).astype(F32)
        weights = jnp.exp(scores - jnp.max(scores, axis=1, keepdims=True))
        scale = 1.0 / jnp.sum(weights, axis=1, keepdims=True)
        mixed = jnp.dot(weights.astype(BF16), v, preferred_element_type=F32) * scale
        context = mixed[0:step]
        for h in range(1, heads):
            context = jnp.where(lane_head == h, mixed[h * step : (h + 1) * step], context)
        ctx_buf[rows_at(c), :] = context.astype(BF16)
        pl.when(is_end)(lambda: ctx_copy(c).start())

    loop(chunks, attend)

    def project_out(context, ref, s):
        block = feats_at(s)
        if wide:
            return jnp.dot(context, ref[:, block], preferred_element_type=F32)
        return lax.dot_general(context, ref[block, :], contract, preferred_element_type=F32)

    def send_out(s, c, up, value):
        out_buf[s, rows_at(c), :] = value.astype(BF16)
        rs_copy(s, c, up).start()

    def own_share(s):
        part[s] = project_out(ctx_buf[...], wo_all, s)

    def originate(c):
        ctx_copy(c).wait_recv()
        context = ctx_in[rows_at(c), :]

        def far(k):
            s = jnp.where(me == 1, n - 1 - k, k)
            value = part[s, rows_at(c), :] + project_out(context, wo_end, s)
            send_out(s, c, jnp.where(me == 1, 1, 0), value)

        def near(k):
            s = jnp.where(me == 1, k, n - 2 + k)
            part[s, rows_at(c), :] += project_out(context, wo_end, s)

        loop(n - 2, far)
        loop(2, near)

    def finished(s, c):
        value = x_all[s, rows_at(c), :].astype(F32) + part[s, rows_at(c), :]
        stream = value.astype(BF16)
        wide_stream = stream.astype(F32)
        return stream, wide_stream * wide_stream

    def finalize(c):
        stream, squares = finished(me, c)
        stream_o[rows_at(c), :] = stream
        part[me, rows_at(c), :] = squares

        @pl.when(is_edge)
        def _():
            end, up = jnp.where(me == 1, 0, n - 1), jnp.where(me == 1, 0, 1)
            stream_end, squares_end = finished(end, c)
            out_buf[end, rows_at(c), :] = stream_end
            rs_copy(end, c, up).start()
            part[me, rows_at(c), :] += squares_end

        total = jnp.sum(part[me, rows_at(c), :], axis=1, keepdims=True)
        turned = jnp.transpose(jnp.broadcast_to(total, (step, 128)))
        ss_mine[c] = turned[0:8, :]
        ss_all[me, c] = turned[0:8, :]
        loop(n, lambda k: ss_copy(me, c, peer_mp(k)).start(), 1)

    def combine(c):
        def message(k):
            for up in (1, 0):
                s = n - 1 - k if up else k
                follows = (me >= 2) if up else (me <= n - 3)
                further = (s > me) if up else (s < me)
                last = (me == n - 2) if up else (me == 1)

                @pl.when(follows & (further | (s == me)))
                def _():
                    rs_copy(s, c, up).wait_recv()
                    value = part[s, rows_at(c), :] + landed[up, s, rows_at(c), :].astype(F32)

                    @pl.when((s == me) | last)
                    def _():
                        part[s, rows_at(c), :] = value

                    @pl.when((s != me) & jnp.logical_not(last))
                    def _():
                        send_out(s, c, up, value)

        loop(n - 2, message)
        finalize(c)

    @pl.when(jnp.logical_not(is_end))
    def _():
        pl.when(odd == 0)(forward_out_weights)
        other_weights(1)
        pl.when(is_edge)(lambda: other_weights(2))
        loop(n, own_share)
        pl.when(is_edge)(lambda: loop(chunks, originate))
        loop(chunks, combine)

    gain = post_v[...].astype(F32).reshape(1, feats)

    def normalize(c):
        def arrived(s):
            pl.when(s != me)(lambda: ss_copy(s, c, s).wait_recv())

        loop(n - 1, arrived, 1)

        @pl.when(is_end)
        def _():
            up = jnp.where(me == 0, 0, 1)
            rs_copy(me, c, up).wait_recv()
            stream_o[rows_at(c), :] = landed[up, me, rows_at(c), :]

        total = jnp.zeros((8, step), F32)
        for s in range(1, n - 1):
            total = total + ss_all[s, c]
        scale = jnp.transpose(lax.rsqrt(total / model + epsilon))[:, 0:1]
        stream = stream_o[rows_at(c), :].astype(F32)
        normed_o[rows_at(c), :] = (stream * scale * gain).astype(BF16)

    loop(chunks, normalize)

    loop(n, lambda k: gain_copy(me, peer_mp(k)).wait_send(), 1)

    def drain_tokens(s):
        def one(c):
            waited = (odd == 0) & (s == me) & is_end

            @pl.when((s <= me) & (me < n - 1) & jnp.logical_not(waited))
            def _():
                tok_copy(s, c, 1).wait_send()

            @pl.when((s >= me) & (me > 0) & jnp.logical_not(waited))
            def _():
                tok_copy(s, c, 0).wait_send()

            @pl.when(jnp.logical_not(is_end) & (s != me))
            def _():
                rs_copy(s, c, 1).wait_send()
                ss_copy(me, c, s).wait_send()

        loop(chunks, one)

    loop(n, drain_tokens)

    def drain_weights(which):
        weight_copy(which, d, partner, False).wait_send()

        def drain(k):
            weight_copy(which, d, same_core(k), False).wait_send()
            weight_copy(which, from_core(k), partner, True).wait_send()

        loop(half, drain, 1)

    drain_weights(0)
    pl.when(is_edge)(lambda: drain_weights(2))

    @pl.when(is_end)
    def _():
        cross_copy().wait_send()
        loop(chunks, lambda c: ctx_copy(c).wait_send())

    pl.when(jnp.logical_not(is_end))(lambda: drain_weights(1))


def line_kernel(
    n,
    groups,
    chunks,
    tok,
    pre,
    win,
    wout,
    bias,
    post,
    stream_o,
    normed_o,
    x_all,
    gain_all,
    post_v,
    w_all,
    wo_own,
    wo_all,
    bias_v,
    acc,
    square,
    qkv,
    ctx_all,
    part,
    out_buf,
    landed,
    ss_mine,
    ss_all,
    ag_send,
    ag_recv,
    g_send,
    g_recv,
    w_send,
    w_recv,
    x_send,
    o_send,
    o_recv,
    ctx_send,
    ctx_recv,
    end_send,
    end_recv,
    ss_send,
    ss_recv,
    local_sem,
    link_free,
):
    rows, feats = tok.shape
    step = rows // chunks
    pieces = ag_recv.shape[1]
    piece = rows // pieces
    head = pieces // 8
    heads, seq = bias.shape[0], bias.shape[1]
    inner = win.shape[2]
    head_dim = inner // heads
    model = n * feats
    wrows = win.shape[1]
    wcols = model // groups
    half = groups // 2
    me = lax.axis_index("mp")
    d = lax.axis_index("dp")
    odd = lax.rem(d, 2)
    pair = d // 2
    partner = d + 1 - 2 * odd
    low = 2 * me < n
    is_end = (me == 0) | (me == n - 1)
    is_inner = jnp.logical_not(is_end)
    near_end, far_end = jnp.where(low, 0, n - 1), jnp.where(low, n - 1, 0)
    other_inner = n - 1 - me
    inwards = me + jnp.where(low, 1, -1)
    home = jnp.where(d < half, 1, n - 2)
    is_source = me == home
    late_cross = is_end & (home == inwards) & (odd == 1)
    all_rows = pl.ds(0, rows)

    def rows_at(c):
        return pl.ds(pl.multiple_of(c * step, step), step)

    def feats_at(s):
        return pl.ds(pl.multiple_of(s * feats, feats), feats)

    def loop(count, body, start=0):
        def wrapped(i, carry):
            body(i)
            return carry

        lax.fori_loop(start, count, wrapped, 0)

    def remote(src, dst, send, recv, target):
        return pltpu.make_async_remote_copy(
            src_ref=src,
            dst_ref=dst,
            send_sem=send,
            recv_sem=recv,
            device_id=target,
            device_id_type=MESH,
        )

    def tok_copy(s, c, up):
        ref = x_all.at[s, pl.ds(pl.multiple_of(c * piece, piece), piece)]
        return remote(ref, ref, ag_send.at[up, s], ag_recv.at[s, c], {"mp": me + 2 * up - 1})

    def sent(ref, sem):
        remote(ref, ref, sem, ctx_recv.at[0], {"mp": inwards}).wait_send()

    def tokens_sent(s, up):
        sent(x_all.at[s], ag_send.at[up, s])

    def gain_copy(origin, target):
        ref = gain_all.at[feats_at(origin)]
        return remote(ref, ref, g_send.at[0], g_recv.at[0], {"mp": target})

    def all_gains():
        ref = gain_all.at[pl.ds(0, (n - 1) * feats)]
        return remote(ref, ref, g_send.at[0], g_recv.at[0], {"mp": inwards})

    def w_slot(o):
        return w_all.at[:, pl.ds(pl.multiple_of(o * wrows, wrows), wrows), :]

    def w_copy(o, target, forward):
        send = w_send.at[1 if forward else 0]
        return remote(w_slot(o), w_slot(o), send, w_recv.at[o], {"dp": target})

    def o_slot(z, o):
        return wo_all.at[z, lax.rem(o, half)]

    def o_copy(z, o, target, forward):
        send = o_send.at[1 if forward else 0]
        return remote(o_slot(z, o), o_slot(z, o), send, o_recv.at[z, lax.rem(o, half)], {"dp": target})

    def cross_copy():
        return remote(wo_own, o_slot(me, d), x_send.at[0], o_recv.at[me, lax.rem(d, half)], {"mp": home})

    def ctx_place(s, c):
        return jnp.where(s == 0, c, jnp.where(s == n - 1, chunks + c, 2 * chunks))

    def ctx_copy(s, c):
        ref = ctx_all.at[s, rows_at(c)]
        return remote(ref, ref, ctx_send.at[jnp.where(s == me, 0, 1)], ctx_recv.at[ctx_place(s, c)], {"mp": inwards})

    def end_copy(c):
        return remote(
            out_buf.at[rows_at(c)], landed.at[rows_at(c)], end_send.at[0], end_recv.at[c], {"mp": near_end}
        )

    def ss_copy(origin, c, target):
        return remote(
            ss_mine.at[c], ss_all.at[origin, c], ss_send.at[0], ss_recv.at[jnp.where(origin == 1, 0, 1), c], {"mp": target}
        )

    tok_in = pltpu.make_async_copy(tok, x_all.at[me], local_sem.at[0])
    win_in = pltpu.make_async_copy(win, w_slot(d), local_sem.at[1])
    pre_in = pltpu.make_async_copy(pre, gain_all.at[feats_at(me)], local_sem.at[2])
    post_in = pltpu.make_async_copy(post, post_v, local_sem.at[3])
    bias_in = pltpu.make_async_copy(bias, bias_v, local_sem.at[4])

    def wout_in(action):
        pl.when(is_source)(lambda: action(pltpu.make_async_copy(wout, o_slot(me, d), local_sem.at[5])))
        pl.when(jnp.logical_not(is_source))(
            lambda: action(pltpu.make_async_copy(wout, wo_own, local_sem.at[5]))
        )

    tok_in.start()
    win_in.start()
    pre_in.start()
    wout_in(lambda copy: copy.start())

    def peer_mp(k):
        return lax.rem(me + k, n)

    def same_core(k):
        return 2 * lax.rem(pair + k, half) + odd

    def from_core(k):
        return 2 * lax.rem(pair + half - k, half) + odd

    barrier = pltpu.get_barrier_semaphore()

    def greet(target):
        pl.semaphore_signal(barrier, inc=1, device_id=target, device_id_type=MESH)

    loop(n, lambda k: greet({"mp": peer_mp(k)}), 1)
    loop(half, lambda k: greet({"dp": same_core(k)}), 1)
    greet({"dp": partner})
    acc[...] = jnp.zeros_like(acc)
    square[...] = jnp.zeros_like(square)
    tok_in.wait()
    post_in.start()
    bias_in.start()
    pl.semaphore_wait(barrier, n - 1 + half - 1 + 1)

    def can_send(up):
        return (me < n - 1) if up else (me > 0)

    def send_own(up):
        @pl.when(can_send(up))
        def _():
            @pl.when(odd == 1)
            def _():
                pl.semaphore_wait(link_free.at[up], 1)
                loop(pieces, lambda c: tok_copy(me, c, up).start(), head)

            pl.when(odd == 0)(lambda: loop(pieces, lambda c: tok_copy(me, c, up).start()))

    def send_head(up):
        pl.when(can_send(up))(lambda: loop(head, lambda c: tok_copy(me, c, up).start()))

    def release(up):
        @pl.when(can_send(up))
        def _():
            pl.semaphore_signal(
                link_free.at[up], inc=1, device_id={"dp": partner}, device_id_type=MESH
            )

    def both_ways(action):
        @pl.when(low)
        def _():
            action(0)
            action(1)

        @pl.when(jnp.logical_not(low))
        def _():
            action(1)
            action(0)

    def in_plane(o):
        return (o < half) == (me == 1)

    def send_slice(z):
        o_copy(z, d, partner, False).start()
        loop(half, lambda k: o_copy(z, d, same_core(k), False).start(), 1)

    def relay_slice(z):
        @pl.when(is_source)
        def _():
            o_copy(z, d, partner, False).wait_recv()
            send_slice(z)

    def forward_slices(z):
        def forward(k):
            o = from_core(k)

            @pl.when(in_plane(o))
            def _():
                o_copy(z, o, partner, False).wait_recv()
                o_copy(z, o, partner, True).start()

        loop(half, forward, 1)

    def other_slices(z):
        def other(k):
            o = 2 * k + 1 - odd
            pl.when(in_plane(o))(lambda: o_copy(z, o, partner, False).wait_recv())

        loop(half, other)

    def send_weights():
        win_in.wait()
        w_copy(d, partner, False).start()
        loop(half, lambda k: w_copy(d, same_core(k), False).start(), 1)
        pre_in.wait()
        loop(n, lambda k: gain_copy(me, peer_mp(k)).start(), 1)
        wout_in(lambda copy: copy.wait())
        pl.when(is_source)(lambda: send_slice(me))
        pl.when(jnp.logical_not(is_source | late_cross))(lambda: cross_copy().start())

    def forward_weights():
        def forward(k):
            o = from_core(k)
            w_copy(o, partner, False).wait_recv()
            w_copy(o, partner, True).start()

        loop(half, forward, 1)
        all_gains().wait_recv()

    def other_weights():
        loop(half, lambda k: w_copy(2 * k + 1 - odd, partner, False).wait_recv())

    def take(up, j, use=None):
        s = me - j if up else me + j

        @pl.when((s >= 0) & (s < n))
        def _():
            def one(c):
                tok_copy(s, c, up).wait_recv()
                pl.when(can_send(up))(lambda: tok_copy(s, c, up).start())

            if use is None:
                loop(pieces, one)
            else:
                per = pieces // chunks

                def block(c):
                    loop(per, lambda i: one(c * per + i))
                    use(s, c)

                loop(chunks, block)

    def accumulate(s, at):
        gain = gain_all[feats_at(s)].astype(F32).reshape(1, feats)
        x = x_all[s, at, :].astype(F32)
        square[at, :] += x * x
        xg = (x * gain).astype(BF16)
        for m in range(3):
            acc[m, at, :] += jnp.dot(xg, w_all[m, feats_at(s), :], preferred_element_type=F32)

    def finish(c):
        total = jnp.sum(square[rows_at(c), :], axis=1, keepdims=True)
        inverse = lax.rsqrt(total / model + epsilon)
        for m in range(3):
            qkv[m, rows_at(c), :] = (acc[m, rows_at(c), :] * inverse).astype(BF16)

    def gather_by_shard(near):
        far = 1 - near
        reach = n - 1 - me if near else me
        loop(n, lambda j: take(near, j), 1)
        pl.when(late_cross)(lambda: cross_copy().start())
        forward_weights()
        relay_slice(near_end)
        relay_slice(far_end)
        relay_slice(other_inner)
        take(far, 1)
        other_weights()

        def known(s):
            pl.when((s <= me + 1) if near else (s >= me - 1))(lambda: accumulate(s, all_rows))

        loop(n, known)

        def later(j):
            @pl.when(j < reach)
            def _():
                take(far, j)
                accumulate(me + j if near else me - j, all_rows)

        def use(s, c):
            accumulate(s, rows_at(c))
            finish(c)

        loop(n, later, 2)
        take(far, reach, use)

    def by_shard():
        pl.when(low)(lambda: gather_by_shard(1))
        pl.when(jnp.logical_not(low))(lambda: gather_by_shard(0))

    def gather_even():
        both_ways(send_own)
        send_weights()

        @pl.when(is_end)
        def _():
            up = jnp.where(me == 0, 1, 0)
            tokens_sent(me, up)
            both_ways(release)
            by_shard()

        def hop(j, start=0, stop=pieces):
            def one(c):
                def side(up):
                    s = me - j if up else me + j

                    @pl.when((s >= 0) & (s < n))
                    def _():
                        tok_copy(s, c, up).wait_recv()
                        pl.when(can_send(up))(lambda: tok_copy(s, c, up).start())

                both_ways(side)

            loop(stop, one, start)

        @pl.when(is_inner)
        def _():
            hop(1)
            pl.when(low)(lambda: release(0))
            pl.when(jnp.logical_not(low))(lambda: release(1))
            hop(2, 0, pieces // 2)
            pl.when(low)(lambda: release(1))
            pl.when(jnp.logical_not(low))(lambda: release(0))
            hop(2, pieces // 2)
            forward_weights()
            relay_slice(near_end)
            relay_slice(far_end)
            relay_slice(other_inner)
            other_weights()
            loop(n, lambda s: accumulate(s, all_rows))
            loop(chunks, finish)
            forward_slices(me)

    def gather_odd():
        both_ways(send_head)
        send_weights()
        both_ways(send_own)
        by_shard()

        @pl.when(is_inner)
        def _():
            forward_slices(me)
            forward_slices(near_end)
            forward_slices(far_end)

    pl.when(odd == 0)(gather_even)
    pl.when(odd == 1)(gather_odd)
    post_in.wait()
    bias_in.wait()

    lane_head = lax.broadcasted_iota(jnp.int32, (1, inner), 1) // head_dim
    contract = (((1,), (1,)), ((), ()))

    def attend(c):
        first = (c * step) // seq * seq
        keys_at = pl.ds(first, seq)
        bias_at = pl.ds(c * step - first, step)
        q = qkv[0, rows_at(c), :]
        k = qkv[1, keys_at, :]
        v = qkv[2, keys_at, :]
        stacked = jnp.concatenate([jnp.where(lane_head == h, q, jnp.zeros_like(q)) for h in range(heads)], axis=0)
        scores = lax.dot_general(stacked, k, contract, preferred_element_type=F32)
        scores = scores + bias_v[:, bias_at, :].reshape(heads * step, seq).astype(F32)
        weights = jnp.exp(scores - jnp.max(scores, axis=1, keepdims=True))
        scale = 1.0 / jnp.sum(weights, axis=1, keepdims=True)
        mixed = jnp.dot(weights.astype(BF16), v, preferred_element_type=F32) * scale
        context = mixed[0:step]
        for h in range(1, heads):
            context = jnp.where(lane_head == h, mixed[h * step : (h + 1) * step], context)
        ctx_all[me, rows_at(c), :] = context.astype(BF16)

    starts = [0, *range(1, chunks, 2), chunks]
    for c, stop in zip(starts[:-1], starts[1:]):
        together = range(c, stop)
        for i in together:
            attend(i)
        for i in together:
            ctx_copy(me, i).start()

    def drain_line(s):
        waited = (odd == 0) & (s == me) & is_end

        @pl.when((s <= me) & (me < n - 1) & jnp.logical_not(waited))
        def _():
            tokens_sent(s, 1)

        @pl.when((s >= me) & (me > 0) & jnp.logical_not(waited))
        def _():
            tokens_sent(s, 0)

    def drain_early():
        all_gains().wait_send()
        loop(n, drain_line)
        sent(w_all.at[:, pl.ds(0, half * wrows), :], w_send.at[0])
        sent(w_all.at[:, pl.ds(0, (half - 1) * wrows), :], w_send.at[1])
        pl.when(jnp.logical_not(is_source))(lambda: cross_copy().wait_send())
        sent(ctx_all.at[me], ctx_send.at[0])

    def project_out(s, at, first=False):
        weight = jnp.concatenate([wo_all[s, i] for i in range(wo_all.shape[1])], axis=1)
        value = jnp.dot(ctx_all[s, at, :], weight, preferred_element_type=F32)
        part[at, :] = value if first else part[at, :] + value

    def pass_on(c):
        ctx_copy(near_end, c).wait_recv()
        ctx_copy(near_end, c).start()

    def finalize(c):
        def block(s, at):
            stream = (x_all[s, rows_at(c), :].astype(F32) + part[rows_at(c), at]).astype(BF16)
            wide_stream = stream.astype(F32)
            return stream, wide_stream * wide_stream

        def both(own_at, end_at):
            stream_end, squares_end = block(near_end, end_at)
            out_buf[rows_at(c), :] = stream_end
            end_copy(c).start()
            stream, squares = block(me, own_at)
            stream_o[rows_at(c), :] = stream
            total = jnp.sum(squares + squares_end, axis=1, keepdims=True)
            turned = jnp.transpose(jnp.broadcast_to(total, (step, 128)))
            ss_mine[c] = turned[0:8, :]
            ss_all[me, c] = turned[0:8, :]

        pl.when(low)(lambda: both(pl.ds(feats, feats), pl.ds(0, feats)))
        pl.when(jnp.logical_not(low))(lambda: both(pl.ds(0, feats), pl.ds(feats, feats)))
        loop(n, lambda k: ss_copy(me, c, peer_mp(k)).start(), 1)

    pl.when(is_end)(drain_early)

    @pl.when(is_inner)
    def _():
        @pl.when(odd == 0)
        def _():
            forward_slices(near_end)
            forward_slices(far_end)

        pl.when(odd == 1)(lambda: forward_slices(other_inner))
        other_slices(me)
        project_out(me, all_rows, True)
        other_slices(near_end)
        def near(c):
            pass_on(c)
            project_out(near_end, rows_at(c))

        loop(chunks // 2, near)
        pl.when(odd == 0)(lambda: forward_slices(other_inner))
        loop(chunks, near, chunks // 2)
        other_slices(other_inner)
        ref = ctx_all.at[other_inner]
        remote(ref, ref, ctx_send.at[0], ctx_recv.at[2 * chunks], {"mp": inwards}).wait_recv()
        project_out(other_inner, all_rows)
        other_slices(far_end)

        def last(c):
            ctx_copy(far_end, c).wait_recv()
            project_out(far_end, rows_at(c))
            finalize(c)

        loop(chunks, last)

    gain = post_v[...].astype(F32).reshape(1, feats)

    def normalize(c):
        def arrived(s):
            pl.when(s != me)(lambda: ss_copy(s, c, s).wait_recv())

        loop(n - 1, arrived, 1)

        @pl.when(is_end)
        def _():
            end_copy(c).wait_recv()
            stream_o[rows_at(c), :] = landed[rows_at(c), :]

        total = ss_all[1, c] + ss_all[n - 2, c]
        scale = jnp.transpose(lax.rsqrt(total / model + epsilon))[:, 0:1]
        stream = stream_o[rows_at(c), :].astype(F32)
        normed_o[rows_at(c), :] = (stream * scale * gain).astype(BF16)

    loop(chunks, normalize)

    @pl.when(is_inner)
    def _():
        drain_early()
        sent(ctx_all.at[near_end], ctx_send.at[1])
        sent(out_buf, end_send.at[0])
        sent(ss_all.at[pl.ds(0, n - 1)], ss_send.at[0])
        few, many = pl.ds(0, half // 2 - 1), pl.ds(0, half // 2)
        pl.when(is_source)(lambda: sent(wo_all, o_send.at[0]))
        pl.when(is_source)(lambda: sent(wo_all.at[:, few], o_send.at[1]))
        pl.when(jnp.logical_not(is_source))(lambda: sent(wo_all.at[:, many], o_send.at[1]))


def publish(stream_i, normed_i, stream_o, normed_o, sems):
    copies = (
        pltpu.make_async_copy(stream_i, stream_o, sems.at[0]),
        pltpu.make_async_copy(normed_i, normed_o, sems.at[1]),
    )
    for copy in copies:
        copy.start()
    for copy in copies:
        copy.wait()


def on_device(n, groups, tokens, pre_gain, input_weight, output_weight, position_bias, post_gain):
    rows, feats = tokens.shape
    step = 128
    chunks = rows // step
    inner = input_weight.shape[2]
    model = n * feats
    wide = output_weight.shape[1] % 128 == 0
    if not wide:
        output_weight = output_weight.T
    dma, any_space = pltpu.SemaphoreType.DMA, pl.BlockSpec(memory_space=pl.ANY)
    vmem = pl.BlockSpec(memory_space=pltpu.VMEM)
    if wide and n - 2 == 2:
        pieces = rows // 64
        body = functools.partial(line_kernel, n, groups, chunks)
        scratch = [
            pltpu.VMEM((n, rows, feats), BF16),
            pltpu.VMEM((n * feats,), BF16),
            pltpu.VMEM((feats,), BF16),
            pltpu.VMEM((3, model, inner), BF16),
            pltpu.VMEM(output_weight.shape, BF16),
            pltpu.VMEM((n, groups // 2, inner, output_weight.shape[1]), BF16),
            pltpu.VMEM(position_bias.shape, BF16),
            pltpu.VMEM((3, rows, inner), F32),
            pltpu.VMEM((rows, feats), F32),
            pltpu.VMEM((3, rows, inner), BF16),
            pltpu.VMEM((n, rows, inner), BF16),
            pltpu.VMEM((rows, 2 * feats), F32),
            pltpu.VMEM((rows, feats), BF16),
            pltpu.VMEM((rows, feats), BF16),
            pltpu.VMEM((chunks, 8, step), F32),
            pltpu.VMEM((n, chunks, 8, step), F32),
            dma((2, n)),
            dma((n, pieces)),
            dma((1,)),
            dma((1,)),
            dma((2,)),
            dma((groups,)),
            dma((1,)),
            dma((2,)),
            dma((n, groups // 2)),
            dma((2,)),
            dma((2 * chunks + 1,)),
            dma((1,)),
            dma((chunks,)),
            dma((1,)),
            dma((2, chunks)),
            dma((6,)),
            pltpu.SemaphoreType.REGULAR((2,)),
        ]
    else:
        body = functools.partial(kernel, n, groups, chunks, wide)
        wo_shape = (inner, model) if wide else (model, inner)
        scratch = [
            pltpu.VMEM((n, rows, feats), BF16),
            pltpu.VMEM((n * feats,), BF16),
            pltpu.VMEM((feats,), BF16),
            pltpu.VMEM((3, model, inner), BF16),
            pltpu.VMEM(wo_shape, BF16),
            pltpu.VMEM(wo_shape, BF16),
            pltpu.VMEM(position_bias.shape, BF16),
            pltpu.VMEM((3, rows, inner), F32),
            pltpu.VMEM((rows, feats), F32),
            pltpu.VMEM((3, rows, inner), BF16),
            pltpu.VMEM((n, rows, feats), F32),
            pltpu.VMEM((n, rows, feats), BF16),
            pltpu.VMEM((2, n, rows, feats), BF16),
            pltpu.VMEM((rows, inner), BF16),
            pltpu.VMEM((rows, inner), BF16),
            pltpu.VMEM((chunks, 8, step), F32),
            pltpu.VMEM((n, chunks, 8, step), F32),
            dma((2, n, chunks)),
            dma((n, chunks)),
            dma((n,)),
            dma((n,)),
            dma((3, 2, groups)),
            dma((3, groups)),
            dma((chunks,)),
            dma((chunks,)),
            dma((n, chunks)),
            dma((2, n, chunks)),
            dma((n, chunks)),
            dma((n, chunks)),
            dma((6,)),
            pltpu.SemaphoreType.REGULAR((2,)),
        ]
    stream, normed = pl.pallas_call(
        body,
        out_shape=(pltpu.VMEM((rows, feats), BF16), pltpu.VMEM((rows, feats), BF16)),
        in_specs=[any_space] * 6,
        out_specs=[vmem] * 2,
        scratch_shapes=scratch,
        compiler_params=pltpu.CompilerParams(
            collective_id=0, has_side_effects=True, vmem_limit_bytes=56 * 1024 * 1024
        ),
    )(tokens, pre_gain, input_weight, output_weight, position_bias, post_gain)
    shape = jax.ShapeDtypeStruct((rows, feats), BF16)
    return pl.pallas_call(
        publish,
        out_shape=(shape, shape),
        in_specs=[vmem] * 2,
        out_specs=[any_space] * 2,
        scratch_shapes=[dma((2,))],
        compiler_params=pltpu.CompilerParams(vmem_limit_bytes=4 * 1024 * 1024),
    )(stream, normed)


def solution(mesh):
    return jax.shard_map(
        functools.partial(on_device, mesh.shape["mp"], mesh.shape["dp"]),
        mesh=mesh,
        in_specs=(
            P("dp", "mp"),
            P("mp"),
            P(None, "dp", "mp"),
            P("mp", "dp"),
            P("mp", None, None),
            P("mp"),
        ),
        out_specs=(P("dp", "mp"), P("dp", "mp")),
        check_vma=False,
    )
```

```python
import functools

import jax
import jax.numpy as jnp
from jax import lax
from jax.experimental import pallas as pl
from jax.experimental.pallas import tpu as pltpu
from jax.sharding import PartitionSpec as P

epsilon = 1e-06
F32, BF16 = jnp.float32, jnp.bfloat16
MESH = pl.DeviceIdType.MESH


def kernel(
    n,
    groups,
    chunks,
    wide,
    tok,
    pre,
    win,
    wout,
    bias,
    post,
    stream_o,
    normed_o,
    x_all,
    gain_all,
    post_v,
    w_all,
    wo_all,
    wo_end,
    bias_v,
    acc,
    square,
    qkv,
    part,
    out_buf,
    landed,
    ctx_buf,
    ctx_in,
    ss_mine,
    ss_all,
    ag_send,
    ag_recv,
    g_send,
    g_recv,
    w_send,
    w_recv,
    ctx_send,
    ctx_recv,
    rs_send,
    rs_recv,
    ss_send,
    ss_recv,
    local_sem,
    link_free,
):
    rows, feats = tok.shape
    step = rows // chunks
    heads, seq = bias.shape[0], bias.shape[1]
    inner = win.shape[2]
    head_dim = inner // heads
    model = n * feats
    wrows = win.shape[1]
    wcols = model // groups
    half = groups // 2
    me = lax.axis_index("mp")
    d = lax.axis_index("dp")
    odd = lax.rem(d, 2)
    pair = d // 2
    partner = d + 1 - 2 * odd
    is_end = (me == 0) | (me == n - 1)
    is_edge = (me == 1) | (me == n - 2)
    all_rows = pl.ds(0, rows)

    def rows_at(c):
        return pl.ds(pl.multiple_of(c * step, step), step)

    def feats_at(s):
        return pl.ds(pl.multiple_of(s * feats, feats), feats)

    def loop(count, body, start=0):
        def wrapped(i, carry):
            body(i)
            return carry

        lax.fori_loop(start, count, wrapped, 0)

    def remote(src, dst, send, recv, target):
        return pltpu.make_async_remote_copy(
            src_ref=src,
            dst_ref=dst,
            send_sem=send,
            recv_sem=recv,
            device_id=target,
            device_id_type=MESH,
        )

    def tok_copy(s, c, up):
        ref = x_all.at[s, rows_at(c)]
        return remote(ref, ref, ag_send.at[up, s, c], ag_recv.at[s, c], {"mp": me + 2 * up - 1})

    def gain_copy(origin, target):
        ref = gain_all.at[feats_at(origin)]
        return remote(ref, ref, g_send.at[target], g_recv.at[origin], {"mp": target})

    def w_slot(o):
        return w_all.at[:, pl.ds(pl.multiple_of(o * wrows, wrows), wrows), :]

    def o_slot(ref, o):
        block = pl.ds(pl.multiple_of(o * wcols, wcols), wcols)
        return ref.at[:, block] if wide else ref.at[block, :]

    def slot(which, o):
        return w_slot(o) if which == 0 else o_slot(wo_all if which == 1 else wo_end, o)

    def weight_copy(which, o, target, forward):
        ref = slot(which, o)
        send = w_send.at[which, 1, o] if forward else w_send.at[which, 0, target]
        return remote(ref, ref, send, w_recv.at[which, o], {"dp": target})

    def cross_copy():
        inwards = jnp.where(me == 0, 1, n - 2)
        return remote(
            o_slot(wo_all, d), o_slot(wo_end, d), w_send.at[2, 0, d], w_recv.at[2, d], {"mp": inwards}
        )

    def ctx_copy(c):
        inwards = jnp.where(me == 0, 1, n - 2)
        return remote(
            ctx_buf.at[rows_at(c)], ctx_in.at[rows_at(c)], ctx_send.at[c], ctx_recv.at[c], {"mp": inwards}
        )

    def rs_copy(s, c, up):
        return remote(
            out_buf.at[s, rows_at(c)],
            landed.at[up, s, rows_at(c)],
            rs_send.at[s, c],
            rs_recv.at[up, s, c],
            {"mp": me + 2 * up - 1},
        )

    def ss_copy(origin, c, target):
        return remote(
            ss_mine.at[c], ss_all.at[origin, c], ss_send.at[target, c], ss_recv.at[origin, c], {"mp": target}
        )

    local = (
        pltpu.make_async_copy(tok, x_all.at[me], local_sem.at[0]),
        pltpu.make_async_copy(pre, gain_all.at[feats_at(me)], local_sem.at[1]),
        pltpu.make_async_copy(win, w_slot(d), local_sem.at[2]),
        pltpu.make_async_copy(wout, o_slot(wo_all, d), local_sem.at[3]),
        pltpu.make_async_copy(post, post_v, local_sem.at[4]),
        pltpu.make_async_copy(bias, bias_v, local_sem.at[5]),
    )
    for copy in local:
        copy.start()

    def peer_mp(k):
        return lax.rem(me + k, n)

    def same_core(k):
        return 2 * lax.rem(pair + k, half) + odd

    def from_core(k):
        return 2 * lax.rem(pair + half - k, half) + odd

    barrier = pltpu.get_barrier_semaphore()

    def greet(target):
        pl.semaphore_signal(barrier, inc=1, device_id=target, device_id_type=MESH)

    loop(n, lambda k: greet({"mp": peer_mp(k)}), 1)
    loop(half, lambda k: greet({"dp": same_core(k)}), 1)
    greet({"dp": partner})
    acc[...] = jnp.zeros_like(acc)
    square[...] = jnp.zeros_like(square)
    for copy in local[:5]:
        copy.wait()
    pl.semaphore_wait(barrier, n - 1 + half - 1 + 1)

    def can_send(up):
        return (me < n - 1) if up else (me > 0)

    def send_own(up):
        @pl.when(can_send(up))
        def _():
            @pl.when(odd == 1)
            def _():
                pl.semaphore_wait(link_free.at[up], 1)

            loop(chunks, lambda c: tok_copy(me, c, up).start())

    def release(up):
        @pl.when(can_send(up))
        def _():
            pl.semaphore_signal(
                link_free.at[up], inc=1, device_id={"dp": partner}, device_id_type=MESH
            )

    def send_weights(which):
        weight_copy(which, d, partner, False).start()
        loop(half, lambda k: weight_copy(which, d, same_core(k), False).start(), 1)

    def forward_weights(which):
        def forward(k):
            o = from_core(k)
            weight_copy(which, o, partner, False).wait_recv()
            weight_copy(which, o, partner, True).start()

        loop(half, forward, 1)

    def other_weights(which):
        loop(half, lambda k: weight_copy(which, 2 * k + 1 - odd, partner, False).wait_recv())

    def pass_end_weights():
        @pl.when(is_edge)
        def _():
            weight_copy(2, d, partner, False).wait_recv()
            send_weights(2)

    def forward_out_weights():
        pl.when(jnp.logical_not(is_end))(lambda: forward_weights(1))
        pl.when(is_edge)(lambda: forward_weights(2))

    def take(up, j, use=None):
        s = me - j if up else me + j

        @pl.when((s >= 0) & (s < n))
        def _():
            def one(c):
                tok_copy(s, c, up).wait_recv()

                @pl.when(can_send(up))
                def _():
                    tok_copy(s, c, up).start()

                if use is not None:
                    use(s, c)

            loop(chunks, one)

    def accumulate(s, at):
        gain = gain_all[feats_at(s)].astype(F32).reshape(1, feats)
        x = x_all[s, at, :].astype(F32)
        square[at, :] += x * x
        xg = (x * gain).astype(BF16)
        for m in range(3):
            acc[m, at, :] += jnp.dot(xg, w_all[m, feats_at(s), :], preferred_element_type=F32)

    def both_ways(action):
        @pl.when(2 * me < n)
        def _():
            action(0)
            action(1)

        @pl.when(2 * me >= n)
        def _():
            action(1)
            action(0)

    def finish(c):
        total = jnp.sum(square[rows_at(c), :], axis=1, keepdims=True)
        inverse = lax.rsqrt(total / model + epsilon)
        for m in range(3):
            qkv[m, rows_at(c), :] = (acc[m, rows_at(c), :] * inverse).astype(BF16)

    def send_all_weights():
        send_weights(0)
        pl.when(is_end)(lambda: cross_copy().start())
        pl.when(jnp.logical_not(is_end))(lambda: send_weights(1))

    def wait_gains():
        loop(n, lambda k: gain_copy(peer_mp(k), peer_mp(k)).wait_recv(), 1)

    def gather_even():
        both_ways(send_own)
        send_all_weights()

        @pl.when(is_end)
        def _():
            up = jnp.where(me == 0, 1, 0)
            loop(chunks, lambda c: tok_copy(me, c, up).wait_send())
            both_ways(release)

        def hop(j):
            def one(c):
                def side(up):
                    s = me - j if up else me + j

                    @pl.when((s >= 0) & (s < n))
                    def _():
                        tok_copy(s, c, up).wait_recv()
                        pl.when(can_send(up))(lambda: tok_copy(s, c, up).start())

                both_ways(side)

            loop(chunks, one)

        loop(n, hop, 1)
        pl.when(jnp.logical_not(is_end))(lambda: both_ways(release))
        pass_end_weights()
        forward_weights(0)
        wait_gains()
        other_weights(0)
        loop(n, lambda s: accumulate(s, all_rows))
        loop(chunks, finish)

    def gather_odd():
        send_all_weights()
        both_ways(send_own)

        def toward(near):
            far = 1 - near
            reach = n - 1 - me if near else me
            loop(n, lambda j: take(near, j), 1)
            pass_end_weights()
            forward_weights(0)
            wait_gains()
            take(far, 1)
            other_weights(0)

            def known(s):
                pl.when((s <= me + 1) if near else (s >= me - 1))(lambda: accumulate(s, all_rows))

            loop(n, known)

            def later(j):
                @pl.when(j < reach)
                def _():
                    take(far, j)
                    accumulate(me + j if near else me - j, all_rows)

            def use(s, c):
                accumulate(s, rows_at(c))
                finish(c)

            loop(n, later, 2)
            pl.when(reach > 1)(lambda: take(far, reach, use))
            pl.when(reach <= 1)(lambda: loop(chunks, finish))

        pl.when(2 * me < n)(lambda: toward(1))
        pl.when(2 * me >= n)(lambda: toward(0))
        forward_out_weights()

    loop(n, lambda k: gain_copy(me, peer_mp(k)).start(), 1)
    pl.when(odd == 0)(gather_even)
    pl.when(odd == 1)(gather_odd)

    local[5].wait()

    lane_head = lax.broadcasted_iota(jnp.int32, (1, inner), 1) // head_dim
    contract = (((1,), (1,)), ((), ()))

    def attend(c):
        first = (c * step) // seq * seq
        keys_at = pl.ds(pl.multiple_of(first, seq), seq)
        bias_at = pl.ds(pl.multiple_of(c * step - first, step), step)
        q = qkv[0, rows_at(c), :]
        k = qkv[1, keys_at, :]
        v = qkv[2, keys_at, :]
        stacked = jnp.concatenate([jnp.where(lane_head == h, q, jnp.zeros_like(q)) for h in range(heads)], axis=0)
        scores = lax.dot_general(stacked, k, contract, preferred_element_type=F32)
        scores = scores + bias_v[:, bias_at, :].reshape(heads * step, seq).astype(F32)
        weights = jnp.exp(scores - jnp.max(scores, axis=1, keepdims=True))
        scale = 1.0 / jnp.sum(weights, axis=1, keepdims=True)
        mixed = jnp.dot(weights.astype(BF16), v, preferred_element_type=F32) * scale
        context = mixed[0:step]
        for h in range(1, heads):
            context = jnp.where(lane_head == h, mixed[h * step : (h + 1) * step], context)
        ctx_buf[rows_at(c), :] = context.astype(BF16)
        pl.when(is_end)(lambda: ctx_copy(c).start())

    loop(chunks, attend)

    def project_out(context, ref, s):
        block = feats_at(s)
        if wide:
            return jnp.dot(context, ref[:, block], preferred_element_type=F32)
        return lax.dot_general(context, ref[block, :], contract, preferred_element_type=F32)

    def send_out(s, c, up, value):
        out_buf[s, rows_at(c), :] = value.astype(BF16)
        rs_copy(s, c, up).start()

    def own_share(s):
        part[s] = project_out(ctx_buf[...], wo_all, s)

    def originate(c):
        ctx_copy(c).wait_recv()
        context = ctx_in[rows_at(c), :]

        def far(k):
            s = jnp.where(me == 1, n - 1 - k, k)
            value = part[s, rows_at(c), :] + project_out(context, wo_end, s)
            send_out(s, c, jnp.where(me == 1, 1, 0), value)

        def near(k):
            s = jnp.where(me == 1, k, n - 2 + k)
            part[s, rows_at(c), :] += project_out(context, wo_end, s)

        loop(n - 2, far)
        loop(2, near)

    def finished(s, c):
        value = x_all[s, rows_at(c), :].astype(F32) + part[s, rows_at(c), :]
        stream = value.astype(BF16)
        wide_stream = stream.astype(F32)
        return stream, wide_stream * wide_stream

    def finalize(c):
        stream, squares = finished(me, c)
        stream_o[rows_at(c), :] = stream
        part[me, rows_at(c), :] = squares

        @pl.when(is_edge)
        def _():
            end, up = jnp.where(me == 1, 0, n - 1), jnp.where(me == 1, 0, 1)
            stream_end, squares_end = finished(end, c)
            out_buf[end, rows_at(c), :] = stream_end
            rs_copy(end, c, up).start()
            part[me, rows_at(c), :] += squares_end

        total = jnp.sum(part[me, rows_at(c), :], axis=1, keepdims=True)
        turned = jnp.transpose(jnp.broadcast_to(total, (step, 128)))
        ss_mine[c] = turned[0:8, :]
        ss_all[me, c] = turned[0:8, :]
        loop(n, lambda k: ss_copy(me, c, peer_mp(k)).start(), 1)

    def combine(c):
        def message(k):
            for up in (1, 0):
                s = n - 1 - k if up else k
                follows = (me >= 2) if up else (me <= n - 3)
                further = (s > me) if up else (s < me)
                last = (me == n - 2) if up else (me == 1)

                @pl.when(follows & (further | (s == me)))
                def _():
                    rs_copy(s, c, up).wait_recv()
                    value = part[s, rows_at(c), :] + landed[up, s, rows_at(c), :].astype(F32)

                    @pl.when((s == me) | last)
                    def _():
                        part[s, rows_at(c), :] = value

                    @pl.when((s != me) & jnp.logical_not(last))
                    def _():
                        send_out(s, c, up, value)

        loop(n - 2, message)
        finalize(c)

    @pl.when(jnp.logical_not(is_end))
    def _():
        pl.when(odd == 0)(forward_out_weights)
        other_weights(1)
        pl.when(is_edge)(lambda: other_weights(2))
        loop(n, own_share)
        pl.when(is_edge)(lambda: loop(chunks, originate))
        loop(chunks, combine)

    gain = post_v[...].astype(F32).reshape(1, feats)

    def normalize(c):
        def arrived(s):
            pl.when(s != me)(lambda: ss_copy(s, c, s).wait_recv())

        loop(n - 1, arrived, 1)

        @pl.when(is_end)
        def _():
            up = jnp.where(me == 0, 0, 1)
            rs_copy(me, c, up).wait_recv()
            stream_o[rows_at(c), :] = landed[up, me, rows_at(c), :]

        total = jnp.zeros((8, step), F32)
        for s in range(1, n - 1):
            total = total + ss_all[s, c]
        scale = jnp.transpose(lax.rsqrt(total / model + epsilon))[:, 0:1]
        stream = stream_o[rows_at(c), :].astype(F32)
        normed_o[rows_at(c), :] = (stream * scale * gain).astype(BF16)

    loop(chunks, normalize)

    loop(n, lambda k: gain_copy(me, peer_mp(k)).wait_send(), 1)

    def drain_tokens(s):
        def one(c):
            waited = (odd == 0) & (s == me) & is_end

            @pl.when((s <= me) & (me < n - 1) & jnp.logical_not(waited))
            def _():
                tok_copy(s, c, 1).wait_send()

            @pl.when((s >= me) & (me > 0) & jnp.logical_not(waited))
            def _():
                tok_copy(s, c, 0).wait_send()

            @pl.when(jnp.logical_not(is_end) & (s != me))
            def _():
                rs_copy(s, c, 1).wait_send()
                ss_copy(me, c, s).wait_send()

        loop(chunks, one)

    loop(n, drain_tokens)

    def drain_weights(which):
        weight_copy(which, d, partner, False).wait_send()

        def drain(k):
            weight_copy(which, d, same_core(k), False).wait_send()
            weight_copy(which, from_core(k), partner, True).wait_send()

        loop(half, drain, 1)

    drain_weights(0)
    pl.when(is_edge)(lambda: drain_weights(2))

    @pl.when(is_end)
    def _():
        cross_copy().wait_send()
        loop(chunks, lambda c: ctx_copy(c).wait_send())

    pl.when(jnp.logical_not(is_end))(lambda: drain_weights(1))


def line_kernel(
    n,
    groups,
    chunks,
    tok,
    pre,
    win,
    wout,
    bias,
    post,
    stream_o,
    normed_o,
    x_all,
    gain_all,
    post_v,
    w_all,
    wo_own,
    wo_all,
    bias_v,
    acc,
    square,
    qkv,
    ctx_all,
    part,
    out_buf,
    landed,
    ss_mine,
    ss_all,
    ag_send,
    ag_recv,
    g_send,
    g_recv,
    w_send,
    w_recv,
    x_send,
    o_send,
    o_recv,
    ctx_send,
    ctx_recv,
    end_send,
    end_recv,
    ss_send,
    ss_recv,
    local_sem,
    link_free,
):
    rows, feats = tok.shape
    step = rows // chunks
    pieces = ag_recv.shape[1]
    piece = rows // pieces
    head = pieces // 8
    heads, seq = bias.shape[0], bias.shape[1]
    inner = win.shape[2]
    head_dim = inner // heads
    model = n * feats
    wrows = win.shape[1]
    wcols = model // groups
    half = groups // 2
    me = lax.axis_index("mp")
    d = lax.axis_index("dp")
    odd = lax.rem(d, 2)
    pair = d // 2
    partner = d + 1 - 2 * odd
    low = 2 * me < n
    is_end = (me == 0) | (me == n - 1)
    is_inner = jnp.logical_not(is_end)
    near_end, far_end = jnp.where(low, 0, n - 1), jnp.where(low, n - 1, 0)
    other_inner = n - 1 - me
    inwards = me + jnp.where(low, 1, -1)
    home = jnp.where(d < half, 1, n - 2)
    is_source = me == home
    late_cross = is_end & (home == inwards) & (odd == 1)
    all_rows = pl.ds(0, rows)

    def rows_at(c):
        return pl.ds(pl.multiple_of(c * step, step), step)

    def feats_at(s):
        return pl.ds(pl.multiple_of(s * feats, feats), feats)

    def loop(count, body, start=0):
        def wrapped(i, carry):
            body(i)
            return carry

        lax.fori_loop(start, count, wrapped, 0)

    def remote(src, dst, send, recv, target):
        return pltpu.make_async_remote_copy(
            src_ref=src,
            dst_ref=dst,
            send_sem=send,
            recv_sem=recv,
            device_id=target,
            device_id_type=MESH,
        )

    def tok_copy(s, c, up):
        ref = x_all.at[s, pl.ds(pl.multiple_of(c * piece, piece), piece)]
        return remote(ref, ref, ag_send.at[up, s], ag_recv.at[s, c], {"mp": me + 2 * up - 1})

    def sent(ref, sem):
        remote(ref, ref, sem, ctx_recv.at[0], {"mp": inwards}).wait_send()

    def tokens_sent(s, up):
        sent(x_all.at[s], ag_send.at[up, s])

    def gain_copy(origin, target):
        ref = gain_all.at[feats_at(origin)]
        return remote(ref, ref, g_send.at[0], g_recv.at[0], {"mp": target})

    def all_gains():
        ref = gain_all.at[pl.ds(0, (n - 1) * feats)]
        return remote(ref, ref, g_send.at[0], g_recv.at[0], {"mp": inwards})

    def w_slot(o):
        return w_all.at[:, pl.ds(pl.multiple_of(o * wrows, wrows), wrows), :]

    def w_copy(o, target, forward):
        send = w_send.at[1 if forward else 0]
        return remote(w_slot(o), w_slot(o), send, w_recv.at[o], {"dp": target})

    def o_slot(z, o):
        return wo_all.at[z, lax.rem(o, half)]

    def o_copy(z, o, target, forward):
        send = o_send.at[1 if forward else 0]
        return remote(o_slot(z, o), o_slot(z, o), send, o_recv.at[z, lax.rem(o, half)], {"dp": target})

    def cross_copy():
        return remote(wo_own, o_slot(me, d), x_send.at[0], o_recv.at[me, lax.rem(d, half)], {"mp": home})

    def ctx_place(s, c):
        return jnp.where(s == 0, c, jnp.where(s == n - 1, chunks + c, 2 * chunks))

    def ctx_copy(s, c):
        ref = ctx_all.at[s, rows_at(c)]
        return remote(ref, ref, ctx_send.at[jnp.where(s == me, 0, 1)], ctx_recv.at[ctx_place(s, c)], {"mp": inwards})

    def end_copy(c):
        return remote(
            out_buf.at[rows_at(c)], landed.at[rows_at(c)], end_send.at[0], end_recv.at[c], {"mp": near_end}
        )

    def ss_copy(origin, c, target):
        return remote(
            ss_mine.at[c], ss_all.at[origin, c], ss_send.at[0], ss_recv.at[jnp.where(origin == 1, 0, 1), c], {"mp": target}
        )

    tok_in = pltpu.make_async_copy(tok, x_all.at[me], local_sem.at[0])
    win_in = pltpu.make_async_copy(win, w_slot(d), local_sem.at[1])
    pre_in = pltpu.make_async_copy(pre, gain_all.at[feats_at(me)], local_sem.at[2])
    post_in = pltpu.make_async_copy(post, post_v, local_sem.at[3])
    bias_in = pltpu.make_async_copy(bias, bias_v, local_sem.at[4])

    def wout_in(action):
        pl.when(is_source)(lambda: action(pltpu.make_async_copy(wout, o_slot(me, d), local_sem.at[5])))
        pl.when(jnp.logical_not(is_source))(
            lambda: action(pltpu.make_async_copy(wout, wo_own, local_sem.at[5]))
        )

    tok_in.start()
    win_in.start()
    pre_in.start()
    wout_in(lambda copy: copy.start())

    def peer_mp(k):
        return lax.rem(me + k, n)

    def same_core(k):
        return 2 * lax.rem(pair + k, half) + odd

    def from_core(k):
        return 2 * lax.rem(pair + half - k, half) + odd

    barrier = pltpu.get_barrier_semaphore()

    def greet(target):
        pl.semaphore_signal(barrier, inc=1, device_id=target, device_id_type=MESH)

    loop(n, lambda k: greet({"mp": peer_mp(k)}), 1)
    loop(half, lambda k: greet({"dp": same_core(k)}), 1)
    greet({"dp": partner})
    acc[...] = jnp.zeros_like(acc)
    square[...] = jnp.zeros_like(square)
    tok_in.wait()
    post_in.start()
    bias_in.start()
    pl.semaphore_wait(barrier, n - 1 + half - 1 + 1)

    def can_send(up):
        return (me < n - 1) if up else (me > 0)

    def send_own(up):
        @pl.when(can_send(up))
        def _():
            @pl.when(odd == 1)
            def _():
                pl.semaphore_wait(link_free.at[up], 1)
                loop(pieces, lambda c: tok_copy(me, c, up).start(), head)

            pl.when(odd == 0)(lambda: loop(pieces, lambda c: tok_copy(me, c, up).start()))

    def send_head(up):
        pl.when(can_send(up))(lambda: loop(head, lambda c: tok_copy(me, c, up).start()))

    def release(up):
        @pl.when(can_send(up))
        def _():
            pl.semaphore_signal(
                link_free.at[up], inc=1, device_id={"dp": partner}, device_id_type=MESH
            )

    def both_ways(action):
        @pl.when(low)
        def _():
            action(0)
            action(1)

        @pl.when(jnp.logical_not(low))
        def _():
            action(1)
            action(0)

    def in_plane(o):
        return (o < half) == (me == 1)

    def send_slice(z):
        o_copy(z, d, partner, False).start()
        loop(half, lambda k: o_copy(z, d, same_core(k), False).start(), 1)

    def relay_slice(z):
        @pl.when(is_source)
        def _():
            o_copy(z, d, partner, False).wait_recv()
            send_slice(z)

    def forward_slices(z):
        def forward(k):
            o = from_core(k)

            @pl.when(in_plane(o))
            def _():
                o_copy(z, o, partner, False).wait_recv()
                o_copy(z, o, partner, True).start()

        loop(half, forward, 1)

    def other_slices(z):
        def other(k):
            o = 2 * k + 1 - odd
            pl.when(in_plane(o))(lambda: o_copy(z, o, partner, False).wait_recv())

        loop(half, other)

    def send_weights():
        win_in.wait()
        w_copy(d, partner, False).start()
        loop(half, lambda k: w_copy(d, same_core(k), False).start(), 1)
        pre_in.wait()
        loop(n, lambda k: gain_copy(me, peer_mp(k)).start(), 1)
        wout_in(lambda copy: copy.wait())
        pl.when(is_source)(lambda: send_slice(me))
        pl.when(jnp.logical_not(is_source | late_cross))(lambda: cross_copy().start())

    def forward_weights():
        def forward(k):
            o = from_core(k)
            w_copy(o, partner, False).wait_recv()
            w_copy(o, partner, True).start()

        loop(half, forward, 1)
        all_gains().wait_recv()

    def other_weights():
        loop(half, lambda k: w_copy(2 * k + 1 - odd, partner, False).wait_recv())

    def take(up, j, use=None):
        s = me - j if up else me + j

        @pl.when((s >= 0) & (s < n))
        def _():
            def one(c):
                tok_copy(s, c, up).wait_recv()
                pl.when(can_send(up))(lambda: tok_copy(s, c, up).start())

            if use is None:
                loop(pieces, one)
            else:
                per = pieces // chunks

                def block(c):
                    loop(per, lambda i: one(c * per + i))
                    use(s, c)

                loop(chunks, block)

    def accumulate(s, at):
        gain = gain_all[feats_at(s)].astype(F32).reshape(1, feats)
        x = x_all[s, at, :].astype(F32)
        square[at, :] += x * x
        xg = (x * gain).astype(BF16)
        for m in range(3):
            acc[m, at, :] += jnp.dot(xg, w_all[m, feats_at(s), :], preferred_element_type=F32)

    def finish(c):
        total = jnp.sum(square[rows_at(c), :], axis=1, keepdims=True)
        inverse = lax.rsqrt(total / model + epsilon)
        for m in range(3):
            qkv[m, rows_at(c), :] = (acc[m, rows_at(c), :] * inverse).astype(BF16)

    def gather_by_shard(near):
        far = 1 - near
        reach = n - 1 - me if near else me
        loop(n, lambda j: take(near, j), 1)
        pl.when(late_cross)(lambda: cross_copy().start())
        forward_weights()
        relay_slice(near_end)
        relay_slice(far_end)
        relay_slice(other_inner)
        take(far, 1)
        other_weights()

        def known(s):
            pl.when((s <= me + 1) if near else (s >= me - 1))(lambda: accumulate(s, all_rows))

        loop(n, known)

        def later(j):
            @pl.when(j < reach)
            def _():
                take(far, j)
                accumulate(me + j if near else me - j, all_rows)

        def use(s, c):
            accumulate(s, rows_at(c))
            finish(c)

        loop(n, later, 2)
        take(far, reach, use)

    def by_shard():
        pl.when(low)(lambda: gather_by_shard(1))
        pl.when(jnp.logical_not(low))(lambda: gather_by_shard(0))

    def gather_even():
        both_ways(send_own)
        send_weights()

        @pl.when(is_end)
        def _():
            up = jnp.where(me == 0, 1, 0)
            tokens_sent(me, up)
            both_ways(release)
            by_shard()

        def hop(j, start=0, stop=pieces):
            def one(c):
                def side(up):
                    s = me - j if up else me + j

                    @pl.when((s >= 0) & (s < n))
                    def _():
                        tok_copy(s, c, up).wait_recv()
                        pl.when(can_send(up))(lambda: tok_copy(s, c, up).start())

                both_ways(side)

            loop(stop, one, start)

        @pl.when(is_inner)
        def _():
            hop(1)
            pl.when(low)(lambda: release(0))
            pl.when(jnp.logical_not(low))(lambda: release(1))
            hop(2, 0, pieces // 2)
            pl.when(low)(lambda: release(1))
            pl.when(jnp.logical_not(low))(lambda: release(0))
            hop(2, pieces // 2)
            forward_weights()
            relay_slice(near_end)
            relay_slice(far_end)
            relay_slice(other_inner)
            other_weights()
            loop(n, lambda s: accumulate(s, all_rows))
            loop(chunks, finish)
            forward_slices(me)

    def gather_odd():
        both_ways(send_head)
        send_weights()
        both_ways(send_own)
        by_shard()

        @pl.when(is_inner)
        def _():
            forward_slices(me)
            forward_slices(near_end)
            forward_slices(far_end)

    pl.when(odd == 0)(gather_even)
    pl.when(odd == 1)(gather_odd)
    post_in.wait()
    bias_in.wait()

    lane_head = lax.broadcasted_iota(jnp.int32, (1, inner), 1) // head_dim
    contract = (((1,), (1,)), ((), ()))

    def attend(c):
        first = (c * step) // seq * seq
        keys_at = pl.ds(first, seq)
        bias_at = pl.ds(c * step - first, step)
        q = qkv[0, rows_at(c), :]
        k = qkv[1, keys_at, :]
        v = qkv[2, keys_at, :]
        stacked = jnp.concatenate([jnp.where(lane_head == h, q, jnp.zeros_like(q)) for h in range(heads)], axis=0)
        scores = lax.dot_general(stacked, k, contract, preferred_element_type=F32)
        scores = scores + bias_v[:, bias_at, :].reshape(heads * step, seq).astype(F32)
        weights = jnp.exp(scores - jnp.max(scores, axis=1, keepdims=True))
        scale = 1.0 / jnp.sum(weights, axis=1, keepdims=True)
        mixed = jnp.dot(weights.astype(BF16), v, preferred_element_type=F32) * scale
        context = mixed[0:step]
        for h in range(1, heads):
            context = jnp.where(lane_head == h, mixed[h * step : (h + 1) * step], context)
        ctx_all[me, rows_at(c), :] = context.astype(BF16)

    starts = [0, *range(1, chunks, 2), chunks]
    for c, stop in zip(starts[:-1], starts[1:]):
        together = range(c, stop)
        for i in together:
            attend(i)
        for i in together:
            ctx_copy(me, i).start()

    def drain_line(s):
        waited = (odd == 0) & (s == me) & is_end

        @pl.when((s <= me) & (me < n - 1) & jnp.logical_not(waited))
        def _():
            tokens_sent(s, 1)

        @pl.when((s >= me) & (me > 0) & jnp.logical_not(waited))
        def _():
            tokens_sent(s, 0)

    def drain_early():
        all_gains().wait_send()
        loop(n, drain_line)
        sent(w_all.at[:, pl.ds(0, half * wrows), :], w_send.at[0])
        sent(w_all.at[:, pl.ds(0, (half - 1) * wrows), :], w_send.at[1])
        pl.when(jnp.logical_not(is_source))(lambda: cross_copy().wait_send())
        sent(ctx_all.at[me], ctx_send.at[0])

    def project_out(s, at, first=False):
        weight = jnp.concatenate([wo_all[s, i] for i in range(wo_all.shape[1])], axis=1)
        value = jnp.dot(ctx_all[s, at, :], weight, preferred_element_type=F32)
        part[at, :] = value if first else part[at, :] + value

    def pass_on(c):
        ctx_copy(near_end, c).wait_recv()
        ctx_copy(near_end, c).start()

    def finalize(c):
        def block(s, at):
            slots = wo_all.shape[1] // 2
            start = slots * (at.start // feats)
            weight = jnp.concatenate([wo_all[far_end, start + i] for i in range(slots)], axis=1)
            value = jnp.dot(ctx_all[far_end, rows_at(c), :], weight, preferred_element_type=F32)
            value = x_all[s, rows_at(c), :].astype(F32) + (part[rows_at(c), at] + value)
            stream = value.astype(BF16)
            wide_stream = stream.astype(F32)
            return stream, wide_stream * wide_stream

        def both(own_at, end_at):
            stream_end, squares_end = block(near_end, end_at)
            out_buf[rows_at(c), :] = stream_end
            end_copy(c).start()
            stream, squares = block(me, own_at)
            stream_o[rows_at(c), :] = stream
            total = jnp.sum(squares + squares_end, axis=1, keepdims=True)
            turned = jnp.transpose(jnp.broadcast_to(total, (step, 128)))
            ss_mine[c] = turned[0:8, :]
            ss_all[me, c] = turned[0:8, :]

        pl.when(low)(lambda: both(pl.ds(feats, feats), pl.ds(0, feats)))
        pl.when(jnp.logical_not(low))(lambda: both(pl.ds(0, feats), pl.ds(feats, feats)))
        loop(n, lambda k: ss_copy(me, c, peer_mp(k)).start(), 1)

    pl.when(is_end)(drain_early)

    @pl.when(is_inner)
    def _():
        @pl.when(odd == 0)
        def _():
            forward_slices(near_end)
            forward_slices(far_end)

        pl.when(odd == 1)(lambda: forward_slices(other_inner))
        other_slices(me)
        project_out(me, all_rows, True)
        other_slices(near_end)
        def near(c):
            pass_on(c)
            project_out(near_end, rows_at(c))

        loop(chunks // 2, near)
        pl.when(odd == 0)(lambda: forward_slices(other_inner))
        loop(chunks, near, chunks // 2)
        other_slices(other_inner)
        ref = ctx_all.at[other_inner]
        remote(ref, ref, ctx_send.at[0], ctx_recv.at[2 * chunks], {"mp": inwards}).wait_recv()
        project_out(other_inner, all_rows)
        other_slices(far_end)

        def last(c):
            ctx_copy(far_end, c).wait_recv()
            finalize(c)

        loop(chunks, last)

    gain = post_v[...].astype(F32).reshape(1, feats)

    def normalize(c):
        def arrived(s):
            pl.when(s != me)(lambda: ss_copy(s, c, s).wait_recv())

        loop(n - 1, arrived, 1)

        @pl.when(is_end)
        def _():
            end_copy(c).wait_recv()
            stream_o[rows_at(c), :] = landed[rows_at(c), :]

        total = ss_all[1, c] + ss_all[n - 2, c]
        scale = jnp.transpose(lax.rsqrt(total / model + epsilon))[:, 0:1]
        stream = stream_o[rows_at(c), :].astype(F32)
        normed_o[rows_at(c), :] = (stream * scale * gain).astype(BF16)

    loop(chunks, normalize)

    @pl.when(is_inner)
    def _():
        drain_early()
        sent(ctx_all.at[near_end], ctx_send.at[1])
        sent(out_buf, end_send.at[0])
        sent(ss_all.at[pl.ds(0, n - 1)], ss_send.at[0])
        few, many = pl.ds(0, half // 2 - 1), pl.ds(0, half // 2)
        pl.when(is_source)(lambda: sent(wo_all, o_send.at[0]))
        pl.when(is_source)(lambda: sent(wo_all.at[:, few], o_send.at[1]))
        pl.when(jnp.logical_not(is_source))(lambda: sent(wo_all.at[:, many], o_send.at[1]))


def publish(stream_i, normed_i, stream_o, normed_o, sems):
    copies = (
        pltpu.make_async_copy(stream_i, stream_o, sems.at[0]),
        pltpu.make_async_copy(normed_i, normed_o, sems.at[1]),
    )
    for copy in copies:
        copy.start()
    for copy in copies:
        copy.wait()


def on_device(n, groups, tokens, pre_gain, input_weight, output_weight, position_bias, post_gain):
    rows, feats = tokens.shape
    step = 128
    chunks = rows // step
    inner = input_weight.shape[2]
    model = n * feats
    wide = output_weight.shape[1] % 128 == 0
    if not wide:
        output_weight = output_weight.T
    dma, any_space = pltpu.SemaphoreType.DMA, pl.BlockSpec(memory_space=pl.ANY)
    vmem = pl.BlockSpec(memory_space=pltpu.VMEM)
    if wide and n - 2 == 2:
        pieces = rows // 64
        body = functools.partial(line_kernel, n, groups, chunks)
        scratch = [
            pltpu.VMEM((n, rows, feats), BF16),
            pltpu.VMEM((n * feats,), BF16),
            pltpu.VMEM((feats,), BF16),
            pltpu.VMEM((3, model, inner), BF16),
            pltpu.VMEM(output_weight.shape, BF16),
            pltpu.VMEM((n, groups // 2, inner, output_weight.shape[1]), BF16),
            pltpu.VMEM(position_bias.shape, BF16),
            pltpu.VMEM((3, rows, inner), F32),
            pltpu.VMEM((rows, feats), F32),
            pltpu.VMEM((3, rows, inner), BF16),
            pltpu.VMEM((n, rows, inner), BF16),
            pltpu.VMEM((rows, 2 * feats), F32),
            pltpu.VMEM((rows, feats), BF16),
            pltpu.VMEM((rows, feats), BF16),
            pltpu.VMEM((chunks, 8, step), F32),
            pltpu.VMEM((n, chunks, 8, step), F32),
            dma((2, n)),
            dma((n, pieces)),
            dma((1,)),
            dma((1,)),
            dma((2,)),
            dma((groups,)),
            dma((1,)),
            dma((2,)),
            dma((n, groups // 2)),
            dma((2,)),
            dma((2 * chunks + 1,)),
            dma((1,)),
            dma((chunks,)),
            dma((1,)),
            dma((2, chunks)),
            dma((6,)),
            pltpu.SemaphoreType.REGULAR((2,)),
        ]
    else:
        body = functools.partial(kernel, n, groups, chunks, wide)
        wo_shape = (inner, model) if wide else (model, inner)
        scratch = [
            pltpu.VMEM((n, rows, feats), BF16),
            pltpu.VMEM((n * feats,), BF16),
            pltpu.VMEM((feats,), BF16),
            pltpu.VMEM((3, model, inner), BF16),
            pltpu.VMEM(wo_shape, BF16),
            pltpu.VMEM(wo_shape, BF16),
            pltpu.VMEM(position_bias.shape, BF16),
            pltpu.VMEM((3, rows, inner), F32),
            pltpu.VMEM((rows, feats), F32),
            pltpu.VMEM((3, rows, inner), BF16),
            pltpu.VMEM((n, rows, feats), F32),
            pltpu.VMEM((n, rows, feats), BF16),
            pltpu.VMEM((2, n, rows, feats), BF16),
            pltpu.VMEM((rows, inner), BF16),
            pltpu.VMEM((rows, inner), BF16),
            pltpu.VMEM((chunks, 8, step), F32),
            pltpu.VMEM((n, chunks, 8, step), F32),
            dma((2, n, chunks)),
            dma((n, chunks)),
            dma((n,)),
            dma((n,)),
            dma((3, 2, groups)),
            dma((3, groups)),
            dma((chunks,)),
            dma((chunks,)),
            dma((n, chunks)),
            dma((2, n, chunks)),
            dma((n, chunks)),
            dma((n, chunks)),
            dma((6,)),
            pltpu.SemaphoreType.REGULAR((2,)),
        ]
    stream, normed = pl.pallas_call(
        body,
        out_shape=(pltpu.VMEM((rows, feats), BF16), pltpu.VMEM((rows, feats), BF16)),
        in_specs=[any_space] * 6,
        out_specs=[vmem] * 2,
        scratch_shapes=scratch,
        compiler_params=pltpu.CompilerParams(
            collective_id=0, has_side_effects=True, vmem_limit_bytes=56 * 1024 * 1024
        ),
    )(tokens, pre_gain, input_weight, output_weight, position_bias, post_gain)
    shape = jax.ShapeDtypeStruct((rows, feats), BF16)
    return pl.pallas_call(
        publish,
        out_shape=(shape, shape),
        in_specs=[vmem] * 2,
        out_specs=[any_space] * 2,
        scratch_shapes=[dma((2,))],
        compiler_params=pltpu.CompilerParams(vmem_limit_bytes=4 * 1024 * 1024),
    )(stream, normed)


def solution(mesh):
    return jax.shard_map(
        functools.partial(on_device, mesh.shape["mp"], mesh.shape["dp"]),
        mesh=mesh,
        in_specs=(
            P("dp", "mp"),
            P("mp"),
            P(None, "dp", "mp"),
            P("mp", "dp"),
            P("mp", None, None),
            P("mp"),
        ),
        out_specs=(P("dp", "mp"), P("dp", "mp")),
        check_vma=False,
    )
```
